32 devices in a mesh: dp: 8 (over z, y), tensor: 4 (over x, core).
Axes of the slice: x: 2, y: 2, z: 4, core: 2. Of those that a mesh axis runs over, the one named last changes fastest.
Arguments:
- tokens: bfloat16 [1024, 16, 768], P(('dp', 'tensor')), may hold values from -6 to 6
- lengths: int32 [16], replicated, may hold values from 1 to 1024, 12288 in all
- dealing: int32 [16], replicated, may hold values from 0 to 15, each once
- project_weight: bfloat16 [768, 2304], P('dp', 'tensor'), may hold values from -0.21875 to 0.21875
- query_projection_bias: float32 [768], replicated, may hold values from -3 to 3
- value_projection_bias: float32 [768], replicated, may hold values from -3 to 3
- attention_output_weight: bfloat16 [768, 768], P('dp', 'tensor'), may hold values from -3.5 to 3.5
- attention_output_bias: float32 [768], replicated, may hold values from -3 to 3
- first_gain: float32 [768], replicated, may hold values from 0.5 to 1.5
- first_shift: float32 [768], replicated, may hold values from -3 to 3
- feed_input_weight: bfloat16 [768, 3072], P('dp', 'tensor'), may hold values from -0.21875 to 0.21875
- feed_input_bias: float32 [3072], replicated, may hold values from -3 to 3
- feed_output_weight: bfloat16 [768, 3072], P('dp', 'tensor'), may hold values from -0.109375 to 0.109375
- feed_output_bias: float32 [768], replicated, may hold values from -3 to 3
- second_gain: float32 [768], replicated, may hold values from 0.5 to 1.5
- second_shift: float32 [768], replicated, may hold values from -3 to 3
- output_grad: bfloat16 [1024, 16, 768], P(('dp', 'tensor')), may hold values from -6 to 6
Outputs:
- layer_output: bfloat16 [1024, 16, 768], P('tensor', 'dp')
- tokens_grad: bfloat16 [1024, 16, 768], P(('dp', 'tensor'))
- project_grad: float32 [768, 2304], P('dp', 'tensor')
- query_bias_grad: float32 [768], P(('dp', 'tensor'))
- value_bias_grad: float32 [768], P(('dp', 'tensor'))
- output_weight_grad: float32 [768, 768], P('dp', 'tensor')
- output_bias_grad: float32 [768], P(('dp', 'tensor'))
- first_gain_grad: float32 [768], P(('dp', 'tensor'))
- first_shift_grad: float32 [768], P(('dp', 'tensor'))
- up_weight_grad: float32 [768, 3072], P('dp', 'tensor')
- up_bias_grad: float32 [3072], P(('dp', 'tensor'))
- down_weight_grad: float32 [768, 3072], P('dp', 'tensor')
- down_bias_grad: float32 [768], P(('dp', 'tensor'))
- second_gain_grad: float32 [768], P(('dp', 'tensor'))
- second_shift_grad: float32 [768], P(('dp', 'tensor'))
The draws below stay inside these ranges and needn't reach their ends.
Inputs may be any that keep to these rules, and one draw needn't show every extreme that they name: `lengths`: the longest sequence has exactly 1024 tokens. A permutation: sequence s is processed in slot dealing[s], and slot q belongs to data index q // 2.
All inputs are finite; a program needn't handle non-finite values.
Results may differ from the reference program's by a relative error of at most 0.022.
Values may be sent and summed in bfloat16 or wider, within the bound.
A program may use at most 128 MiB of HBM per device.

```python
import math
import jax
import jax.numpy as jnp
import numpy as np
from jax import lax

D = 768
HEADS = 12
HD = 64
FF = 3072
L = 1024
SEQ_DEV = 2
NSEQ = 16
PB = 32
N_DP = 8
N_TENSOR = 4


def levels(own_key, extent, shards, smallest, high):
    level, own = 1.0, jax.random.fold_in(own_key, 6)
    for dim, parts in shards:
        draws = jnp.exp(jax.random.uniform(jax.random.fold_in(own, dim), (parts,), jnp.float32, smallest / len(shards), high / len(shards)))
        level = level * jnp.repeat(draws, extent[dim] // parts).reshape([-1 if axis == dim else 1 for axis in range(len(extent))])
    return level


def length_profile(number_of, total, limit, slope):
    weights = [(1 << 20) // math.isqrt(rank ** slope) + 1 for rank in range(2, number_of + 1)]
    spare, given = total - limit - (number_of - 1), [1] * (number_of - 1)
    while spare > 0:
        movable = [i for i in range(number_of - 1) if given[i] < limit]
        pool, left = sum([weights[i] for i in movable]), spare
        for i in movable:
            addition = min(limit - given[i], max(1, left * weights[i] // pool), spare)
            given[i] = given[i] + addition
            spare = spare - addition
    return np.array([limit] + given)


def ragged_sizes(key, number_of, total, reach, skew):
    if number_of == 2:
        one = jax.random.randint(key, (), max(1, total - reach), min(reach, total - 1) + 1)
        return jnp.stack([one, total - one])
    sizes = jnp.asarray(length_profile(number_of, total, reach, skew), jnp.int32)
    couples = (number_of - 1) // 2
    source_of, sink = sizes[1:1 + 2 * couples:2], sizes[2:2 + 2 * couples:2]
    margin = jnp.minimum(source_of - 1, reach - sink)
    shifted = jax.random.randint(jax.random.fold_in(key, 1), (couples,), 0, 1 << 20) % (margin + 1)
    sizes = sizes.at[1:1 + 2 * couples:2].set(source_of - shifted).at[2:2 + 2 * couples:2].set(sink + shifted)
    return sizes[jax.random.permutation(jax.random.fold_in(key, 2), number_of)]


def gaussian(key, shape, spread, reach, cuts=(), held_as=jnp.bfloat16):
    entries = spread * jax.random.normal(key, shape, jnp.float32)
    if cuts:
        entries = entries * levels(key, shape, cuts, -0.22, 0.18)
    return jnp.clip(entries, -reach, reach).astype(held_as)


def setup_inputs(seed: int = 0) -> dict:
    seeds = jax.random.split(jax.random.key(seed), 18)
    tokens = gaussian(seeds[0], (L, NSEQ, D), 1.0, 6.0, ((0, 32),))
    lengths = ragged_sizes(seeds[1], NSEQ, NSEQ * L * 3 // 4, L, 2).astype(jnp.int32)
    dealing = jax.random.permutation(seeds[2], NSEQ).astype(jnp.int32)
    project_weight = gaussian(seeds[3], (D, 3 * D), D ** -0.5, 0.21875, ((0, 8), (1, 4)))
    query_projection_bias = gaussian(seeds[4], (D,), 0.5, 3.0, (), jnp.float32)
    value_projection_bias = gaussian(seeds[5], (D,), 0.5, 3.0, (), jnp.float32)
    attention_output_weight = gaussian(seeds[6], (D, D), (D // 256) ** -0.5, 3.5, ((0, 8), (1, 4)))
    attention_output_bias = gaussian(seeds[7], (D,), 0.5, 3.0, (), jnp.float32)
    first_gain = jnp.clip(1.0 + 0.1 * jax.random.normal(seeds[8], (D,), jnp.float32), 0.5, 1.5)
    first_shift = gaussian(seeds[9], (D,), 0.5, 3.0, (), jnp.float32)
    feed_input_weight = gaussian(seeds[10], (D, FF), D ** -0.5, 0.21875, ((0, 8), (1, 4)))
    feed_input_bias = gaussian(seeds[11], (FF,), 0.5, 3.0, (), jnp.float32)
    feed_output_weight = gaussian(seeds[12], (D, FF), FF ** -0.5, 0.109375, ((0, 8), (1, 4)))
    feed_output_bias = gaussian(seeds[13], (D,), 0.5, 3.0, (), jnp.float32)
    second_gain = jnp.clip(1.0 + 0.1 * jax.random.normal(seeds[14], (D,), jnp.float32), 0.5, 1.5)
    second_shift = gaussian(seeds[15], (D,), 0.5, 3.0, (), jnp.float32)
    output_grad = gaussian(seeds[16], (L, NSEQ, D), 1.0, 6.0, ((0, 32),))
    return {"tokens": tokens, "lengths": lengths, "dealing": dealing, "project_weight": project_weight, "query_projection_bias": query_projection_bias, "value_projection_bias": value_projection_bias, "attention_output_weight": attention_output_weight, "attention_output_bias": attention_output_bias, "first_gain": first_gain, "first_shift": first_shift, "feed_input_weight": feed_input_weight, "feed_input_bias": feed_input_bias, "feed_output_weight": feed_output_weight, "feed_output_bias": feed_output_bias, "second_gain": second_gain, "second_shift": second_shift, "output_grad": output_grad}


@jax.custom_vjp
def reduced_rows(v):
    return lax.optimization_barrier(v.astype(jnp.bfloat16)).astype(jnp.float32)

@jax.custom_vjp
def reduced_backward(v):
    return v

def low_keep(v):
    return (reduced_rows(v), None)

def low_pass(kept, grad):
    return (grad,)

def back_keep(v):
    return (v, None)

def back_low(kept, grad):
    return (reduced_rows(grad),)
reduced_rows.defvjp(low_keep, low_pass)
reduced_backward.defvjp(back_keep, back_low)
EXACT_MATMUL = lax.Precision.HIGHEST
EPSILON = 1e-12
MASKED = -1e+30

def normalize(value, gain, shift):
    centred = value - lax.optimization_barrier(jnp.mean(value, axis=-1, keepdims=True))
    inverse = lax.rsqrt(lax.optimization_barrier(jnp.mean(centred * centred, axis=-1, keepdims=True)) + EPSILON)
    return centred * inverse * gain + shift

def attend(query_matrix_rows, key_matrix_rows, value_matrix_rows, length):
    queries = query_matrix_rows.reshape(L, HEADS, HD)
    keyset = key_matrix_rows.reshape(L, HEADS, HD)
    values = value_matrix_rows.reshape(L, HEADS, HD)
    scores = reduced_backward(jnp.einsum('qhe,khe->hqk', queries, keyset, precision=EXACT_MATMUL) * HD ** (-0.5))
    key_valid = jnp.arange(L) < length
    scores = jnp.where(key_valid[None, None, :], scores, MASKED)
    row_max = lax.optimization_barrier(jnp.max(scores, axis=-1, keepdims=True))
    exponent = jnp.exp(scores - row_max)
    weights = exponent / lax.optimization_barrier(jnp.sum(exponent, axis=-1, keepdims=True))
    mixed_heads = jnp.einsum('hqk,khe->qhe', reduced_rows(weights), values, precision=EXACT_MATMUL)
    return reduced_rows(reduced_backward(mixed_heads.reshape(L, D)))

def block_forward(input_rows, lengths_here, params):
    project_weight, query_projection_bias, value_projection_bias, attention_output_weight, attention_output_bias, first_gain, first_shift, feed_input_weight, feed_input_bias, feed_output_weight, feed_output_bias, second_gain, second_shift = params
    sections = project_weight.reshape(D, N_TENSOR, 3, D // N_TENSOR)
    query_projection_weight = sections[:, :, 0, :].reshape(D, D)
    key_projection_weight = sections[:, :, 1, :].reshape(D, D)
    value_projection_weight = sections[:, :, 2, :].reshape(D, D)
    query_matrix_rows = reduced_rows(reduced_backward(jnp.einsum('mow,wf->mof', input_rows, query_projection_weight, precision=EXACT_MATMUL) + query_projection_bias))
    key_matrix_rows = reduced_rows(reduced_backward(jnp.einsum('mow,wf->mof', input_rows, key_projection_weight, precision=EXACT_MATMUL)))
    value_matrix_rows = reduced_rows(reduced_backward(jnp.einsum('mow,wf->mof', input_rows, value_projection_weight, precision=EXACT_MATMUL) + value_projection_bias))
    mixed_output = lax.map(lambda item: jax.checkpoint(attend)(*item), (query_matrix_rows, key_matrix_rows, value_matrix_rows, lengths_here))
    branch_output = reduced_backward(jnp.einsum('awx,bx->awb', mixed_output, attention_output_weight, precision=EXACT_MATMUL)) + attention_output_bias
    first_normed_rows = normalize(input_rows + branch_output, first_gain, first_shift)
    before_gelu = reduced_backward(jnp.einsum('kit,tj->kij', reduced_rows(first_normed_rows), feed_input_weight, precision=EXACT_MATMUL) + feed_input_bias)
    hidden_rows = reduced_rows(jax.nn.gelu(before_gelu, approximate=False))
    feed_output = reduced_backward(jnp.einsum('nhy,uy->nhu', hidden_rows, feed_output_weight, precision=EXACT_MATMUL)) + feed_output_bias
    return normalize(first_normed_rows + feed_output, second_gain, second_shift)

def reference(tokens, lengths, dealing, project_weight, query_projection_bias, value_projection_bias, attention_output_weight, attention_output_bias, first_gain, first_shift, feed_input_weight, feed_input_bias, feed_output_weight, feed_output_bias, second_gain, second_shift, output_grad):
    params = tuple((item.astype(jnp.float32) for item in (project_weight, query_projection_bias, value_projection_bias, attention_output_weight, attention_output_bias, first_gain, first_shift, feed_input_weight, feed_input_bias, feed_output_weight, feed_output_bias, second_gain, second_shift)))
    input_rows = jnp.swapaxes(tokens.astype(jnp.float32), 0, 1)
    length_rows = lengths.reshape(NSEQ // SEQ_DEV, SEQ_DEV)

    def forward(input_rows, params):
        grouped = input_rows.reshape(NSEQ // SEQ_DEV, SEQ_DEV, L, D)

        def scan_step(carry, item):
            return (carry, jax.checkpoint(block_forward)(item[0], item[1], params))
        unused, results = lax.scan(scan_step, jnp.zeros((), jnp.float32), (grouped, length_rows))
        return results.reshape(NSEQ, L, D)
    result, pullback = jax.vjp(forward, input_rows, params)
    cotangent = jnp.swapaxes(output_grad.astype(jnp.float32), 0, 1)
    inputs_grad, grads = pullback(cotangent)
    dealt = jnp.zeros_like(result).at[dealing].set(result)
    arranged = dealt.reshape(NSEQ, N_DP, N_TENSOR, PB, D).transpose(2, 1, 3, 0, 4).reshape(L, NSEQ, D)
    tokens_grad = jnp.swapaxes(inputs_grad, 0, 1).astype(jnp.bfloat16)
    return (arranged.astype(jnp.bfloat16), tokens_grad, grads[0], grads[1], grads[2], grads[3], grads[4], grads[5], grads[6], grads[7], grads[8], grads[9], grads[10], grads[11], grads[12])
```

```python
from functools import partial

import jax
import jax.numpy as jnp
from jax import lax
from jax.sharding import PartitionSpec as P

HD = 64


EPSILON = 1e-12
MASKED = -1e30


def norm_forward(value, gain, shift):
    centred = value - jnp.mean(value, axis=-1, keepdims=True)
    inverse = lax.rsqrt(jnp.mean(centred * centred, axis=-1, keepdims=True) + EPSILON)
    normed = centred * inverse
    return (normed * gain + shift, normed, inverse)


def norm_backward(upstream, normed, inverse, gain):
    scaled = upstream * gain
    first_mean = jnp.mean(scaled, axis=-1, keepdims=True)
    second_mean = jnp.mean(scaled * normed, axis=-1, keepdims=True)
    return inverse * (scaled - first_mean - normed * second_mean)


def spread_block(values, block_index, length_total):
    blank = jnp.zeros((length_total,), jnp.float32)
    return lax.dynamic_update_slice_in_dim(blank, values, block_index * values.shape[0], 0)


def gather_rows(block):
    return lax.all_gather(block, "tensor", axis=0, tiled=True)


def scatter_rows(partial_sum):
    return lax.psum_scatter(
        partial_sum.astype(jnp.bfloat16), "tensor", scatter_dimension=0, tiled=True
    ).astype(jnp.float32)


def scatter_weight(grad):
    return lax.psum_scatter(
        grad.astype(jnp.bfloat16), "dp", scatter_dimension=0, tiled=True
    ).astype(jnp.float32)


def on_device(
    tokens,
    lengths,
    dealing,
    project_weight,
    query_projection_bias,
    value_projection_bias,
    attention_output_weight,
    attention_output_bias,
    first_gain,
    first_shift,
    feed_input_weight,
    feed_input_bias,
    feed_output_weight,
    feed_output_bias,
    second_gain,
    second_shift,
    output_grad,
):
    n_data = lax.axis_size("dp")
    n_tensor = lax.axis_size("tensor")
    n_all = n_data * n_tensor
    data_index = lax.axis_index("dp")
    tensor_index = lax.axis_index("tensor")
    seq_total = dealing.shape[0]
    seq_here = seq_total // n_data
    piece_rows = tokens.shape[0]
    local_rows = piece_rows * n_data
    seq_rows = local_rows * n_tensor
    width = tokens.shape[2]
    head_cols = attention_output_weight.shape[1]
    heads_here = head_cols // HD
    hidden_cols = feed_input_weight.shape[1]
    score_scale = HD ** (-0.5)

    slot_ids = jnp.arange(seq_total, dtype=jnp.int32)
    placing = (dealing[None, :] == slot_ids[:, None]).astype(jnp.bfloat16)
    send_tokens = jnp.einsum(
        "qs,psd->pqd", placing, tokens, preferred_element_type=jnp.float32
    ).astype(jnp.bfloat16)
    send_grad = jnp.einsum(
        "qs,psd->pqd", placing, output_grad, preferred_element_type=jnp.float32
    ).astype(jnp.bfloat16)
    tokens_here = lax.all_to_all(send_tokens, "dp", split_axis=1, concat_axis=0, tiled=True)
    cotangent_here = lax.all_to_all(send_grad, "dp", split_axis=1, concat_axis=0, tiled=True)

    my_slots = data_index * seq_here + jnp.arange(seq_here, dtype=jnp.int32)
    mine = dealing[None, :] == my_slots[:, None]
    seq_length = jnp.sum(jnp.where(mine, lengths[None, :], 0), axis=1)
    row_ids = jnp.arange(seq_rows, dtype=jnp.int32)
    owner_rows = row_ids // local_rows
    inner_rows = row_ids % local_rows
    position = (
        inner_rows // piece_rows * n_tensor + owner_rows
    ) * piece_rows + inner_rows % piece_rows
    key_valid = position[None, :] < seq_length[:, None]

    project_full = lax.all_gather(project_weight, "dp", axis=0, tiled=True)
    output_full = lax.all_gather(attention_output_weight, "dp", axis=0, tiled=True)
    up_full = lax.all_gather(feed_input_weight, "dp", axis=0, tiled=True)
    down_full = lax.all_gather(feed_output_weight, "dp", axis=0, tiled=True)

    query_part = lax.dynamic_slice_in_dim(
        query_projection_bias, tensor_index * head_cols, head_cols
    )
    value_part = lax.dynamic_slice_in_dim(
        value_projection_bias, tensor_index * head_cols, head_cols
    )
    project_bias = jnp.concatenate([query_part, jnp.zeros_like(query_part), value_part])
    up_bias_here = lax.dynamic_slice_in_dim(
        feed_input_bias, tensor_index * hidden_cols, hidden_cols
    )

    def split_heads(qkv_block):
        query_rows = qkv_block[:, :head_cols].reshape(seq_rows, heads_here, HD)
        key_rows = qkv_block[:, head_cols : 2 * head_cols].reshape(seq_rows, heads_here, HD)
        value_rows = qkv_block[:, 2 * head_cols :].reshape(seq_rows, heads_here, HD)
        return (query_rows, key_rows, value_rows)

    def masked_scores(query_rows, key_rows, valid_keys):
        raw_scores = (
            jnp.einsum("qhe,khe->hqk", query_rows, key_rows, preferred_element_type=jnp.float32)
            * score_scale
        )
        return jnp.where(valid_keys[None, None, :], raw_scores, MASKED)

    def attend(qkv_block, valid_keys):
        query_rows, key_rows, value_rows = split_heads(qkv_block)
        scores = masked_scores(query_rows, key_rows, valid_keys)
        row_max = jnp.max(scores, axis=-1, keepdims=True)
        exponent = jnp.exp(scores - row_max)
        row_total = jnp.sum(exponent, axis=-1, keepdims=True)
        weights = (exponent / row_total).astype(jnp.bfloat16)
        mixed_heads = jnp.einsum(
            "hqk,khe->qhe", weights, value_rows, preferred_element_type=jnp.float32
        )
        return (
            mixed_heads.reshape(seq_rows, head_cols).astype(jnp.bfloat16),
            (row_max + jnp.log(row_total))[..., 0],
        )

    def attend_back(qkv_block, valid_keys, row_lse, grad_block):
        query_rows, key_rows, value_rows = split_heads(qkv_block)
        weights = jnp.exp(masked_scores(query_rows, key_rows, valid_keys) - row_lse[..., None])
        grad_heads = grad_block.reshape(seq_rows, heads_here, HD)
        grad_weights = jnp.einsum(
            "qhe,khe->hqk", grad_heads, value_rows, preferred_element_type=jnp.float32
        )
        inner_sum = jnp.sum(weights * grad_weights, axis=-1, keepdims=True)
        grad_scores = (weights * (grad_weights - inner_sum)).astype(jnp.bfloat16)
        grad_query = (
            jnp.einsum("hqk,khe->qhe", grad_scores, key_rows, preferred_element_type=jnp.float32)
            * score_scale
        )
        grad_key = (
            jnp.einsum("hqk,qhe->khe", grad_scores, query_rows, preferred_element_type=jnp.float32)
            * score_scale
        )
        grad_value = jnp.einsum(
            "hqk,qhe->khe", weights.astype(jnp.bfloat16), grad_heads,
            preferred_element_type=jnp.float32,
        )
        joined = jnp.concatenate(
            [
                grad_query.reshape(seq_rows, head_cols),
                grad_key.reshape(seq_rows, head_cols),
                grad_value.reshape(seq_rows, head_cols),
            ],
            axis=-1,
        )
        return joined.astype(jnp.bfloat16)

    gelu_exact = partial(jax.nn.gelu, approximate=False)
    seqs = range(seq_here)

    inputs_full = [gather_rows(tokens_here[:, s, :]) for s in seqs]
    projected = [
        (
            jnp.dot(inputs_full[s], project_full, preferred_element_type=jnp.float32)
            + project_bias
        ).astype(jnp.bfloat16)
        for s in seqs
    ]
    attended = [attend(projected[s], key_valid[s]) for s in seqs]
    mixed = [a[0] for a in attended]
    log_total = [a[1] for a in attended]
    branch = [
        scatter_rows(
            lax.dot_general(
                mixed[s], output_full, (((1,), (1,)), ((), ())),
                preferred_element_type=jnp.float32,
            )
        )
        for s in seqs
    ]
    first = [
        norm_forward(
            tokens_here[:, s, :].astype(jnp.float32) + branch[s] + attention_output_bias,
            first_gain,
            first_shift,
        )
        for s in seqs
    ]
    first_full = [gather_rows(first[s][0].astype(jnp.bfloat16)) for s in seqs]
    preact = [
        jnp.dot(first_full[s], up_full, preferred_element_type=jnp.float32) + up_bias_here
        for s in seqs
    ]
    gelu_pairs = [jax.vjp(gelu_exact, preact[s]) for s in seqs]
    hidden = [g[0].astype(jnp.bfloat16) for g in gelu_pairs]
    feed = [
        scatter_rows(
            lax.dot_general(
                hidden[s], down_full, (((1,), (1,)), ((), ())),
                preferred_element_type=jnp.float32,
            )
        )
        for s in seqs
    ]
    second = [
        norm_forward(first[s][0] + feed[s] + feed_output_bias, second_gain, second_shift)
        for s in seqs
    ]
    layer_output = jnp.stack([second[s][0] for s in seqs], axis=1).astype(jnp.bfloat16)

    cot = [cotangent_here[:, s, :].astype(jnp.float32) for s in seqs]
    second_gain_part = sum(jnp.sum(cot[s] * second[s][1], axis=0) for s in seqs)
    second_shift_part = sum(jnp.sum(cot[s], axis=0) for s in seqs)
    grad_second = [norm_backward(cot[s], second[s][1], second[s][2], second_gain) for s in seqs]
    down_bias_part = sum(jnp.sum(grad_second[s], axis=0) for s in seqs)
    grad_feed_full = [gather_rows(grad_second[s].astype(jnp.bfloat16)) for s in seqs]
    grad_hidden = [
        jnp.dot(grad_feed_full[s], down_full, preferred_element_type=jnp.float32) for s in seqs
    ]
    down_grad = sum(
        lax.dot_general(
            grad_feed_full[s], hidden[s], (((0,), (0,)), ((), ())),
            preferred_element_type=jnp.float32,
        )
        for s in seqs
    )
    down_shard = scatter_weight(down_grad)
    grad_preact = [gelu_pairs[s][1](grad_hidden[s])[0].astype(jnp.bfloat16) for s in seqs]
    up_grad = sum(
        lax.dot_general(
            first_full[s], grad_preact[s], (((0,), (0,)), ((), ())),
            preferred_element_type=jnp.float32,
        )
        for s in seqs
    )
    up_shard = scatter_weight(up_grad)
    up_bias_part = sum(jnp.sum(grad_preact[s], axis=0, dtype=jnp.float32) for s in seqs)
    grad_first = [
        grad_second[s]
        + scatter_rows(
            lax.dot_general(
                grad_preact[s], up_full, (((1,), (1,)), ((), ())),
                preferred_element_type=jnp.float32,
            )
        )
        for s in seqs
    ]
    first_gain_part = sum(jnp.sum(grad_first[s] * first[s][1], axis=0) for s in seqs)
    first_shift_part = sum(jnp.sum(grad_first[s], axis=0) for s in seqs)
    grad_residual = [
        norm_backward(grad_first[s], first[s][1], first[s][2], first_gain) for s in seqs
    ]
    output_bias_part = sum(jnp.sum(grad_residual[s], axis=0) for s in seqs)
    early_vectors = jnp.concatenate(
        [
            v.reshape(n_all, -1)
            for v in (
                output_bias_part,
                first_gain_part,
                first_shift_part,
                spread_block(up_bias_part, tensor_index, hidden_cols * n_tensor),
                down_bias_part,
                second_gain_part,
                second_shift_part,
            )
        ],
        axis=1,
    )
    early_reduced = lax.psum_scatter(
        early_vectors, ("dp", "tensor"), scatter_dimension=0, tiled=True
    )[0]
    branch_grad_full = [gather_rows(grad_residual[s].astype(jnp.bfloat16)) for s in seqs]
    grad_mixed = [
        jnp.dot(branch_grad_full[s], output_full, preferred_element_type=jnp.float32).astype(
            jnp.bfloat16
        )
        for s in seqs
    ]
    output_grad_weight = sum(
        lax.dot_general(
            branch_grad_full[s], mixed[s], (((0,), (0,)), ((), ())),
            preferred_element_type=jnp.float32,
        )
        for s in seqs
    )
    output_shard = scatter_weight(output_grad_weight)
    grad_projected = [
        attend_back(projected[s], key_valid[s], log_total[s], grad_mixed[s]) for s in seqs
    ]
    project_grad = sum(
        lax.dot_general(
            inputs_full[s], grad_projected[s], (((0,), (0,)), ((), ())),
            preferred_element_type=jnp.float32,
        )
        for s in seqs
    )
    project_shard = scatter_weight(project_grad)
    bias_sums = sum(jnp.sum(grad_projected[s], axis=0, dtype=jnp.float32) for s in seqs)
    late_vectors = jnp.concatenate(
        [
            spread_block(bias_sums[:head_cols], tensor_index, width).reshape(n_all, -1),
            spread_block(bias_sums[2 * head_cols :], tensor_index, width).reshape(n_all, -1),
        ],
        axis=1,
    )
    late_reduced = lax.psum_scatter(
        late_vectors, ("dp", "tensor"), scatter_dimension=0, tiled=True
    )[0]
    grad_inputs = [
        grad_residual[s]
        + scatter_rows(
            lax.dot_general(
                grad_projected[s], project_full, (((1,), (1,)), ((), ())),
                preferred_element_type=jnp.float32,
            )
        )
        for s in seqs
    ]
    grad_here = jnp.stack(grad_inputs, axis=1).astype(jnp.bfloat16)
    returned = lax.all_to_all(grad_here, "dp", split_axis=0, concat_axis=1, tiled=True)
    tokens_grad = jnp.einsum(
        "qs,pqd->psd", placing, returned, preferred_element_type=jnp.float32
    ).astype(jnp.bfloat16)

    vec_block = width // n_all
    early_split = [vec_block] * 3 + [hidden_cols * n_tensor // n_all] + [vec_block] * 3
    offsets = [sum(early_split[:k]) for k in range(len(early_split) + 1)]
    early = [early_reduced[offsets[k] : offsets[k + 1]] for k in range(len(early_split))]
    late = [late_reduced[:vec_block], late_reduced[vec_block:]]
    return (
        layer_output,
        tokens_grad,
        project_shard,
        late[0],
        late[1],
        output_shard,
        early[0],
        early[1],
        early[2],
        up_shard,
        early[3],
        down_shard,
        early[4],
        early[5],
        early[6],
    )


def solution(mesh):
    in_specs = (
        P(("dp", "tensor"), None, None),
        P(),
        P(),
        P("dp", "tensor"),
        P(),
        P(),
        P("dp", "tensor"),
        P(),
        P(),
        P(),
        P("dp", "tensor"),
        P(),
        P("dp", "tensor"),
        P(),
        P(),
        P(),
        P(("dp", "tensor"), None, None),
    )
    out_specs = (
        P("tensor", "dp", None),
        P(("dp", "tensor"), None, None),
        P("dp", "tensor"),
        P(("dp", "tensor")),
        P(("dp", "tensor")),
        P("dp", "tensor"),
        P(("dp", "tensor")),
        P(("dp", "tensor")),
        P(("dp", "tensor")),
        P("dp", "tensor"),
        P(("dp", "tensor")),
        P("dp", "tensor"),
        P(("dp", "tensor")),
        P(("dp", "tensor")),
        P(("dp", "tensor")),
    )
    return jax.shard_map(
        on_device, mesh=mesh, in_specs=in_specs, out_specs=out_specs, check_vma=False
    )
```

```python
from functools import partial

import jax
import jax.numpy as jnp
from jax import lax
from jax.sharding import PartitionSpec as P

HD = 64


EPSILON = 1e-12
MASKED = -1e30


def norm_forward(value, gain, shift):
    centred = value - jnp.mean(value, axis=-1, keepdims=True)
    inverse = lax.rsqrt(jnp.mean(centred * centred, axis=-1, keepdims=True) + EPSILON)
    normed = centred * inverse
    return (normed * gain + shift, normed, inverse)


def norm_backward(upstream, normed, inverse, gain):
    scaled = upstream * gain
    first_mean = jnp.mean(scaled, axis=-1, keepdims=True)
    second_mean = jnp.mean(scaled * normed, axis=-1, keepdims=True)
    return inverse * (scaled - first_mean - normed * second_mean)


def dot_nt(a, b):
    return lax.dot_general(a, b, (((1,), (1,)), ((), ())), preferred_element_type=jnp.float32)


def dot_tn(a, b):
    return lax.dot_general(a, b, (((0,), (0,)), ((), ())), preferred_element_type=jnp.float32)


def dot_nn(a, b):
    return jnp.dot(a, b, preferred_element_type=jnp.float32)


def on_device(
    tokens,
    lengths,
    dealing,
    project_weight,
    query_projection_bias,
    value_projection_bias,
    attention_output_weight,
    attention_output_bias,
    first_gain,
    first_shift,
    feed_input_weight,
    feed_input_bias,
    feed_output_weight,
    feed_output_bias,
    second_gain,
    second_shift,
    output_grad,
):
    n_data = lax.axis_size("dp")
    n_tensor = lax.axis_size("tensor")
    n_all = n_data * n_tensor
    data_index = lax.axis_index("dp")
    tensor_index = lax.axis_index("tensor")
    seq_total = dealing.shape[0]
    seq_here = seq_total // n_data
    assert n_tensor == 4 and seq_here == 2
    piece_rows = tokens.shape[0]
    block_rows = piece_rows * n_data
    seq_rows = block_rows * n_tensor
    half_rows = seq_rows // 2
    width = tokens.shape[2]
    head_cols = attention_output_weight.shape[1]
    heads_here = head_cols // HD
    hidden_cols = feed_input_weight.shape[1]
    project_cols = project_weight.shape[1]
    score_scale = HD ** (-0.5)

    chip_side = tensor_index // 2
    core = tensor_index % 2
    partner_slice = tensor_index ^ 2
    across_chips = [(k, k ^ 2) for k in range(n_tensor)]
    across_cores = [(k, k ^ 1) for k in range(n_tensor)]

    def to_chip_partner(value):
        return lax.ppermute(value, "tensor", across_chips)

    def to_core_partner(value):
        return lax.ppermute(value, "tensor", across_cores)

    def gather_cores(mine):
        low = mine.astype(jnp.bfloat16)
        return jnp.concatenate([low, to_core_partner(low)], axis=0)

    def scatter_cores(partial_sum):
        sent = to_core_partner(partial_sum[half_rows:].astype(jnp.bfloat16))
        return partial_sum[:half_rows] + sent.astype(jnp.float32)

    slot_ids = jnp.arange(seq_total, dtype=jnp.int32)
    placing = (dealing[None, :] == slot_ids[:, None]).astype(jnp.bfloat16)
    both = jnp.concatenate([tokens, output_grad], axis=-1)
    send_both = jnp.einsum(
        "qs,psd->pqd", placing, both, preferred_element_type=jnp.float32
    ).astype(jnp.bfloat16)
    here = lax.all_to_all(send_both, "dp", split_axis=1, concat_axis=0, tiled=True)
    slot_mine = lax.dynamic_index_in_dim(here, chip_side, axis=1, keepdims=False)
    slot_other = lax.dynamic_index_in_dim(here, 1 - chip_side, axis=1, keepdims=False)
    mine_both = jnp.concatenate([slot_mine, to_chip_partner(slot_other)], axis=0)
    inputs_mine = mine_both[:, :width]
    cot_mine = mine_both[:, width:]
    inputs_full = jnp.concatenate([inputs_mine, to_core_partner(inputs_mine)], axis=0)

    my_slot = data_index * seq_here + chip_side
    seq_length = jnp.sum(jnp.where(dealing == my_slot, lengths, 0))
    blocks = jnp.stack(
        [
            tensor_index,
            partner_slice,
            tensor_index ^ 1,
            partner_slice ^ 1,
        ]
    )
    row_ids = jnp.arange(seq_rows, dtype=jnp.int32)
    owner = blocks[row_ids // block_rows]
    inner = row_ids % block_rows
    position = (inner // piece_rows * n_tensor + owner) * piece_rows + inner % piece_rows
    key_valid = position < seq_length

    attn_w = jnp.concatenate([project_weight, attention_output_weight], axis=1)
    feed_w = jnp.concatenate([feed_input_weight, feed_output_weight], axis=1)
    attn_own = lax.all_gather(attn_w, "dp", axis=0, tiled=True)
    feed_own = lax.all_gather(feed_w, "dp", axis=0, tiled=True)
    attn_part = to_chip_partner(attn_own)
    feed_part = to_chip_partner(feed_own)
    slices = (tensor_index, partner_slice)
    attn_sets = (attn_own, attn_part)
    feed_sets = (feed_own, feed_part)
    project_ws = [a[:, :project_cols] for a in attn_sets]
    output_ws = [a[:, project_cols:] for a in attn_sets]
    up_ws = [f[:, :hidden_cols] for f in feed_sets]
    down_ws = [f[:, hidden_cols:] for f in feed_sets]

    def project_bias(k):
        query_part = lax.dynamic_slice_in_dim(query_projection_bias, k * head_cols, head_cols)
        value_part = lax.dynamic_slice_in_dim(value_projection_bias, k * head_cols, head_cols)
        return jnp.concatenate([query_part, jnp.zeros_like(query_part), value_part])

    project_biases = [project_bias(k) for k in slices]
    up_biases = [
        lax.dynamic_slice_in_dim(feed_input_bias, k * hidden_cols, hidden_cols) for k in slices
    ]

    def split_heads(qkv_block):
        query_rows = qkv_block[:, :head_cols].reshape(seq_rows, heads_here, HD)
        key_rows = qkv_block[:, head_cols : 2 * head_cols].reshape(seq_rows, heads_here, HD)
        value_rows = qkv_block[:, 2 * head_cols :].reshape(seq_rows, heads_here, HD)
        return (query_rows, key_rows, value_rows)

    def masked_scores(query_rows, key_rows):
        raw_scores = (
            jnp.einsum("qhe,khe->hqk", query_rows, key_rows, preferred_element_type=jnp.float32)
            * score_scale
        )
        return jnp.where(key_valid[None, None, :], raw_scores, MASKED)

    def attend(qkv_block):
        query_rows, key_rows, value_rows = split_heads(qkv_block)
        scores = masked_scores(query_rows, key_rows)
        row_max = jnp.max(scores, axis=-1, keepdims=True)
        exponent = jnp.exp(scores - row_max)
        row_total = jnp.sum(exponent, axis=-1, keepdims=True)
        weights = (exponent / row_total).astype(jnp.bfloat16)
        mixed_heads = jnp.einsum(
            "hqk,khe->qhe", weights, value_rows, preferred_element_type=jnp.float32
        )
        return (
            mixed_heads.reshape(seq_rows, head_cols).astype(jnp.bfloat16),
            (row_max + jnp.log(row_total))[..., 0],
        )

    def attend_back(qkv_block, row_lse, grad_block):
        query_rows, key_rows, value_rows = split_heads(qkv_block)
        weights = jnp.exp(masked_scores(query_rows, key_rows) - row_lse[..., None])
        grad_heads = grad_block.reshape(seq_rows, heads_here, HD)
        grad_weights = jnp.einsum(
            "qhe,khe->hqk", grad_heads, value_rows, preferred_element_type=jnp.float32
        )
        inner_sum = jnp.sum(weights * grad_weights, axis=-1, keepdims=True)
        grad_scores = (weights * (grad_weights - inner_sum)).astype(jnp.bfloat16)
        grad_query = (
            jnp.einsum("hqk,khe->qhe", grad_scores, key_rows, preferred_element_type=jnp.float32)
            * score_scale
        )
        grad_key = (
            jnp.einsum("hqk,qhe->khe", grad_scores, query_rows, preferred_element_type=jnp.float32)
            * score_scale
        )
        grad_value = jnp.einsum(
            "hqk,qhe->khe", weights.astype(jnp.bfloat16), grad_heads,
            preferred_element_type=jnp.float32,
        )
        joined = jnp.concatenate(
            [
                grad_query.reshape(seq_rows, head_cols),
                grad_key.reshape(seq_rows, head_cols),
                grad_value.reshape(seq_rows, head_cols),
            ],
            axis=-1,
        )
        return joined.astype(jnp.bfloat16)

    gelu_exact = partial(jax.nn.gelu, approximate=False)
    groups = range(2)

    projected = [
        (dot_nn(inputs_full, project_ws[g]) + project_biases[g]).astype(jnp.bfloat16)
        for g in groups
    ]
    attended = [attend(projected[g]) for g in groups]
    mixed = [a[0] for a in attended]
    log_total = [a[1] for a in attended]
    branch = scatter_cores(sum(dot_nt(mixed[g], output_ws[g]) for g in groups))
    first, normed_first, inverse_first = norm_forward(
        inputs_mine.astype(jnp.float32) + branch + attention_output_bias, first_gain, first_shift
    )
    first_full = gather_cores(first)
    preact = [dot_nn(first_full, up_ws[g]) + up_biases[g] for g in groups]
    gelu_pairs = [jax.vjp(gelu_exact, preact[g]) for g in groups]
    hidden = [p[0].astype(jnp.bfloat16) for p in gelu_pairs]
    feed = scatter_cores(sum(dot_nt(hidden[g], down_ws[g]) for g in groups))
    second, normed_second, inverse_second = norm_forward(
        first + feed + feed_output_bias, second_gain, second_shift
    )
    out_mine = second.astype(jnp.bfloat16)
    out_other = to_chip_partner(out_mine[block_rows:])
    out_own = out_mine[:block_rows]
    on_left = chip_side == 0
    layer_output = jnp.stack(
        [jnp.where(on_left, out_own, out_other), jnp.where(on_left, out_other, out_own)], axis=1
    )

    cot = cot_mine.astype(jnp.float32)
    second_gain_part = jnp.sum(cot * normed_second, axis=0)
    second_shift_part = jnp.sum(cot, axis=0)
    grad_second = norm_backward(cot, normed_second, inverse_second, second_gain)
    down_bias_part = jnp.sum(grad_second, axis=0)
    grad_feed_full = gather_cores(grad_second)
    grad_hidden = [dot_nn(grad_feed_full, down_ws[g]) for g in groups]
    down_grads = [dot_tn(grad_feed_full, hidden[g]) for g in groups]
    grad_preact = [gelu_pairs[g][1](grad_hidden[g])[0].astype(jnp.bfloat16) for g in groups]
    up_grads = [dot_tn(first_full, grad_preact[g]) for g in groups]
    up_bias_sums = [jnp.sum(grad_preact[g], axis=0, dtype=jnp.float32) for g in groups]
    grad_first = grad_second + scatter_cores(sum(dot_nt(grad_preact[g], up_ws[g]) for g in groups))
    first_gain_part = jnp.sum(grad_first * normed_first, axis=0)
    first_shift_part = jnp.sum(grad_first, axis=0)
    grad_residual = norm_backward(grad_first, normed_first, inverse_first, first_gain)
    output_bias_part = jnp.sum(grad_residual, axis=0)
    branch_grad_full = gather_cores(grad_residual)
    grad_mixed = [dot_nn(branch_grad_full, output_ws[g]).astype(jnp.bfloat16) for g in groups]
    output_grads = [dot_tn(branch_grad_full, mixed[g]) for g in groups]
    grad_projected = [attend_back(projected[g], log_total[g], grad_mixed[g]) for g in groups]
    project_grads = [dot_tn(inputs_full, grad_projected[g]) for g in groups]
    qkv_bias_sums = [jnp.sum(grad_projected[g], axis=0, dtype=jnp.float32) for g in groups]
    grad_inputs = grad_residual + scatter_cores(
        sum(dot_nt(grad_projected[g], project_ws[g]) for g in groups)
    )

    def reduce_weights(own_parts, partner_parts):
        own = jnp.concatenate(own_parts, axis=1)
        sent = to_chip_partner(jnp.concatenate(partner_parts, axis=1).astype(jnp.bfloat16))
        total = (own + sent.astype(jnp.float32)).astype(jnp.bfloat16)
        return lax.psum_scatter(total, "dp", scatter_dimension=0, tiled=True).astype(jnp.float32)

    feed_shard = reduce_weights([up_grads[0], down_grads[0]], [up_grads[1], down_grads[1]])
    attn_shard = reduce_weights(
        [project_grads[0], output_grads[0]], [project_grads[1], output_grads[1]]
    )
    up_shard = feed_shard[:, :hidden_cols]
    down_shard = feed_shard[:, hidden_cols:]
    project_shard = attn_shard[:, :project_cols]
    output_shard = attn_shard[:, project_cols:]

    def place(parts, part_len, total_len):
        blank = jnp.zeros((total_len,), jnp.float32)
        for g in groups:
            blank = lax.dynamic_update_slice_in_dim(blank, parts[g], slices[g] * part_len, 0)
        return blank

    vectors = (
        place([q[:head_cols] for q in qkv_bias_sums], head_cols, width),
        place([q[2 * head_cols :] for q in qkv_bias_sums], head_cols, width),
        output_bias_part,
        first_gain_part,
        first_shift_part,
        place(up_bias_sums, hidden_cols, hidden_cols * n_tensor),
        down_bias_part,
        second_gain_part,
        second_shift_part,
    )
    packed = jnp.concatenate([v.reshape(n_all, -1) for v in vectors], axis=1)
    reduced = lax.psum_scatter(packed, ("dp", "tensor"), scatter_dimension=0, tiled=True)[0]
    sizes = [v.shape[0] // n_all for v in vectors]
    offsets = [sum(sizes[:k]) for k in range(len(sizes) + 1)]
    small = [reduced[offsets[k] : offsets[k + 1]] for k in range(len(sizes))]

    grad_low = grad_inputs.astype(jnp.bfloat16)
    grad_other = to_chip_partner(grad_low[block_rows:])
    grad_own = grad_low[:block_rows]
    grad_here = jnp.stack(
        [jnp.where(on_left, grad_own, grad_other), jnp.where(on_left, grad_other, grad_own)],
        axis=1,
    )
    returned = lax.all_to_all(grad_here, "dp", split_axis=0, concat_axis=1, tiled=True)
    tokens_grad = jnp.einsum(
        "qs,pqd->psd", placing, returned, preferred_element_type=jnp.float32
    ).astype(jnp.bfloat16)

    return (
        layer_output,
        tokens_grad,
        project_shard,
        small[0],
        small[1],
        output_shard,
        small[2],
        small[3],
        small[4],
        up_shard,
        small[5],
        down_shard,
        small[6],
        small[7],
        small[8],
    )


def solution(mesh):
    in_specs = (
        P(("dp", "tensor"), None, None),
        P(),
        P(),
        P("dp", "tensor"),
        P(),
        P(),
        P("dp", "tensor"),
        P(),
        P(),
        P(),
        P("dp", "tensor"),
        P(),
        P("dp", "tensor"),
        P(),
        P(),
        P(),
        P(("dp", "tensor"), None, None),
    )
    out_specs = (
        P("tensor", "dp", None),
        P(("dp", "tensor"), None, None),
        P("dp", "tensor"),
        P(("dp", "tensor")),
        P(("dp", "tensor")),
        P("dp", "tensor"),
        P(("dp", "tensor")),
        P(("dp", "tensor")),
        P(("dp", "tensor")),
        P("dp", "tensor"),
        P(("dp", "tensor")),
        P("dp", "tensor"),
        P(("dp", "tensor")),
        P(("dp", "tensor")),
        P(("dp", "tensor")),
    )
    return jax.shard_map(
        on_device, mesh=mesh, in_specs=in_specs, out_specs=out_specs, check_vma=False
    )
```

```python
from functools import partial

import jax
import jax.numpy as jnp
from jax import lax
from jax.sharding import PartitionSpec as P

HD = 64


EPSILON = 1e-12
MASKED = -1e30


def norm_forward(value, gain, shift):
    centred = value - jnp.mean(value, axis=-1, keepdims=True)
    inverse = lax.rsqrt(jnp.mean(centred * centred, axis=-1, keepdims=True) + EPSILON)
    normed = centred * inverse
    return (normed * gain + shift, normed, inverse)


def norm_backward(upstream, normed, inverse, gain):
    scaled = upstream * gain
    first_mean = jnp.mean(scaled, axis=-1, keepdims=True)
    second_mean = jnp.mean(scaled * normed, axis=-1, keepdims=True)
    return inverse * (scaled - first_mean - normed * second_mean)


def dot_nt(a, b):
    return lax.dot_general(a, b, (((1,), (1,)), ((), ())), preferred_element_type=jnp.float32)


def dot_tn(a, b):
    return lax.dot_general(a, b, (((0,), (0,)), ((), ())), preferred_element_type=jnp.float32)


def dot_nn(a, b):
    return jnp.dot(a, b, preferred_element_type=jnp.float32)


def on_device(
    tokens,
    lengths,
    dealing,
    project_weight,
    query_projection_bias,
    value_projection_bias,
    attention_output_weight,
    attention_output_bias,
    first_gain,
    first_shift,
    feed_input_weight,
    feed_input_bias,
    feed_output_weight,
    feed_output_bias,
    second_gain,
    second_shift,
    output_grad,
):
    n_data = lax.axis_size("dp")
    n_tensor = lax.axis_size("tensor")
    n_all = n_data * n_tensor
    data_index = lax.axis_index("dp")
    tensor_index = lax.axis_index("tensor")
    seq_total = dealing.shape[0]
    seq_here = seq_total // n_data
    assert n_tensor == 4 and seq_here == 2
    piece_rows = tokens.shape[0]
    block_rows = piece_rows * n_data
    seq_rows = block_rows * n_tensor
    half_rows = seq_rows // 2
    width = tokens.shape[2]
    head_cols = attention_output_weight.shape[1]
    heads_here = head_cols // HD
    hidden_cols = feed_input_weight.shape[1]
    project_cols = project_weight.shape[1]
    score_scale = HD ** (-0.5)

    chip_side = tensor_index // 2
    core = tensor_index % 2
    partner_slice = tensor_index ^ 2
    across_chips = [(k, k ^ 2) for k in range(n_tensor)]
    across_cores = [(k, k ^ 1) for k in range(n_tensor)]

    def to_chip_partner(value):
        return lax.ppermute(value, "tensor", across_chips)

    def to_core_partner(value):
        return lax.ppermute(value, "tensor", across_cores)

    def gather_dp(block):
        if n_data > 8:
            return lax.all_gather(block, "dp", axis=0, tiled=True)
        got = [block] + [
            lax.ppermute(block, "dp", [(j, (j + k) % n_data) for j in range(n_data)])
            for k in range(1, n_data)
        ]
        stacked = jnp.stack(got)
        ordered = jnp.take(stacked, (data_index - jnp.arange(n_data)) % n_data, axis=0)
        return ordered.reshape(n_data * block.shape[0], *block.shape[1:])

    def scatter_dp(total):
        if n_data > 8:
            return lax.psum_scatter(
                total.astype(jnp.bfloat16), "dp", scatter_dimension=0, tiled=True
            ).astype(jnp.float32)
        pieces = total.astype(jnp.bfloat16).reshape(n_data, -1, *total.shape[1:])
        acc = lax.dynamic_index_in_dim(total.reshape(pieces.shape), data_index, 0, keepdims=False)
        for k in range(1, n_data):
            sent = lax.dynamic_index_in_dim(pieces, (data_index + k) % n_data, 0, keepdims=False)
            acc = acc + lax.ppermute(
                sent, "dp", [(j, (j + k) % n_data) for j in range(n_data)]
            ).astype(jnp.float32)
        return acc

    def gather_cores(mine):
        low = mine.astype(jnp.bfloat16)
        return jnp.concatenate([low, to_core_partner(low)], axis=0)

    def scatter_cores(partial_sum):
        sent = to_core_partner(partial_sum[half_rows:].astype(jnp.bfloat16))
        return partial_sum[:half_rows] + sent.astype(jnp.float32)

    slot_ids = jnp.arange(seq_total, dtype=jnp.int32)
    placing = (dealing[None, :] == slot_ids[:, None]).astype(jnp.bfloat16)
    def deal(values):
        sent = jnp.einsum(
            "qs,psd->pqd", placing, values, preferred_element_type=jnp.float32
        ).astype(jnp.bfloat16)
        here = lax.all_to_all(sent, "dp", split_axis=1, concat_axis=0, tiled=True)
        slot_mine = lax.dynamic_index_in_dim(here, chip_side, axis=1, keepdims=False)
        slot_other = lax.dynamic_index_in_dim(here, 1 - chip_side, axis=1, keepdims=False)
        return jnp.concatenate([slot_mine, to_chip_partner(slot_other)], axis=0)

    inputs_mine = deal(tokens)
    cot_mine = deal(output_grad)
    inputs_full = jnp.concatenate([inputs_mine, to_core_partner(inputs_mine)], axis=0)

    my_slot = data_index * seq_here + chip_side
    seq_length = jnp.sum(jnp.where(dealing == my_slot, lengths, 0))
    blocks = jnp.stack(
        [
            tensor_index,
            partner_slice,
            tensor_index ^ 1,
            partner_slice ^ 1,
        ]
    )
    row_ids = jnp.arange(seq_rows, dtype=jnp.int32)
    owner = blocks[row_ids // block_rows]
    inner = row_ids % block_rows
    position = (inner // piece_rows * n_tensor + owner) * piece_rows + inner % piece_rows
    key_valid = position < seq_length

    attn_w = jnp.concatenate([project_weight, attention_output_weight], axis=1)
    feed_w = jnp.concatenate([feed_input_weight, feed_output_weight], axis=1)
    attn_own = gather_dp(attn_w)
    feed_own = gather_dp(feed_w)
    attn_part = to_chip_partner(attn_own)
    feed_part = to_chip_partner(feed_own)
    slices = (tensor_index, partner_slice)
    attn_sets = (attn_own, attn_part)
    feed_sets = (feed_own, feed_part)
    project_ws = [a[:, :project_cols] for a in attn_sets]
    output_ws = [a[:, project_cols:] for a in attn_sets]
    up_ws = [f[:, :hidden_cols] for f in feed_sets]
    down_ws = [f[:, hidden_cols:] for f in feed_sets]

    def project_bias(k):
        query_part = lax.dynamic_slice_in_dim(query_projection_bias, k * head_cols, head_cols)
        value_part = lax.dynamic_slice_in_dim(value_projection_bias, k * head_cols, head_cols)
        return jnp.concatenate([query_part, jnp.zeros_like(query_part), value_part])

    project_biases = [project_bias(k) for k in slices]
    up_biases = [
        lax.dynamic_slice_in_dim(feed_input_bias, k * hidden_cols, hidden_cols) for k in slices
    ]

    def split_heads(qkv_block):
        query_rows = qkv_block[:, :head_cols].reshape(seq_rows, heads_here, HD)
        key_rows = qkv_block[:, head_cols : 2 * head_cols].reshape(seq_rows, heads_here, HD)
        value_rows = qkv_block[:, 2 * head_cols :].reshape(seq_rows, heads_here, HD)
        return (query_rows, key_rows, value_rows)

    def masked_scores(query_rows, key_rows):
        raw_scores = (
            jnp.einsum("qhe,khe->hqk", query_rows, key_rows, preferred_element_type=jnp.float32)
            * score_scale
        )
        return jnp.where(key_valid[None, None, :], raw_scores, MASKED)

    def attend(qkv_block):
        query_rows, key_rows, value_rows = split_heads(qkv_block)
        scores = masked_scores(query_rows, key_rows)
        row_max = jnp.max(scores, axis=-1, keepdims=True)
        exponent = jnp.exp(scores - row_max)
        row_total = jnp.sum(exponent, axis=-1, keepdims=True)
        weights = (exponent / row_total).astype(jnp.bfloat16)
        mixed_heads = jnp.einsum(
            "hqk,khe->qhe", weights, value_rows, preferred_element_type=jnp.float32
        )
        return (
            mixed_heads.reshape(seq_rows, head_cols).astype(jnp.bfloat16),
            (row_max + jnp.log(row_total))[..., 0],
        )

    def attend_back(qkv_block, row_lse, grad_block):
        query_rows, key_rows, value_rows = split_heads(qkv_block)
        weights = jnp.exp(masked_scores(query_rows, key_rows) - row_lse[..., None])
        grad_heads = grad_block.reshape(seq_rows, heads_here, HD)
        grad_weights = jnp.einsum(
            "qhe,khe->hqk", grad_heads, value_rows, preferred_element_type=jnp.float32
        )
        inner_sum = jnp.sum(weights * grad_weights, axis=-1, keepdims=True)
        grad_scores = (weights * (grad_weights - inner_sum)).astype(jnp.bfloat16)
        grad_query = (
            jnp.einsum("hqk,khe->qhe", grad_scores, key_rows, preferred_element_type=jnp.float32)
            * score_scale
        )
        grad_key = (
            jnp.einsum("hqk,qhe->khe", grad_scores, query_rows, preferred_element_type=jnp.float32)
            * score_scale
        )
        grad_value = jnp.einsum(
            "hqk,qhe->khe", weights.astype(jnp.bfloat16), grad_heads,
            preferred_element_type=jnp.float32,
        )
        joined = jnp.concatenate(
            [
                grad_query.reshape(seq_rows, head_cols),
                grad_key.reshape(seq_rows, head_cols),
                grad_value.reshape(seq_rows, head_cols),
            ],
            axis=-1,
        )
        return joined.astype(jnp.bfloat16)

    gelu_exact = partial(jax.nn.gelu, approximate=False)
    groups = range(2)

    projected = [
        (dot_nn(inputs_full, project_ws[g]) + project_biases[g]).astype(jnp.bfloat16)
        for g in groups
    ]
    attended = [attend(projected[g]) for g in groups]
    mixed = [a[0] for a in attended]
    log_total = [a[1] for a in attended]
    branch = scatter_cores(sum(dot_nt(mixed[g], output_ws[g]) for g in groups))
    first, normed_first, inverse_first = norm_forward(
        inputs_mine.astype(jnp.float32) + branch + attention_output_bias, first_gain, first_shift
    )
    first_full = gather_cores(first)
    preact = [dot_nn(first_full, up_ws[g]) + up_biases[g] for g in groups]
    gelu_pairs = [jax.vjp(gelu_exact, preact[g]) for g in groups]
    hidden = [p[0].astype(jnp.bfloat16) for p in gelu_pairs]
    feed = scatter_cores(sum(dot_nt(hidden[g], down_ws[g]) for g in groups))
    second, normed_second, inverse_second = norm_forward(
        first + feed + feed_output_bias, second_gain, second_shift
    )
    out_mine = second.astype(jnp.bfloat16)
    out_other = to_chip_partner(out_mine[block_rows:])
    out_own = out_mine[:block_rows]
    on_left = chip_side == 0
    layer_output = jnp.stack(
        [jnp.where(on_left, out_own, out_other), jnp.where(on_left, out_other, out_own)], axis=1
    )

    cot = cot_mine.astype(jnp.float32)
    second_gain_part = jnp.sum(cot * normed_second, axis=0)
    second_shift_part = jnp.sum(cot, axis=0)
    grad_second = norm_backward(cot, normed_second, inverse_second, second_gain)
    down_bias_part = jnp.sum(grad_second, axis=0)
    grad_feed_full = gather_cores(grad_second)
    grad_hidden = [dot_nn(grad_feed_full, down_ws[g]) for g in groups]
    down_grads = [dot_tn(grad_feed_full, hidden[g]) for g in groups]
    grad_preact = [gelu_pairs[g][1](grad_hidden[g])[0].astype(jnp.bfloat16) for g in groups]
    up_grads = [dot_tn(first_full, grad_preact[g]) for g in groups]
    up_bias_sums = [jnp.sum(grad_preact[g], axis=0, dtype=jnp.float32) for g in groups]
    grad_first = grad_second + scatter_cores(sum(dot_nt(grad_preact[g], up_ws[g]) for g in groups))
    first_gain_part = jnp.sum(grad_first * normed_first, axis=0)
    first_shift_part = jnp.sum(grad_first, axis=0)
    grad_residual = norm_backward(grad_first, normed_first, inverse_first, first_gain)
    output_bias_part = jnp.sum(grad_residual, axis=0)
    branch_grad_full = gather_cores(grad_residual)
    grad_mixed = [dot_nn(branch_grad_full, output_ws[g]).astype(jnp.bfloat16) for g in groups]
    output_grads = [dot_tn(branch_grad_full, mixed[g]) for g in groups]
    grad_projected = [attend_back(projected[g], log_total[g], grad_mixed[g]) for g in groups]
    project_grads = [dot_tn(inputs_full, grad_projected[g]) for g in groups]
    qkv_bias_sums = [jnp.sum(grad_projected[g], axis=0, dtype=jnp.float32) for g in groups]
    grad_inputs = grad_residual + scatter_cores(
        sum(dot_nt(grad_projected[g], project_ws[g]) for g in groups)
    )

    def place(parts, part_len, total_len):
        blank = jnp.zeros((total_len,), jnp.float32)
        for g in groups:
            blank = lax.dynamic_update_slice_in_dim(blank, parts[g], slices[g] * part_len, 0)
        return blank

    rows_block = width // n_data
    vec_block = width // n_all

    def reduce_weights(own_parts, partner_parts, extra=None):
        own = jnp.concatenate(own_parts, axis=1)
        partner = jnp.concatenate(partner_parts, axis=1)
        if extra is not None:
            extra = extra + to_core_partner(extra)
            own = jnp.concatenate([own, extra], axis=1)
            partner = jnp.concatenate([partner, extra], axis=1)
        sent = to_chip_partner(partner.astype(jnp.bfloat16))
        return scatter_dp(own + sent.astype(jnp.float32))

    feed_shard = reduce_weights([up_grads[0], down_grads[0]], [up_grads[1], down_grads[1]])
    up_placed = place(up_bias_sums, hidden_cols, hidden_cols * n_tensor)
    up_columns = (
        up_placed.reshape(n_data, n_tensor, rows_block).transpose(0, 2, 1).reshape(width, n_tensor)
    )
    early_columns = jnp.concatenate(
        [
            jnp.stack(
                [
                    output_bias_part,
                    first_gain_part,
                    first_shift_part,
                    down_bias_part,
                    second_gain_part,
                    second_shift_part,
                ],
                axis=1,
            ),
            up_columns,
        ],
        axis=1,
    )
    output_shard_ext = reduce_weights([output_grads[0]], [output_grads[1]], early_columns)
    late_columns = jnp.stack(
        [
            place([q[:head_cols] for q in qkv_bias_sums], head_cols, width),
            place([q[2 * head_cols :] for q in qkv_bias_sums], head_cols, width),
        ],
        axis=1,
    )
    project_shard_ext = reduce_weights([project_grads[0]], [project_grads[1]], late_columns)
    up_shard = feed_shard[:, :hidden_cols]
    down_shard = feed_shard[:, hidden_cols:]
    head_out = output_shard_ext.shape[1] - early_columns.shape[1]
    output_shard = output_shard_ext[:, :head_out]
    project_shard = project_shard_ext[:, :project_cols]

    def mine_of(column):
        return lax.dynamic_slice_in_dim(column, tensor_index * vec_block, vec_block)

    early = [mine_of(output_shard_ext[:, head_out + k]) for k in range(6)]
    up_bias_shard = lax.dynamic_index_in_dim(
        output_shard_ext[:, head_out + 6 :], tensor_index, axis=1, keepdims=False
    )
    late = [mine_of(project_shard_ext[:, project_cols + k]) for k in range(2)]
    small = [
        late[0],
        late[1],
        early[0],
        early[1],
        early[2],
        up_bias_shard,
        early[3],
        early[4],
        early[5],
    ]

    grad_low = grad_inputs.astype(jnp.bfloat16)
    grad_other = to_chip_partner(grad_low[block_rows:])
    grad_own = grad_low[:block_rows]
    grad_here = jnp.stack(
        [jnp.where(on_left, grad_own, grad_other), jnp.where(on_left, grad_other, grad_own)],
        axis=1,
    )
    returned = lax.all_to_all(grad_here, "dp", split_axis=0, concat_axis=1, tiled=True)
    tokens_grad = jnp.einsum(
        "qs,pqd->psd", placing, returned, preferred_element_type=jnp.float32
    ).astype(jnp.bfloat16)

    return (
        layer_output,
        tokens_grad,
        project_shard,
        small[0],
        small[1],
        output_shard,
        small[2],
        small[3],
        small[4],
        up_shard,
        small[5],
        down_shard,
        small[6],
        small[7],
        small[8],
    )


def solution(mesh):
    in_specs = (
        P(("dp", "tensor"), None, None),
        P(),
        P(),
        P("dp", "tensor"),
        P(),
        P(),
        P("dp", "tensor"),
        P(),
        P(),
        P(),
        P("dp", "tensor"),
        P(),
        P("dp", "tensor"),
        P(),
        P(),
        P(),
        P(("dp", "tensor"), None, None),
    )
    out_specs = (
        P("tensor", "dp", None),
        P(("dp", "tensor"), None, None),
        P("dp", "tensor"),
        P(("dp", "tensor")),
        P(("dp", "tensor")),
        P("dp", "tensor"),
        P(("dp", "tensor")),
        P(("dp", "tensor")),
        P(("dp", "tensor")),
        P("dp", "tensor"),
        P(("dp", "tensor")),
        P("dp", "tensor"),
        P(("dp", "tensor")),
        P(("dp", "tensor")),
        P(("dp", "tensor")),
    )
    return jax.shard_map(
        on_device, mesh=mesh, in_specs=in_specs, out_specs=out_specs, check_vma=False
    )
```

```python
from functools import partial

import jax
import jax.numpy as jnp
from jax import lax
from jax.sharding import PartitionSpec as P

HD = 64


EPSILON = 1e-12
MASKED = -1e30


def norm_forward(value, gain, shift):
    centred = value - jnp.mean(value, axis=-1, keepdims=True)
    inverse = lax.rsqrt(jnp.mean(centred * centred, axis=-1, keepdims=True) + EPSILON)
    normed = centred * inverse
    return (normed * gain + shift, normed, inverse)


def norm_backward(upstream, normed, inverse, gain):
    scaled = upstream * gain
    first_mean = jnp.mean(scaled, axis=-1, keepdims=True)
    second_mean = jnp.mean(scaled * normed, axis=-1, keepdims=True)
    return inverse * (scaled - first_mean - normed * second_mean)


def dot_nt(a, b):
    return lax.dot_general(a, b, (((1,), (1,)), ((), ())), preferred_element_type=jnp.float32)


def dot_tn(a, b):
    return lax.dot_general(a, b, (((0,), (0,)), ((), ())), preferred_element_type=jnp.float32)


def dot_nn(a, b):
    return jnp.dot(a, b, preferred_element_type=jnp.float32)


def on_device(
    tokens,
    lengths,
    dealing,
    project_weight,
    query_projection_bias,
    value_projection_bias,
    attention_output_weight,
    attention_output_bias,
    first_gain,
    first_shift,
    feed_input_weight,
    feed_input_bias,
    feed_output_weight,
    feed_output_bias,
    second_gain,
    second_shift,
    output_grad,
):
    n_data = lax.axis_size("dp")
    n_tensor = lax.axis_size("tensor")
    n_all = n_data * n_tensor
    data_index = lax.axis_index("dp")
    tensor_index = lax.axis_index("tensor")
    seq_total = dealing.shape[0]
    seq_here = seq_total // n_data
    assert n_tensor == 4 and seq_here == 2
    piece_rows = tokens.shape[0]
    block_rows = piece_rows * n_data
    seq_rows = block_rows * n_tensor
    half_rows = seq_rows // 2
    width = tokens.shape[2]
    head_cols = attention_output_weight.shape[1]
    heads_here = head_cols // HD
    hidden_cols = feed_input_weight.shape[1]
    project_cols = project_weight.shape[1]
    score_scale = HD ** (-0.5)

    chip_side = tensor_index // 2
    core = tensor_index % 2
    partner_slice = tensor_index ^ 2
    across_chips = [(k, k ^ 2) for k in range(n_tensor)]
    across_cores = [(k, k ^ 1) for k in range(n_tensor)]

    def to_chip_partner(value):
        return lax.ppermute(value, "tensor", across_chips)

    def to_core_partner(value):
        return lax.ppermute(value, "tensor", across_cores)

    def gather_dp(block):
        return lax.all_gather(block, "dp", axis=0, tiled=True)

    def scatter_dp(total):
        return lax.psum_scatter(
            total.astype(jnp.bfloat16), "dp", scatter_dimension=0, tiled=True
        ).astype(jnp.float32)

    def gather_cores(mine):
        low = mine.astype(jnp.bfloat16)
        return jnp.concatenate([low, to_core_partner(low)], axis=0)

    def scatter_cores(partial_sum):
        sent = to_core_partner(partial_sum[half_rows:].astype(jnp.bfloat16))
        return partial_sum[:half_rows] + sent.astype(jnp.float32)

    slot_ids = jnp.arange(seq_total, dtype=jnp.int32)
    placing = (dealing[None, :] == slot_ids[:, None]).astype(jnp.bfloat16)
    def deal(values):
        sent = jnp.einsum(
            "qs,psd->pqd", placing, values, preferred_element_type=jnp.float32
        ).astype(jnp.bfloat16)
        here = lax.all_to_all(sent, "dp", split_axis=1, concat_axis=0, tiled=True)
        slot_mine = lax.dynamic_index_in_dim(here, chip_side, axis=1, keepdims=False)
        slot_other = lax.dynamic_index_in_dim(here, 1 - chip_side, axis=1, keepdims=False)
        return jnp.concatenate([slot_mine, to_chip_partner(slot_other)], axis=0)

    inputs_mine = deal(tokens)
    cot_mine = deal(output_grad)
    inputs_full = jnp.concatenate([inputs_mine, to_core_partner(inputs_mine)], axis=0)

    my_slot = data_index * seq_here + chip_side
    seq_length = jnp.sum(jnp.where(dealing == my_slot, lengths, 0))
    blocks = jnp.stack(
        [
            tensor_index,
            partner_slice,
            tensor_index ^ 1,
            partner_slice ^ 1,
        ]
    )
    row_ids = jnp.arange(seq_rows, dtype=jnp.int32)
    owner = blocks[row_ids // block_rows]
    inner = row_ids % block_rows
    position = (inner // piece_rows * n_tensor + owner) * piece_rows + inner % piece_rows
    key_valid = position < seq_length

    attn_w = jnp.concatenate([project_weight, attention_output_weight], axis=1)
    feed_w = jnp.concatenate([feed_input_weight, feed_output_weight], axis=1)
    attn_own = gather_dp(attn_w)
    feed_own = gather_dp(feed_w)
    attn_part = to_chip_partner(attn_own)
    feed_part = to_chip_partner(feed_own)
    slices = (tensor_index, partner_slice)
    attn_sets = (attn_own, attn_part)
    feed_sets = (feed_own, feed_part)
    project_ws = [a[:, :project_cols] for a in attn_sets]
    output_ws = [a[:, project_cols:] for a in attn_sets]
    up_ws = [f[:, :hidden_cols] for f in feed_sets]
    down_ws = [f[:, hidden_cols:] for f in feed_sets]

    def project_bias(k):
        query_part = lax.dynamic_slice_in_dim(query_projection_bias, k * head_cols, head_cols)
        value_part = lax.dynamic_slice_in_dim(value_projection_bias, k * head_cols, head_cols)
        return jnp.concatenate([query_part, jnp.zeros_like(query_part), value_part])

    project_biases = [project_bias(k) for k in slices]
    up_biases = [
        lax.dynamic_slice_in_dim(feed_input_bias, k * hidden_cols, hidden_cols) for k in slices
    ]

    def split_heads(qkv_block):
        query_rows = qkv_block[:, :head_cols].reshape(seq_rows, heads_here, HD)
        key_rows = qkv_block[:, head_cols : 2 * head_cols].reshape(seq_rows, heads_here, HD)
        value_rows = qkv_block[:, 2 * head_cols :].reshape(seq_rows, heads_here, HD)
        return (query_rows, key_rows, value_rows)

    def masked_scores(query_rows, key_rows):
        raw_scores = (
            jnp.einsum("qhe,khe->hqk", query_rows, key_rows, preferred_element_type=jnp.float32)
            * score_scale
        )
        return jnp.where(key_valid[None, None, :], raw_scores, MASKED)

    def attend(qkv_block):
        query_rows, key_rows, value_rows = split_heads(qkv_block)
        scores = masked_scores(query_rows, key_rows)
        row_max = jnp.max(scores, axis=-1, keepdims=True)
        exponent = jnp.exp(scores - row_max)
        row_total = jnp.sum(exponent, axis=-1, keepdims=True)
        weights = (exponent / row_total).astype(jnp.bfloat16)
        mixed_heads = jnp.einsum(
            "hqk,khe->qhe", weights, value_rows, preferred_element_type=jnp.float32
        )
        return (
            mixed_heads.reshape(seq_rows, head_cols).astype(jnp.bfloat16),
            (row_max + jnp.log(row_total))[..., 0],
        )

    def attend_back(qkv_block, row_lse, grad_block):
        query_rows, key_rows, value_rows = split_heads(qkv_block)
        weights = jnp.exp(masked_scores(query_rows, key_rows) - row_lse[..., None])
        grad_heads = grad_block.reshape(seq_rows, heads_here, HD)
        grad_weights = jnp.einsum(
            "qhe,khe->hqk", grad_heads, value_rows, preferred_element_type=jnp.float32
        )
        inner_sum = jnp.sum(weights * grad_weights, axis=-1, keepdims=True)
        grad_scores = (weights * (grad_weights - inner_sum)).astype(jnp.bfloat16)
        grad_query = (
            jnp.einsum("hqk,khe->qhe", grad_scores, key_rows, preferred_element_type=jnp.float32)
            * score_scale
        )
        grad_key = (
            jnp.einsum("hqk,qhe->khe", grad_scores, query_rows, preferred_element_type=jnp.float32)
            * score_scale
        )
        grad_value = jnp.einsum(
            "hqk,qhe->khe", weights.astype(jnp.bfloat16), grad_heads,
            preferred_element_type=jnp.float32,
        )
        joined = jnp.concatenate(
            [
                grad_query.reshape(seq_rows, head_cols),
                grad_key.reshape(seq_rows, head_cols),
                grad_value.reshape(seq_rows, head_cols),
            ],
            axis=-1,
        )
        return joined.astype(jnp.bfloat16)

    gelu_exact = partial(jax.nn.gelu, approximate=False)
    groups = range(2)

    projected = [
        (dot_nn(inputs_full, project_ws[g]) + project_biases[g]).astype(jnp.bfloat16)
        for g in groups
    ]
    attended = [attend(projected[g]) for g in groups]
    mixed = [a[0] for a in attended]
    log_total = [a[1] for a in attended]
    branch = scatter_cores(sum(dot_nt(mixed[g], output_ws[g]) for g in groups))
    first, normed_first, inverse_first = norm_forward(
        inputs_mine.astype(jnp.float32) + branch + attention_output_bias, first_gain, first_shift
    )
    first_full = gather_cores(first)
    preact = [dot_nn(first_full, up_ws[g]) + up_biases[g] for g in groups]
    gelu_pairs = [jax.vjp(gelu_exact, preact[g]) for g in groups]
    hidden = [p[0].astype(jnp.bfloat16) for p in gelu_pairs]
    feed = scatter_cores(sum(dot_nt(hidden[g], down_ws[g]) for g in groups))
    second, normed_second, inverse_second = norm_forward(
        first + feed + feed_output_bias, second_gain, second_shift
    )
    out_mine = second.astype(jnp.bfloat16)
    out_other = to_chip_partner(out_mine[block_rows:])
    out_own = out_mine[:block_rows]
    on_left = chip_side == 0
    layer_output = jnp.stack(
        [jnp.where(on_left, out_own, out_other), jnp.where(on_left, out_other, out_own)], axis=1
    )

    cot = cot_mine.astype(jnp.float32)
    second_gain_part = jnp.sum(cot * normed_second, axis=0)
    second_shift_part = jnp.sum(cot, axis=0)
    grad_second = norm_backward(cot, normed_second, inverse_second, second_gain)
    down_bias_part = jnp.sum(grad_second, axis=0)
    grad_feed_full = gather_cores(grad_second)
    grad_hidden = [dot_nn(grad_feed_full, down_ws[g]) for g in groups]
    down_grads = [dot_tn(grad_feed_full, hidden[g]) for g in groups]
    grad_preact = [gelu_pairs[g][1](grad_hidden[g])[0].astype(jnp.bfloat16) for g in groups]
    up_grads = [dot_tn(first_full, grad_preact[g]) for g in groups]
    up_bias_sums = [jnp.sum(grad_preact[g], axis=0, dtype=jnp.float32) for g in groups]
    grad_first = grad_second + scatter_cores(sum(dot_nt(grad_preact[g], up_ws[g]) for g in groups))
    first_gain_part = jnp.sum(grad_first * normed_first, axis=0)
    first_shift_part = jnp.sum(grad_first, axis=0)
    grad_residual = norm_backward(grad_first, normed_first, inverse_first, first_gain)
    output_bias_part = jnp.sum(grad_residual, axis=0)
    branch_grad_full = gather_cores(grad_residual)
    grad_mixed = [dot_nn(branch_grad_full, output_ws[g]).astype(jnp.bfloat16) for g in groups]
    output_grads = [dot_tn(branch_grad_full, mixed[g]) for g in groups]
    grad_projected = [attend_back(projected[g], log_total[g], grad_mixed[g]) for g in groups]
    project_grads = [dot_tn(inputs_full, grad_projected[g]) for g in groups]
    qkv_bias_sums = [jnp.sum(grad_projected[g], axis=0, dtype=jnp.float32) for g in groups]
    grad_inputs = grad_residual + scatter_cores(
        sum(dot_nt(grad_projected[g], project_ws[g]) for g in groups)
    )

    def place(parts, part_len, total_len):
        blank = jnp.zeros((total_len,), jnp.float32)
        for g in groups:
            blank = lax.dynamic_update_slice_in_dim(blank, parts[g], slices[g] * part_len, 0)
        return blank

    rows_block = width // n_data
    vec_block = width // n_all

    def reduce_weights(own_parts, partner_parts, extra=None):
        own = jnp.concatenate(own_parts, axis=1)
        partner = jnp.concatenate(partner_parts, axis=1)
        if extra is not None:
            extra = extra + to_core_partner(extra)
            own = jnp.concatenate([own, extra], axis=1)
            partner = jnp.concatenate([partner, extra], axis=1)
        sent = to_chip_partner(partner.astype(jnp.bfloat16))
        return scatter_dp(own + sent.astype(jnp.float32))

    feed_shard = reduce_weights([up_grads[0], down_grads[0]], [up_grads[1], down_grads[1]])
    up_placed = place(up_bias_sums, hidden_cols, hidden_cols * n_tensor)
    up_columns = (
        up_placed.reshape(n_data, n_tensor, rows_block).transpose(0, 2, 1).reshape(width, n_tensor)
    )
    early_columns = jnp.concatenate(
        [
            jnp.stack(
                [
                    output_bias_part,
                    first_gain_part,
                    first_shift_part,
                    down_bias_part,
                    second_gain_part,
                    second_shift_part,
                ],
                axis=1,
            ),
            up_columns,
        ],
        axis=1,
    )
    late_columns = jnp.stack(
        [
            place([q[:head_cols] for q in qkv_bias_sums], head_cols, width),
            place([q[2 * head_cols :] for q in qkv_bias_sums], head_cols, width),
        ],
        axis=1,
    )
    attn_shard = reduce_weights(
        [project_grads[0], output_grads[0]],
        [project_grads[1], output_grads[1]],
        jnp.concatenate([early_columns, late_columns], axis=1),
    )
    up_shard = feed_shard[:, :hidden_cols]
    down_shard = feed_shard[:, hidden_cols:]
    head_out = project_cols + head_cols
    project_shard = attn_shard[:, :project_cols]
    output_shard = attn_shard[:, project_cols:head_out]
    late_at = head_out + early_columns.shape[1]

    def mine_of(column):
        return lax.dynamic_slice_in_dim(column, tensor_index * vec_block, vec_block)

    early = [mine_of(attn_shard[:, head_out + k]) for k in range(6)]
    up_bias_shard = lax.dynamic_index_in_dim(
        attn_shard[:, head_out + 6 : late_at], tensor_index, axis=1, keepdims=False
    )
    late = [mine_of(attn_shard[:, late_at + k]) for k in range(2)]
    small = [
        late[0],
        late[1],
        early[0],
        early[1],
        early[2],
        up_bias_shard,
        early[3],
        early[4],
        early[5],
    ]

    grad_low = grad_inputs.astype(jnp.bfloat16)
    grad_other = to_chip_partner(grad_low[block_rows:])
    grad_own = grad_low[:block_rows]
    grad_here = jnp.stack(
        [jnp.where(on_left, grad_own, grad_other), jnp.where(on_left, grad_other, grad_own)],
        axis=1,
    )
    returned = lax.all_to_all(grad_here, "dp", split_axis=0, concat_axis=1, tiled=True)
    tokens_grad = jnp.einsum(
        "qs,pqd->psd", placing, returned, preferred_element_type=jnp.float32
    ).astype(jnp.bfloat16)

    return (
        layer_output,
        tokens_grad,
        project_shard,
        small[0],
        small[1],
        output_shard,
        small[2],
        small[3],
        small[4],
        up_shard,
        small[5],
        down_shard,
        small[6],
        small[7],
        small[8],
    )


def solution(mesh):
    in_specs = (
        P(("dp", "tensor"), None, None),
        P(),
        P(),
        P("dp", "tensor"),
        P(),
        P(),
        P("dp", "tensor"),
        P(),
        P(),
        P(),
        P("dp", "tensor"),
        P(),
        P("dp", "tensor"),
        P(),
        P(),
        P(),
        P(("dp", "tensor"), None, None),
    )
    out_specs = (
        P("tensor", "dp", None),
        P(("dp", "tensor"), None, None),
        P("dp", "tensor"),
        P(("dp", "tensor")),
        P(("dp", "tensor")),
        P("dp", "tensor"),
        P(("dp", "tensor")),
        P(("dp", "tensor")),
        P(("dp", "tensor")),
        P("dp", "tensor"),
        P(("dp", "tensor")),
        P("dp", "tensor"),
        P(("dp", "tensor")),
        P(("dp", "tensor")),
        P(("dp", "tensor")),
    )
    return jax.shard_map(
        on_device, mesh=mesh, in_specs=in_specs, out_specs=out_specs, check_vma=False
    )
```

```python
from functools import partial

import jax
import jax.numpy as jnp
from jax import lax
from jax.sharding import PartitionSpec as P

HD = 64


EPSILON = 1e-12
MASKED = -1e30


def norm_forward(value, gain, shift):
    centred = value - jnp.mean(value, axis=-1, keepdims=True)
    inverse = lax.rsqrt(jnp.mean(centred * centred, axis=-1, keepdims=True) + EPSILON)
    normed = centred * inverse
    return (normed * gain + shift, normed, inverse)


def norm_backward(upstream, normed, inverse, gain):
    scaled = upstream * gain
    first_mean = jnp.mean(scaled, axis=-1, keepdims=True)
    second_mean = jnp.mean(scaled * normed, axis=-1, keepdims=True)
    return inverse * (scaled - first_mean - normed * second_mean)


def dot_nt(a, b):
    return lax.dot_general(a, b, (((1,), (1,)), ((), ())), preferred_element_type=jnp.float32)


def dot_tn(a, b):
    return lax.dot_general(a, b, (((0,), (0,)), ((), ())), preferred_element_type=jnp.float32)


def dot_nn(a, b):
    return jnp.dot(a, b, preferred_element_type=jnp.float32)


def on_device(
    tokens,
    lengths,
    dealing,
    project_weight,
    query_projection_bias,
    value_projection_bias,
    attention_output_weight,
    attention_output_bias,
    first_gain,
    first_shift,
    feed_input_weight,
    feed_input_bias,
    feed_output_weight,
    feed_output_bias,
    second_gain,
    second_shift,
    output_grad,
):
    n_data = lax.axis_size("dp")
    n_tensor = lax.axis_size("tensor")
    n_all = n_data * n_tensor
    data_index = lax.axis_index("dp")
    tensor_index = lax.axis_index("tensor")
    seq_total = dealing.shape[0]
    seq_here = seq_total // n_data
    assert n_tensor == 4 and seq_here == 2
    piece_rows = tokens.shape[0]
    block_rows = piece_rows * n_data
    seq_rows = block_rows * n_tensor
    half_rows = seq_rows // 2
    width = tokens.shape[2]
    head_cols = attention_output_weight.shape[1]
    heads_here = head_cols // HD
    hidden_cols = feed_input_weight.shape[1]
    project_cols = project_weight.shape[1]
    score_scale = HD ** (-0.5)

    chip_side = tensor_index // 2
    core = tensor_index % 2
    partner_slice = tensor_index ^ 2
    across_chips = [(k, k ^ 2) for k in range(n_tensor)]
    across_cores = [(k, k ^ 1) for k in range(n_tensor)]

    def to_chip_partner(value):
        return lax.ppermute(value, "tensor", across_chips)

    def to_core_partner(value):
        return lax.ppermute(value, "tensor", across_cores)

    def gather_dp(block):
        return lax.all_gather(block, "dp", axis=0, tiled=True)

    def scatter_dp(total):
        return lax.psum_scatter(
            total.astype(jnp.bfloat16), "dp", scatter_dimension=0, tiled=True
        ).astype(jnp.float32)

    def scatter_dp_permutes(total):
        if n_data > 8:
            return scatter_dp(total)
        pieces = total.astype(jnp.bfloat16).reshape(n_data, -1, *total.shape[1:])
        acc = lax.dynamic_index_in_dim(
            total.reshape(pieces.shape), data_index, 0, keepdims=False
        )
        for k in range(1, n_data):
            sent = lax.dynamic_index_in_dim(pieces, (data_index + k) % n_data, 0, keepdims=False)
            acc = acc + lax.ppermute(
                sent, "dp", [(j, (j + k) % n_data) for j in range(n_data)]
            ).astype(jnp.float32)
        return acc

    def gather_cores(mine):
        low = mine.astype(jnp.bfloat16)
        return jnp.concatenate([low, to_core_partner(low)], axis=0)

    def scatter_cores(partial_sum):
        sent = to_core_partner(partial_sum[half_rows:].astype(jnp.bfloat16))
        return partial_sum[:half_rows] + sent.astype(jnp.float32)

    slot_ids = jnp.arange(seq_total, dtype=jnp.int32)
    placing = (dealing[None, :] == slot_ids[:, None]).astype(jnp.bfloat16)
    def deal(values):
        sent = jnp.einsum(
            "qs,psd->pqd", placing, values, preferred_element_type=jnp.float32
        ).astype(jnp.bfloat16)
        here = lax.all_to_all(sent, "dp", split_axis=1, concat_axis=0, tiled=True)
        slot_mine = lax.dynamic_index_in_dim(here, chip_side, axis=1, keepdims=False)
        slot_other = lax.dynamic_index_in_dim(here, 1 - chip_side, axis=1, keepdims=False)
        return jnp.concatenate([slot_mine, to_chip_partner(slot_other)], axis=0)

    inputs_mine = deal(tokens)
    cot_mine = deal(output_grad)
    inputs_full = jnp.concatenate([inputs_mine, to_core_partner(inputs_mine)], axis=0)

    my_slot = data_index * seq_here + chip_side
    seq_length = jnp.sum(jnp.where(dealing == my_slot, lengths, 0))
    blocks = jnp.stack(
        [
            tensor_index,
            partner_slice,
            tensor_index ^ 1,
            partner_slice ^ 1,
        ]
    )
    row_ids = jnp.arange(seq_rows, dtype=jnp.int32)
    owner = blocks[row_ids // block_rows]
    inner = row_ids % block_rows
    position = (inner // piece_rows * n_tensor + owner) * piece_rows + inner % piece_rows
    key_valid = position < seq_length

    attn_w = jnp.concatenate([project_weight, attention_output_weight], axis=1)
    feed_w = jnp.concatenate([feed_input_weight, feed_output_weight], axis=1)
    attn_own = gather_dp(attn_w)
    feed_own = gather_dp(feed_w)
    attn_part = to_chip_partner(attn_own)
    feed_part = to_chip_partner(feed_own)
    slices = (tensor_index, partner_slice)
    attn_sets = (attn_own, attn_part)
    feed_sets = (feed_own, feed_part)
    project_ws = [a[:, :project_cols] for a in attn_sets]
    output_ws = [a[:, project_cols:] for a in attn_sets]
    up_ws = [f[:, :hidden_cols] for f in feed_sets]
    down_ws = [f[:, hidden_cols:] for f in feed_sets]

    def project_bias(k):
        query_part = lax.dynamic_slice_in_dim(query_projection_bias, k * head_cols, head_cols)
        value_part = lax.dynamic_slice_in_dim(value_projection_bias, k * head_cols, head_cols)
        return jnp.concatenate([query_part, jnp.zeros_like(query_part), value_part])

    project_biases = [project_bias(k) for k in slices]
    up_biases = [
        lax.dynamic_slice_in_dim(feed_input_bias, k * hidden_cols, hidden_cols) for k in slices
    ]

    def split_heads(qkv_block):
        query_rows = qkv_block[:, :head_cols].reshape(seq_rows, heads_here, HD)
        key_rows = qkv_block[:, head_cols : 2 * head_cols].reshape(seq_rows, heads_here, HD)
        value_rows = qkv_block[:, 2 * head_cols :].reshape(seq_rows, heads_here, HD)
        return (query_rows, key_rows, value_rows)

    def masked_scores(query_rows, key_rows):
        raw_scores = (
            jnp.einsum("qhe,khe->hqk", query_rows, key_rows, preferred_element_type=jnp.float32)
            * score_scale
        )
        return jnp.where(key_valid[None, None, :], raw_scores, MASKED)

    def attend(qkv_block):
        query_rows, key_rows, value_rows = split_heads(qkv_block)
        scores = masked_scores(query_rows, key_rows)
        row_max = jnp.max(scores, axis=-1, keepdims=True)
        exponent = jnp.exp(scores - row_max)
        row_total = jnp.sum(exponent, axis=-1, keepdims=True)
        weights = (exponent / row_total).astype(jnp.bfloat16)
        mixed_heads = jnp.einsum(
            "hqk,khe->qhe", weights, value_rows, preferred_element_type=jnp.float32
        )
        return (
            mixed_heads.reshape(seq_rows, head_cols).astype(jnp.bfloat16),
            (row_max + jnp.log(row_total))[..., 0],
        )

    def attend_back(qkv_block, row_lse, grad_block):
        query_rows, key_rows, value_rows = split_heads(qkv_block)
        weights = jnp.exp(masked_scores(query_rows, key_rows) - row_lse[..., None])
        grad_heads = grad_block.reshape(seq_rows, heads_here, HD)
        grad_weights = jnp.einsum(
            "qhe,khe->hqk", grad_heads, value_rows, preferred_element_type=jnp.float32
        )
        inner_sum = jnp.sum(weights * grad_weights, axis=-1, keepdims=True)
        grad_scores = (weights * (grad_weights - inner_sum)).astype(jnp.bfloat16)
        grad_query = (
            jnp.einsum("hqk,khe->qhe", grad_scores, key_rows, preferred_element_type=jnp.float32)
            * score_scale
        )
        grad_key = (
            jnp.einsum("hqk,qhe->khe", grad_scores, query_rows, preferred_element_type=jnp.float32)
            * score_scale
        )
        grad_value = jnp.einsum(
            "hqk,qhe->khe", weights.astype(jnp.bfloat16), grad_heads,
            preferred_element_type=jnp.float32,
        )
        joined = jnp.concatenate(
            [
                grad_query.reshape(seq_rows, head_cols),
                grad_key.reshape(seq_rows, head_cols),
                grad_value.reshape(seq_rows, head_cols),
            ],
            axis=-1,
        )
        return joined.astype(jnp.bfloat16)

    gelu_exact = partial(jax.nn.gelu, approximate=False)
    groups = range(2)

    projected = [
        (dot_nn(inputs_full, project_ws[g]) + project_biases[g]).astype(jnp.bfloat16)
        for g in groups
    ]
    attended = [attend(projected[g]) for g in groups]
    mixed = [a[0] for a in attended]
    log_total = [a[1] for a in attended]
    branch = scatter_cores(sum(dot_nt(mixed[g], output_ws[g]) for g in groups))
    first, normed_first, inverse_first = norm_forward(
        inputs_mine.astype(jnp.float32) + branch + attention_output_bias, first_gain, first_shift
    )
    first_full = gather_cores(first)
    preact = [dot_nn(first_full, up_ws[g]) + up_biases[g] for g in groups]
    gelu_pairs = [jax.vjp(gelu_exact, preact[g]) for g in groups]
    hidden = [p[0].astype(jnp.bfloat16) for p in gelu_pairs]
    feed = scatter_cores(sum(dot_nt(hidden[g], down_ws[g]) for g in groups))
    second, normed_second, inverse_second = norm_forward(
        first + feed + feed_output_bias, second_gain, second_shift
    )
    out_mine = second.astype(jnp.bfloat16)
    out_other = to_chip_partner(out_mine[block_rows:])
    out_own = out_mine[:block_rows]
    on_left = chip_side == 0
    layer_output = jnp.stack(
        [jnp.where(on_left, out_own, out_other), jnp.where(on_left, out_other, out_own)], axis=1
    )

    cot = cot_mine.astype(jnp.float32)
    second_gain_part = jnp.sum(cot * normed_second, axis=0)
    second_shift_part = jnp.sum(cot, axis=0)
    grad_second = norm_backward(cot, normed_second, inverse_second, second_gain)
    down_bias_part = jnp.sum(grad_second, axis=0)
    grad_feed_full = gather_cores(grad_second)
    grad_hidden = [dot_nn(grad_feed_full, down_ws[g]) for g in groups]
    down_grads = [dot_tn(grad_feed_full, hidden[g]) for g in groups]
    grad_preact = [gelu_pairs[g][1](grad_hidden[g])[0].astype(jnp.bfloat16) for g in groups]
    up_grads = [dot_tn(first_full, grad_preact[g]) for g in groups]
    up_bias_sums = [jnp.sum(grad_preact[g], axis=0, dtype=jnp.float32) for g in groups]
    grad_first = grad_second + scatter_cores(sum(dot_nt(grad_preact[g], up_ws[g]) for g in groups))
    first_gain_part = jnp.sum(grad_first * normed_first, axis=0)
    first_shift_part = jnp.sum(grad_first, axis=0)
    grad_residual = norm_backward(grad_first, normed_first, inverse_first, first_gain)
    output_bias_part = jnp.sum(grad_residual, axis=0)
    branch_grad_full = gather_cores(grad_residual)
    grad_mixed = [dot_nn(branch_grad_full, output_ws[g]).astype(jnp.bfloat16) for g in groups]
    output_grads = [dot_tn(branch_grad_full, mixed[g]) for g in groups]

    def place(parts, part_len, total_len):
        blank = jnp.zeros((total_len,), jnp.float32)
        for g in groups:
            blank = lax.dynamic_update_slice_in_dim(blank, parts[g], slices[g] * part_len, 0)
        return blank

    rows_block = width // n_data
    vec_block = width // n_all
    up_placed = place(up_bias_sums, hidden_cols, hidden_cols * n_tensor)
    up_columns = (
        up_placed.reshape(n_data, n_tensor, rows_block).transpose(0, 2, 1).reshape(width, n_tensor)
    )
    early_columns = jnp.concatenate(
        [
            jnp.stack(
                [
                    output_bias_part,
                    first_gain_part,
                    first_shift_part,
                    down_bias_part,
                    second_gain_part,
                    second_shift_part,
                ],
                axis=1,
            ),
            up_columns,
        ],
        axis=1,
    )
    early_columns = early_columns + to_core_partner(early_columns)
    early_own = jnp.concatenate([up_grads[0], down_grads[0], output_grads[0]], axis=1)
    early_partner = jnp.concatenate([up_grads[1], down_grads[1], output_grads[1]], axis=1)
    early_cols = early_own.shape[1]
    early_pack = jnp.concatenate([early_own, early_partner, early_columns], axis=1).astype(
        jnp.bfloat16
    )
    early_pack, grad_mixed = lax.optimization_barrier((early_pack, grad_mixed))
    early_reduced = lax.psum_scatter(
        early_pack, "dp", scatter_dimension=0, tiled=True
    ).astype(jnp.float32)
    early_sent = to_chip_partner(early_reduced[:, early_cols:].astype(jnp.bfloat16)).astype(
        jnp.float32
    )
    early_shard = early_reduced[:, :early_cols] + early_sent[:, :early_cols]
    early_small = early_reduced[:, 2 * early_cols :] + early_sent[:, early_cols:]
    up_shard = early_shard[:, :hidden_cols]
    down_shard = early_shard[:, hidden_cols : 2 * hidden_cols]
    output_shard = early_shard[:, 2 * hidden_cols :]

    grad_projected = [attend_back(projected[g], log_total[g], grad_mixed[g]) for g in groups]
    project_grads = [dot_tn(inputs_full, grad_projected[g]) for g in groups]
    qkv_bias_sums = [jnp.sum(grad_projected[g], axis=0, dtype=jnp.float32) for g in groups]
    grad_inputs = grad_residual + scatter_cores(
        sum(dot_nt(grad_projected[g], project_ws[g]) for g in groups)
    )

    late_columns = jnp.stack(
        [
            place([q[:head_cols] for q in qkv_bias_sums], head_cols, width),
            place([q[2 * head_cols :] for q in qkv_bias_sums], head_cols, width),
        ],
        axis=1,
    )
    late_columns = late_columns + to_core_partner(late_columns)
    late_own = jnp.concatenate([project_grads[0], late_columns], axis=1)
    late_partner = jnp.concatenate([project_grads[1], late_columns], axis=1)
    late_total = late_own + to_chip_partner(late_partner.astype(jnp.bfloat16)).astype(jnp.float32)
    late_shard = scatter_dp_permutes(late_total)
    project_shard = late_shard[:, :project_cols]

    def mine_of(column):
        return lax.dynamic_slice_in_dim(column, tensor_index * vec_block, vec_block)

    early = [mine_of(early_small[:, k]) for k in range(6)]
    up_bias_shard = lax.dynamic_index_in_dim(early_small[:, 6:], tensor_index, axis=1, keepdims=False)
    late = [mine_of(late_shard[:, project_cols + k]) for k in range(2)]
    small = [
        late[0],
        late[1],
        early[0],
        early[1],
        early[2],
        up_bias_shard,
        early[3],
        early[4],
        early[5],
    ]

    grad_low = grad_inputs.astype(jnp.bfloat16)
    grad_other = to_chip_partner(grad_low[block_rows:])
    grad_own = grad_low[:block_rows]
    grad_here = jnp.stack(
        [jnp.where(on_left, grad_own, grad_other), jnp.where(on_left, grad_other, grad_own)],
        axis=1,
    )
    returned = lax.all_to_all(grad_here, "dp", split_axis=0, concat_axis=1, tiled=True)
    tokens_grad = jnp.einsum(
        "qs,pqd->psd", placing, returned, preferred_element_type=jnp.float32
    ).astype(jnp.bfloat16)

    return (
        layer_output,
        tokens_grad,
        project_shard,
        small[0],
        small[1],
        output_shard,
        small[2],
        small[3],
        small[4],
        up_shard,
        small[5],
        down_shard,
        small[6],
        small[7],
        small[8],
    )


def solution(mesh):
    in_specs = (
        P(("dp", "tensor"), None, None),
        P(),
        P(),
        P("dp", "tensor"),
        P(),
        P(),
        P("dp", "tensor"),
        P(),
        P(),
        P(),
        P("dp", "tensor"),
        P(),
        P("dp", "tensor"),
        P(),
        P(),
        P(),
        P(("dp", "tensor"), None, None),
    )
    out_specs = (
        P("tensor", "dp", None),
        P(("dp", "tensor"), None, None),
        P("dp", "tensor"),
        P(("dp", "tensor")),
        P(("dp", "tensor")),
        P("dp", "tensor"),
        P(("dp", "tensor")),
        P(("dp", "tensor")),
        P(("dp", "tensor")),
        P("dp", "tensor"),
        P(("dp", "tensor")),
        P("dp", "tensor"),
        P(("dp", "tensor")),
        P(("dp", "tensor")),
        P(("dp", "tensor")),
    )
    return jax.shard_map(
        on_device, mesh=mesh, in_specs=in_specs, out_specs=out_specs, check_vma=False
    )
```

```python
from functools import partial

import jax
import jax.numpy as jnp
from jax import lax
from jax.sharding import PartitionSpec as P


HD = 64


EPSILON = 1e-12
MASKED = -1e30


def norm_forward(value, gain, shift):
    centred = value - jnp.mean(value, axis=-1, keepdims=True)
    inverse = lax.rsqrt(jnp.mean(centred * centred, axis=-1, keepdims=True) + EPSILON)
    normed = centred * inverse
    return (normed * gain + shift, normed, inverse)


def norm_backward(upstream, normed, inverse, gain):
    scaled = upstream * gain
    first_mean = jnp.mean(scaled, axis=-1, keepdims=True)
    second_mean = jnp.mean(scaled * normed, axis=-1, keepdims=True)
    return inverse * (scaled - first_mean - normed * second_mean)


def dot_nt(a, b):
    return lax.dot_general(a, b, (((1,), (1,)), ((), ())), preferred_element_type=jnp.float32)


def dot_tn(a, b):
    return lax.dot_general(a, b, (((0,), (0,)), ((), ())), preferred_element_type=jnp.float32)


def dot_nn(a, b):
    return jnp.dot(a, b, preferred_element_type=jnp.float32)


def on_device(
    tokens,
    lengths,
    dealing,
    project_weight,
    query_projection_bias,
    value_projection_bias,
    attention_output_weight,
    attention_output_bias,
    first_gain,
    first_shift,
    feed_input_weight,
    feed_input_bias,
    feed_output_weight,
    feed_output_bias,
    second_gain,
    second_shift,
    output_grad,
):
    n_data = lax.axis_size("dp")
    n_tensor = lax.axis_size("tensor")
    n_all = n_data * n_tensor
    data_index = lax.axis_index("dp")
    tensor_index = lax.axis_index("tensor")
    seq_total = dealing.shape[0]
    seq_here = seq_total // n_data
    assert n_tensor == 4 and seq_here == 2
    piece_rows = tokens.shape[0]
    block_rows = piece_rows * n_data
    seq_rows = block_rows * n_tensor
    half_rows = seq_rows // 2
    width = tokens.shape[2]
    head_cols = attention_output_weight.shape[1]
    heads_here = head_cols // HD
    hidden_cols = feed_input_weight.shape[1]
    project_cols = project_weight.shape[1]
    score_scale = HD ** (-0.5)

    chip_side = tensor_index // 2
    partner_slice = tensor_index ^ 2
    across_chips = [(k, k ^ 2) for k in range(n_tensor)]
    across_cores = [(k, k ^ 1) for k in range(n_tensor)]

    def to_chip_partner(value):
        return lax.ppermute(value, "tensor", across_chips)

    def to_core_partner(value):
        return lax.ppermute(value, "tensor", across_cores)

    def gather_dp(block):
        return lax.all_gather(block, "dp", axis=0, tiled=True)

    def scatter_dp(total):
        return lax.psum_scatter(
            total.astype(jnp.bfloat16), "dp", scatter_dimension=0, tiled=True
        ).astype(jnp.float32)

    def gather_dp_permutes(block):
        if n_data > 8:
            return gather_dp(block)
        got = [block] + [
            lax.ppermute(block, "dp", [(j, (j + k) % n_data) for j in range(n_data)])
            for k in range(1, n_data)
        ]
        stacked = jnp.stack(got)
        ordered = jnp.take(stacked, (data_index - jnp.arange(n_data)) % n_data, axis=0)
        return ordered.reshape(n_data * block.shape[0], *block.shape[1:])

    def scatter_dp_permutes(total):
        if n_data > 8:
            return scatter_dp(total)
        pieces = total.astype(jnp.bfloat16).reshape(n_data, -1, *total.shape[1:])
        acc = lax.dynamic_index_in_dim(
            total.reshape(pieces.shape), data_index, 0, keepdims=False
        )
        for k in range(1, n_data):
            sent = lax.dynamic_index_in_dim(pieces, (data_index + k) % n_data, 0, keepdims=False)
            acc = acc + lax.ppermute(
                sent, "dp", [(j, (j + k) % n_data) for j in range(n_data)]
            ).astype(jnp.float32)
        return acc

    def gather_cores(mine):
        low = mine.astype(jnp.bfloat16)
        return jnp.concatenate([low, to_core_partner(low)], axis=0)

    def scatter_cores(partial_sum):
        sent = to_core_partner(partial_sum[half_rows:].astype(jnp.bfloat16))
        return partial_sum[:half_rows] + sent.astype(jnp.float32)

    slot_ids = jnp.arange(seq_total, dtype=jnp.int32)
    placing = (dealing[None, :] == slot_ids[:, None]).astype(jnp.bfloat16)

    def deal(values):
        sent = jnp.einsum(
            "qs,psd->pqd", placing, values, preferred_element_type=jnp.float32
        ).astype(jnp.bfloat16)
        here = lax.all_to_all(sent, "dp", split_axis=1, concat_axis=0, tiled=True)
        slot_mine = lax.dynamic_index_in_dim(here, chip_side, axis=1, keepdims=False)
        slot_other = lax.dynamic_index_in_dim(here, 1 - chip_side, axis=1, keepdims=False)
        return jnp.concatenate([slot_mine, to_chip_partner(slot_other)], axis=0)

    inputs_mine = deal(tokens)
    cot_mine = deal(output_grad)
    inputs_full = jnp.concatenate([inputs_mine, to_core_partner(inputs_mine)], axis=0)

    my_slot = data_index * seq_here + chip_side
    seq_length = jnp.sum(jnp.where(dealing == my_slot, lengths, 0))
    blocks = jnp.stack(
        [
            tensor_index,
            partner_slice,
            tensor_index ^ 1,
            partner_slice ^ 1,
        ]
    )
    row_ids = jnp.arange(seq_rows, dtype=jnp.int32)
    owner = blocks[row_ids // block_rows]
    inner = row_ids % block_rows
    position = (inner // piece_rows * n_tensor + owner) * piece_rows + inner % piece_rows
    key_valid = position < seq_length

    attn_w = jnp.concatenate([project_weight, attention_output_weight], axis=1)
    feed_w = jnp.concatenate([feed_input_weight, feed_output_weight], axis=1)
    attn_own = gather_dp_permutes(attn_w)
    attn_part = to_chip_partner(attn_own)
    feed_own = gather_dp(feed_w)
    feed_part = to_chip_partner(feed_own)
    slices = (tensor_index, partner_slice)
    attn_sets = (attn_own, attn_part)
    feed_sets = (feed_own, feed_part)
    project_ws = [a[:, :project_cols] for a in attn_sets]
    output_ws = [a[:, project_cols:] for a in attn_sets]
    up_ws = [f[:, :hidden_cols] for f in feed_sets]
    down_ws = [f[:, hidden_cols:] for f in feed_sets]

    def project_bias(k):
        query_part = lax.dynamic_slice_in_dim(query_projection_bias, k * head_cols, head_cols)
        value_part = lax.dynamic_slice_in_dim(value_projection_bias, k * head_cols, head_cols)
        return jnp.concatenate([query_part, jnp.zeros_like(query_part), value_part])

    project_biases = [project_bias(k) for k in slices]
    up_biases = [
        lax.dynamic_slice_in_dim(feed_input_bias, k * hidden_cols, hidden_cols) for k in slices
    ]

    def split_heads(qkv_block):
        query_rows = qkv_block[:, :head_cols].reshape(seq_rows, heads_here, HD)
        key_rows = qkv_block[:, head_cols : 2 * head_cols].reshape(seq_rows, heads_here, HD)
        value_rows = qkv_block[:, 2 * head_cols :].reshape(seq_rows, heads_here, HD)
        return (query_rows, key_rows, value_rows)

    def masked_scores(query_rows, key_rows):
        raw_scores = (
            jnp.einsum("qhe,khe->hqk", query_rows, key_rows, preferred_element_type=jnp.float32)
            * score_scale
        )
        return jnp.where(key_valid[None, None, :], raw_scores, MASKED)

    def attend(qkv_block):
        query_rows, key_rows, value_rows = split_heads(qkv_block)
        scores = masked_scores(query_rows, key_rows)
        row_max = jnp.max(scores, axis=-1, keepdims=True)
        exponent = jnp.exp(scores - row_max)
        row_total = jnp.sum(exponent, axis=-1, keepdims=True)
        weights = (exponent / row_total).astype(jnp.bfloat16)
        mixed_heads = jnp.einsum(
            "hqk,khe->qhe", weights, value_rows, preferred_element_type=jnp.float32
        )
        return (
            mixed_heads.reshape(seq_rows, head_cols).astype(jnp.bfloat16),
            (row_max + jnp.log(row_total))[..., 0],
        )

    def attend_back(qkv_block, row_lse, grad_block):
        query_rows, key_rows, value_rows = split_heads(qkv_block)
        weights = jnp.exp(masked_scores(query_rows, key_rows) - row_lse[..., None])
        grad_heads = grad_block.reshape(seq_rows, heads_here, HD)
        grad_weights = jnp.einsum(
            "qhe,khe->hqk", grad_heads, value_rows, preferred_element_type=jnp.float32
        )
        inner_sum = jnp.sum(weights * grad_weights, axis=-1, keepdims=True)
        grad_scores = (weights * (grad_weights - inner_sum)).astype(jnp.bfloat16)
        grad_query = (
            jnp.einsum("hqk,khe->qhe", grad_scores, key_rows, preferred_element_type=jnp.float32)
            * score_scale
        )
        grad_key = (
            jnp.einsum("hqk,qhe->khe", grad_scores, query_rows, preferred_element_type=jnp.float32)
            * score_scale
        )
        grad_value = jnp.einsum(
            "hqk,qhe->khe", weights.astype(jnp.bfloat16), grad_heads,
            preferred_element_type=jnp.float32,
        )
        joined = jnp.concatenate(
            [
                grad_query.reshape(seq_rows, head_cols),
                grad_key.reshape(seq_rows, head_cols),
                grad_value.reshape(seq_rows, head_cols),
            ],
            axis=-1,
        )
        return joined.astype(jnp.bfloat16)

    gelu_exact = partial(jax.nn.gelu, approximate=False)
    groups = range(2)

    projected = [
        (dot_nn(inputs_full, project_ws[g]) + project_biases[g]).astype(jnp.bfloat16)
        for g in groups
    ]
    attended = [attend(projected[g]) for g in groups]
    mixed = [a[0] for a in attended]
    log_total = [a[1] for a in attended]
    branch = scatter_cores(sum(dot_nt(mixed[g], output_ws[g]) for g in groups))
    first, normed_first, inverse_first = norm_forward(
        inputs_mine.astype(jnp.float32) + branch + attention_output_bias, first_gain, first_shift
    )
    first_full = gather_cores(first)
    preact = [dot_nn(first_full, up_ws[g]) + up_biases[g] for g in groups]
    gelu_pairs = [jax.vjp(gelu_exact, preact[g]) for g in groups]
    hidden = [p[0].astype(jnp.bfloat16) for p in gelu_pairs]
    feed = scatter_cores(sum(dot_nt(hidden[g], down_ws[g]) for g in groups))
    second, normed_second, inverse_second = norm_forward(
        first + feed + feed_output_bias, second_gain, second_shift
    )
    out_mine = second.astype(jnp.bfloat16)
    out_other = to_chip_partner(out_mine[block_rows:])
    out_own = out_mine[:block_rows]
    on_left = chip_side == 0
    layer_output = jnp.stack(
        [jnp.where(on_left, out_own, out_other), jnp.where(on_left, out_other, out_own)], axis=1
    )

    cot = cot_mine.astype(jnp.float32)
    second_gain_part = jnp.sum(cot * normed_second, axis=0)
    second_shift_part = jnp.sum(cot, axis=0)
    grad_second = norm_backward(cot, normed_second, inverse_second, second_gain)
    down_bias_part = jnp.sum(grad_second, axis=0)
    grad_feed_full = gather_cores(grad_second)
    grad_hidden = [dot_nn(grad_feed_full, down_ws[g]) for g in groups]
    down_grads = [dot_tn(grad_feed_full, hidden[g]) for g in groups]
    grad_preact = [gelu_pairs[g][1](grad_hidden[g])[0].astype(jnp.bfloat16) for g in groups]
    up_grads = [dot_tn(first_full, grad_preact[g]) for g in groups]
    up_bias_sums = [jnp.sum(grad_preact[g], axis=0, dtype=jnp.float32) for g in groups]
    grad_first = grad_second + scatter_cores(sum(dot_nt(grad_preact[g], up_ws[g]) for g in groups))
    first_gain_part = jnp.sum(grad_first * normed_first, axis=0)
    first_shift_part = jnp.sum(grad_first, axis=0)
    grad_residual = norm_backward(grad_first, normed_first, inverse_first, first_gain)
    output_bias_part = jnp.sum(grad_residual, axis=0)
    branch_grad_full = gather_cores(grad_residual)
    grad_mixed = [dot_nn(branch_grad_full, output_ws[g]).astype(jnp.bfloat16) for g in groups]
    output_grads = [dot_tn(branch_grad_full, mixed[g]) for g in groups]

    def place(parts, part_len, total_len):
        blank = jnp.zeros((total_len,), jnp.float32)
        for g in groups:
            blank = lax.dynamic_update_slice_in_dim(blank, parts[g], slices[g] * part_len, 0)
        return blank

    rows_block = width // n_data
    vec_block = width // n_all
    up_placed = place(up_bias_sums, hidden_cols, hidden_cols * n_tensor)
    up_columns = (
        up_placed.reshape(n_data, n_tensor, rows_block).transpose(0, 2, 1).reshape(width, n_tensor)
    )
    early_columns = jnp.concatenate(
        [
            jnp.stack(
                [
                    output_bias_part,
                    first_gain_part,
                    first_shift_part,
                    down_bias_part,
                    second_gain_part,
                    second_shift_part,
                ],
                axis=1,
            ),
            up_columns,
        ],
        axis=1,
    )
    early_columns = early_columns + to_core_partner(early_columns)
    early_own = jnp.concatenate([up_grads[0], down_grads[0], output_grads[0]], axis=1)
    early_partner = jnp.concatenate([up_grads[1], down_grads[1], output_grads[1]], axis=1)
    early_cols = early_own.shape[1]
    early_pack = jnp.concatenate([early_own, early_partner, early_columns], axis=1).astype(
        jnp.bfloat16
    )
    early_pack, grad_mixed = lax.optimization_barrier((early_pack, grad_mixed))
    early_reduced = lax.psum_scatter(
        early_pack, "dp", scatter_dimension=0, tiled=True
    ).astype(jnp.float32)
    early_sent = to_chip_partner(early_reduced[:, early_cols:].astype(jnp.bfloat16)).astype(
        jnp.float32
    )
    early_shard = early_reduced[:, :early_cols] + early_sent[:, :early_cols]
    early_small = early_reduced[:, 2 * early_cols :] + early_sent[:, early_cols:]
    up_shard = early_shard[:, :hidden_cols]
    down_shard = early_shard[:, hidden_cols : 2 * hidden_cols]
    output_shard = early_shard[:, 2 * hidden_cols :]

    grad_projected = [None, None]
    grad_projected[1] = attend_back(projected[1], log_total[1], grad_mixed[1])
    partner_project_grad = dot_tn(inputs_full, grad_projected[1])
    partner_low, own_grad_mixed = lax.optimization_barrier(
        (partner_project_grad.astype(jnp.bfloat16), grad_mixed[0])
    )
    crossed_project_grad = to_chip_partner(partner_low)
    grad_projected[0] = attend_back(projected[0], log_total[0], own_grad_mixed)
    own_project_grad = dot_tn(inputs_full, grad_projected[0])
    qkv_bias_sums = [jnp.sum(grad_projected[g], axis=0, dtype=jnp.float32) for g in groups]
    grad_inputs = grad_residual + scatter_cores(
        sum(dot_nt(grad_projected[g], project_ws[g]) for g in groups)
    )

    late_columns = jnp.stack(
        [
            place([q[:head_cols] for q in qkv_bias_sums], head_cols, width),
            place([q[2 * head_cols :] for q in qkv_bias_sums], head_cols, width),
        ],
        axis=1,
    )
    late_columns = late_columns + to_core_partner(late_columns)
    late_total = jnp.concatenate(
        [own_project_grad + crossed_project_grad.astype(jnp.float32), late_columns], axis=1
    )
    late_shard = scatter_dp_permutes(late_total)
    project_shard = late_shard[:, :project_cols]
    late_small = late_shard[:, project_cols:]
    late_small = late_small + to_chip_partner(late_small)

    def mine_of(column):
        return lax.dynamic_slice_in_dim(column, tensor_index * vec_block, vec_block)

    early = [mine_of(early_small[:, k]) for k in range(6)]
    up_bias_shard = lax.dynamic_index_in_dim(early_small[:, 6:], tensor_index, axis=1, keepdims=False)
    late = [mine_of(late_small[:, k]) for k in range(2)]
    small = [
        late[0],
        late[1],
        early[0],
        early[1],
        early[2],
        up_bias_shard,
        early[3],
        early[4],
        early[5],
    ]

    grad_low = grad_inputs.astype(jnp.bfloat16)
    grad_other = to_chip_partner(grad_low[block_rows:])
    grad_own = grad_low[:block_rows]
    grad_here = jnp.stack(
        [jnp.where(on_left, grad_own, grad_other), jnp.where(on_left, grad_other, grad_own)],
        axis=1,
    )
    returned = lax.all_to_all(grad_here, "dp", split_axis=0, concat_axis=1, tiled=True)
    tokens_grad = jnp.einsum(
        "qs,pqd->psd", placing, returned, preferred_element_type=jnp.float32
    ).astype(jnp.bfloat16)

    return (
        layer_output,
        tokens_grad,
        project_shard,
        small[0],
        small[1],
        output_shard,
        small[2],
        small[3],
        small[4],
        up_shard,
        small[5],
        down_shard,
        small[6],
        small[7],
        small[8],
    )


def solution(mesh):
    in_specs = (
        P(("dp", "tensor"), None, None),
        P(),
        P(),
        P("dp", "tensor"),
        P(),
        P(),
        P("dp", "tensor"),
        P(),
        P(),
        P(),
        P("dp", "tensor"),
        P(),
        P("dp", "tensor"),
        P(),
        P(),
        P(),
        P(("dp", "tensor"), None, None),
    )
    out_specs = (
        P("tensor", "dp", None),
        P(("dp", "tensor"), None, None),
        P("dp", "tensor"),
        P(("dp", "tensor")),
        P(("dp", "tensor")),
        P("dp", "tensor"),
        P(("dp", "tensor")),
        P(("dp", "tensor")),
        P(("dp", "tensor")),
        P("dp", "tensor"),
        P(("dp", "tensor")),
        P("dp", "tensor"),
        P(("dp", "tensor")),
        P(("dp", "tensor")),
        P(("dp", "tensor")),
    )

    return jax.shard_map(
        on_device, mesh=mesh, in_specs=in_specs, out_specs=out_specs, check_vma=False
    )
```

```python
from functools import partial

import jax
import jax.numpy as jnp
from jax import lax
from jax.sharding import PartitionSpec as P


HD = 64


EPSILON = 1e-12
MASKED = -1e30


def norm_forward(value, gain, shift):
    centred = value - jnp.mean(value, axis=-1, keepdims=True)
    inverse = lax.rsqrt(jnp.mean(centred * centred, axis=-1, keepdims=True) + EPSILON)
    normed = centred * inverse
    return (normed * gain + shift, normed, inverse)


def norm_backward(upstream, normed, inverse, gain):
    scaled = upstream * gain
    first_mean = jnp.mean(scaled, axis=-1, keepdims=True)
    second_mean = jnp.mean(scaled * normed, axis=-1, keepdims=True)
    return inverse * (scaled - first_mean - normed * second_mean)


def dot_nt(a, b):
    return lax.dot_general(a, b, (((1,), (1,)), ((), ())), preferred_element_type=jnp.float32)


def dot_tn(a, b):
    return lax.dot_general(a, b, (((0,), (0,)), ((), ())), preferred_element_type=jnp.float32)


def dot_nn(a, b):
    return jnp.dot(a, b, preferred_element_type=jnp.float32)


def on_device(
    tokens,
    lengths,
    dealing,
    project_weight,
    query_projection_bias,
    value_projection_bias,
    attention_output_weight,
    attention_output_bias,
    first_gain,
    first_shift,
    feed_input_weight,
    feed_input_bias,
    feed_output_weight,
    feed_output_bias,
    second_gain,
    second_shift,
    output_grad,
):
    n_data = lax.axis_size("dp")
    n_tensor = lax.axis_size("tensor")
    n_all = n_data * n_tensor
    data_index = lax.axis_index("dp")
    tensor_index = lax.axis_index("tensor")
    seq_total = dealing.shape[0]
    seq_here = seq_total // n_data
    assert n_tensor == 4 and seq_here == 2
    piece_rows = tokens.shape[0]
    block_rows = piece_rows * n_data
    seq_rows = block_rows * n_tensor
    half_rows = seq_rows // 2
    width = tokens.shape[2]
    head_cols = attention_output_weight.shape[1]
    heads_here = head_cols // HD
    hidden_cols = feed_input_weight.shape[1]
    project_cols = project_weight.shape[1]
    score_scale = HD ** (-0.5)

    chip_side = tensor_index // 2
    partner_slice = tensor_index ^ 2
    across_chips = [(k, k ^ 2) for k in range(n_tensor)]
    across_cores = [(k, k ^ 1) for k in range(n_tensor)]

    def to_chip_partner(value):
        return lax.ppermute(value, "tensor", across_chips)

    def to_core_partner(value):
        return lax.ppermute(value, "tensor", across_cores)

    def gather_dp(block):
        return lax.all_gather(block, "dp", axis=0, tiled=True)

    def scatter_dp(total):
        return lax.psum_scatter(
            total.astype(jnp.bfloat16), "dp", scatter_dimension=0, tiled=True
        ).astype(jnp.float32)

    def scatter_dp_permutes(total):
        if n_data > 8:
            return scatter_dp(total)
        pieces = total.astype(jnp.bfloat16).reshape(n_data, -1, *total.shape[1:])
        acc = lax.dynamic_index_in_dim(
            total.reshape(pieces.shape), data_index, 0, keepdims=False
        )
        for k in range(1, n_data):
            sent = lax.dynamic_index_in_dim(pieces, (data_index + k) % n_data, 0, keepdims=False)
            acc = acc + lax.ppermute(
                sent, "dp", [(j, (j + k) % n_data) for j in range(n_data)]
            ).astype(jnp.float32)
        return acc

    def gather_cores(mine):
        low = mine.astype(jnp.bfloat16)
        return jnp.concatenate([low, to_core_partner(low)], axis=0)

    def scatter_cores(partial_sum):
        sent = to_core_partner(partial_sum[half_rows:].astype(jnp.bfloat16))
        return partial_sum[:half_rows] + sent.astype(jnp.float32)

    slot_ids = jnp.arange(seq_total, dtype=jnp.int32)
    placing = (dealing[None, :] == slot_ids[:, None]).astype(jnp.bfloat16)

    def deal(values):
        sent = jnp.einsum(
            "qs,psd->pqd", placing, values, preferred_element_type=jnp.float32
        ).astype(jnp.bfloat16)
        here = lax.all_to_all(sent, "dp", split_axis=1, concat_axis=0, tiled=True)
        slot_mine = lax.dynamic_index_in_dim(here, chip_side, axis=1, keepdims=False)
        slot_other = lax.dynamic_index_in_dim(here, 1 - chip_side, axis=1, keepdims=False)
        return jnp.concatenate([slot_mine, to_chip_partner(slot_other)], axis=0)

    inputs_mine = deal(tokens)
    cot_mine = deal(output_grad)
    inputs_full = jnp.concatenate([inputs_mine, to_core_partner(inputs_mine)], axis=0)

    my_slot = data_index * seq_here + chip_side
    seq_length = jnp.sum(jnp.where(dealing == my_slot, lengths, 0))
    blocks = jnp.stack(
        [
            tensor_index,
            partner_slice,
            tensor_index ^ 1,
            partner_slice ^ 1,
        ]
    )
    row_ids = jnp.arange(seq_rows, dtype=jnp.int32)
    owner = blocks[row_ids // block_rows]
    inner = row_ids % block_rows
    position = (inner // piece_rows * n_tensor + owner) * piece_rows + inner % piece_rows
    key_valid = position < seq_length

    attn_w = jnp.concatenate([project_weight, attention_output_weight], axis=1)
    feed_w = jnp.concatenate([feed_input_weight, feed_output_weight], axis=1)
    attn_own = gather_dp(attn_w)
    attn_part = to_chip_partner(attn_own)
    feed_own = gather_dp(feed_w)
    feed_part = to_chip_partner(feed_own)
    slices = (tensor_index, partner_slice)
    attn_sets = (attn_own, attn_part)
    feed_sets = (feed_own, feed_part)
    project_ws = [a[:, :project_cols] for a in attn_sets]
    output_ws = [a[:, project_cols:] for a in attn_sets]
    up_ws = [f[:, :hidden_cols] for f in feed_sets]
    down_ws = [f[:, hidden_cols:] for f in feed_sets]

    def project_bias(k):
        query_part = lax.dynamic_slice_in_dim(query_projection_bias, k * head_cols, head_cols)
        value_part = lax.dynamic_slice_in_dim(value_projection_bias, k * head_cols, head_cols)
        return jnp.concatenate([query_part, jnp.zeros_like(query_part), value_part])

    project_biases = [project_bias(k) for k in slices]
    up_biases = [
        lax.dynamic_slice_in_dim(feed_input_bias, k * hidden_cols, hidden_cols) for k in slices
    ]

    def split_heads(qkv_block):
        query_rows = qkv_block[:, :head_cols].reshape(seq_rows, heads_here, HD)
        key_rows = qkv_block[:, head_cols : 2 * head_cols].reshape(seq_rows, heads_here, HD)
        value_rows = qkv_block[:, 2 * head_cols :].reshape(seq_rows, heads_here, HD)
        return (query_rows, key_rows, value_rows)

    def masked_scores(query_rows, key_rows):
        raw_scores = (
            jnp.einsum("qhe,khe->hqk", query_rows, key_rows, preferred_element_type=jnp.float32)
            * score_scale
        )
        return jnp.where(key_valid[None, None, :], raw_scores, MASKED)

    def attend(qkv_block):
        query_rows, key_rows, value_rows = split_heads(qkv_block)
        scores = masked_scores(query_rows, key_rows)
        row_max = jnp.max(scores, axis=-1, keepdims=True)
        exponent = jnp.exp(scores - row_max)
        row_total = jnp.sum(exponent, axis=-1, keepdims=True)
        weights = (exponent / row_total).astype(jnp.bfloat16)
        mixed_heads = jnp.einsum(
            "hqk,khe->qhe", weights, value_rows, preferred_element_type=jnp.float32
        )
        return (
            mixed_heads.reshape(seq_rows, head_cols).astype(jnp.bfloat16),
            (row_max + jnp.log(row_total))[..., 0],
        )

    def attend_back(qkv_block, row_lse, grad_block):
        query_rows, key_rows, value_rows = split_heads(qkv_block)
        weights = jnp.exp(masked_scores(query_rows, key_rows) - row_lse[..., None])
        grad_heads = grad_block.reshape(seq_rows, heads_here, HD)
        grad_weights = jnp.einsum(
            "qhe,khe->hqk", grad_heads, value_rows, preferred_element_type=jnp.float32
        )
        inner_sum = jnp.sum(weights * grad_weights, axis=-1, keepdims=True)
        grad_scores = (weights * (grad_weights - inner_sum)).astype(jnp.bfloat16)
        grad_query = (
            jnp.einsum("hqk,khe->qhe", grad_scores, key_rows, preferred_element_type=jnp.float32)
            * score_scale
        )
        grad_key = (
            jnp.einsum("hqk,qhe->khe", grad_scores, query_rows, preferred_element_type=jnp.float32)
            * score_scale
        )
        grad_value = jnp.einsum(
            "hqk,qhe->khe", weights.astype(jnp.bfloat16), grad_heads,
            preferred_element_type=jnp.float32,
        )
        joined = jnp.concatenate(
            [
                grad_query.reshape(seq_rows, head_cols),
                grad_key.reshape(seq_rows, head_cols),
                grad_value.reshape(seq_rows, head_cols),
            ],
            axis=-1,
        )
        return joined.astype(jnp.bfloat16)

    gelu_exact = partial(jax.nn.gelu, approximate=False)
    groups = range(2)

    projected = [
        (dot_nn(inputs_full, project_ws[g]) + project_biases[g]).astype(jnp.bfloat16)
        for g in groups
    ]
    attended = [attend(projected[g]) for g in groups]
    mixed = [a[0] for a in attended]
    log_total = [a[1] for a in attended]
    branch = scatter_cores(sum(dot_nt(mixed[g], output_ws[g]) for g in groups))
    first, normed_first, inverse_first = norm_forward(
        inputs_mine.astype(jnp.float32) + branch + attention_output_bias, first_gain, first_shift
    )
    first_full = gather_cores(first)
    preact = [dot_nn(first_full, up_ws[g]) + up_biases[g] for g in groups]
    gelu_pairs = [jax.vjp(gelu_exact, preact[g]) for g in groups]
    hidden = [p[0].astype(jnp.bfloat16) for p in gelu_pairs]
    feed = scatter_cores(sum(dot_nt(hidden[g], down_ws[g]) for g in groups))
    second, normed_second, inverse_second = norm_forward(
        first + feed + feed_output_bias, second_gain, second_shift
    )
    out_mine = second.astype(jnp.bfloat16)
    out_other = to_chip_partner(out_mine[block_rows:])
    out_own = out_mine[:block_rows]
    on_left = chip_side == 0
    layer_output = jnp.stack(
        [jnp.where(on_left, out_own, out_other), jnp.where(on_left, out_other, out_own)], axis=1
    )

    cot = cot_mine.astype(jnp.float32)
    second_gain_part = jnp.sum(cot * normed_second, axis=0)
    second_shift_part = jnp.sum(cot, axis=0)
    grad_second = norm_backward(cot, normed_second, inverse_second, second_gain)
    down_bias_part = jnp.sum(grad_second, axis=0)
    grad_feed_full = gather_cores(grad_second)
    grad_hidden = [dot_nn(grad_feed_full, down_ws[g]) for g in groups]
    down_grads = [dot_tn(grad_feed_full, hidden[g]) for g in groups]
    grad_preact = [gelu_pairs[g][1](grad_hidden[g])[0].astype(jnp.bfloat16) for g in groups]
    up_grads = [dot_tn(first_full, grad_preact[g]) for g in groups]
    up_bias_sums = [jnp.sum(grad_preact[g], axis=0, dtype=jnp.float32) for g in groups]
    feed_own_grad = jnp.concatenate([up_grads[0], down_grads[0]], axis=1)
    feed_partner_grad = jnp.concatenate([up_grads[1], down_grads[1]], axis=1)
    feed_cols = feed_own_grad.shape[1]
    feed_pack = jnp.concatenate([feed_own_grad, feed_partner_grad], axis=1).astype(jnp.bfloat16)
    first_partial = sum(dot_nt(grad_preact[g], up_ws[g]) for g in groups)
    feed_pack, first_partial = lax.optimization_barrier((feed_pack, first_partial))
    feed_reduced = lax.psum_scatter(
        feed_pack, "dp", scatter_dimension=0, tiled=True
    ).astype(jnp.float32)
    feed_sent = to_chip_partner(feed_reduced[:, feed_cols:].astype(jnp.bfloat16))
    feed_shard = feed_reduced[:, :feed_cols] + feed_sent.astype(jnp.float32)
    up_shard = feed_shard[:, :hidden_cols]
    down_shard = feed_shard[:, hidden_cols:]

    grad_first = grad_second + scatter_cores(first_partial)
    first_gain_part = jnp.sum(grad_first * normed_first, axis=0)
    first_shift_part = jnp.sum(grad_first, axis=0)
    grad_residual = norm_backward(grad_first, normed_first, inverse_first, first_gain)
    output_bias_part = jnp.sum(grad_residual, axis=0)
    branch_grad_full = gather_cores(grad_residual)
    grad_mixed = [dot_nn(branch_grad_full, output_ws[g]).astype(jnp.bfloat16) for g in groups]
    output_grads = [dot_tn(branch_grad_full, mixed[g]) for g in groups]

    def place(parts, part_len, total_len):
        blank = jnp.zeros((total_len,), jnp.float32)
        for g in groups:
            blank = lax.dynamic_update_slice_in_dim(blank, parts[g], slices[g] * part_len, 0)
        return blank

    rows_block = width // n_data
    vec_block = width // n_all
    up_placed = place(up_bias_sums, hidden_cols, hidden_cols * n_tensor)
    up_columns = (
        up_placed.reshape(n_data, n_tensor, rows_block).transpose(0, 2, 1).reshape(width, n_tensor)
    )
    early_columns = jnp.concatenate(
        [
            jnp.stack(
                [
                    output_bias_part,
                    first_gain_part,
                    first_shift_part,
                    down_bias_part,
                    second_gain_part,
                    second_shift_part,
                ],
                axis=1,
            ),
            up_columns,
        ],
        axis=1,
    )
    early_columns = early_columns + to_core_partner(early_columns)

    grad_projected = [None, None]
    grad_projected[1] = attend_back(projected[1], log_total[1], grad_mixed[1])
    partner_project_grad = dot_tn(inputs_full, grad_projected[1])
    cross_pack = jnp.concatenate(
        [partner_project_grad, output_grads[1], early_columns], axis=1
    ).astype(jnp.bfloat16)
    cross_pack, own_grad_mixed = lax.optimization_barrier((cross_pack, grad_mixed[0]))
    crossed = to_chip_partner(cross_pack)
    grad_projected[0] = attend_back(projected[0], log_total[0], own_grad_mixed)
    own_project_grad = dot_tn(inputs_full, grad_projected[0])
    qkv_bias_sums = [jnp.sum(grad_projected[g], axis=0, dtype=jnp.float32) for g in groups]
    grad_inputs = grad_residual + scatter_cores(
        sum(dot_nt(grad_projected[g], project_ws[g]) for g in groups)
    )

    late_columns = jnp.stack(
        [
            place([q[:head_cols] for q in qkv_bias_sums], head_cols, width),
            place([q[2 * head_cols :] for q in qkv_bias_sums], head_cols, width),
        ],
        axis=1,
    )
    late_columns = late_columns + to_core_partner(late_columns)
    late_total = jnp.concatenate(
        [
            jnp.concatenate([own_project_grad, output_grads[0], early_columns], axis=1)
            + crossed.astype(jnp.float32),
            late_columns,
        ],
        axis=1,
    )
    late_shard = scatter_dp_permutes(late_total)
    project_shard = late_shard[:, :project_cols]
    output_shard = late_shard[:, project_cols : project_cols + head_cols]
    early_at = project_cols + head_cols
    late_at = early_at + early_columns.shape[1]
    early_small = late_shard[:, early_at:late_at]
    late_small = late_shard[:, late_at:]
    late_small = late_small + to_chip_partner(late_small)

    def mine_of(column):
        return lax.dynamic_slice_in_dim(column, tensor_index * vec_block, vec_block)

    early = [mine_of(early_small[:, k]) for k in range(6)]
    up_bias_shard = lax.dynamic_index_in_dim(early_small[:, 6:], tensor_index, axis=1, keepdims=False)
    late = [mine_of(late_small[:, k]) for k in range(2)]
    small = [
        late[0],
        late[1],
        early[0],
        early[1],
        early[2],
        up_bias_shard,
        early[3],
        early[4],
        early[5],
    ]

    grad_low = grad_inputs.astype(jnp.bfloat16)
    grad_other = to_chip_partner(grad_low[block_rows:])
    grad_own = grad_low[:block_rows]
    grad_here = jnp.stack(
        [jnp.where(on_left, grad_own, grad_other), jnp.where(on_left, grad_other, grad_own)],
        axis=1,
    )
    returned = lax.all_to_all(grad_here, "dp", split_axis=0, concat_axis=1, tiled=True)
    tokens_grad = jnp.einsum(
        "qs,pqd->psd", placing, returned, preferred_element_type=jnp.float32
    ).astype(jnp.bfloat16)

    return (
        layer_output,
        tokens_grad,
        project_shard,
        small[0],
        small[1],
        output_shard,
        small[2],
        small[3],
        small[4],
        up_shard,
        small[5],
        down_shard,
        small[6],
        small[7],
        small[8],
    )


def solution(mesh):
    in_specs = (
        P(("dp", "tensor"), None, None),
        P(),
        P(),
        P("dp", "tensor"),
        P(),
        P(),
        P("dp", "tensor"),
        P(),
        P(),
        P(),
        P("dp", "tensor"),
        P(),
        P("dp", "tensor"),
        P(),
        P(),
        P(),
        P(("dp", "tensor"), None, None),
    )
    out_specs = (
        P("tensor", "dp", None),
        P(("dp", "tensor"), None, None),
        P("dp", "tensor"),
        P(("dp", "tensor")),
        P(("dp", "tensor")),
        P("dp", "tensor"),
        P(("dp", "tensor")),
        P(("dp", "tensor")),
        P(("dp", "tensor")),
        P("dp", "tensor"),
        P(("dp", "tensor")),
        P("dp", "tensor"),
        P(("dp", "tensor")),
        P(("dp", "tensor")),
        P(("dp", "tensor")),
    )

    return jax.shard_map(
        on_device, mesh=mesh, in_specs=in_specs, out_specs=out_specs, check_vma=False
    )
```

```python
from functools import partial

import jax
import jax.numpy as jnp
from jax import lax
from jax.sharding import PartitionSpec as P

HD = 64


EPSILON = 1e-12
MASKED = -1e30


def norm_forward(value, gain, shift):
    centred = value - jnp.mean(value, axis=-1, keepdims=True)
    inverse = lax.rsqrt(jnp.mean(centred * centred, axis=-1, keepdims=True) + EPSILON)
    normed = centred * inverse
    return (normed * gain + shift, normed, inverse)


def norm_backward(upstream, normed, inverse, gain):
    scaled = upstream * gain
    first_mean = jnp.mean(scaled, axis=-1, keepdims=True)
    second_mean = jnp.mean(scaled * normed, axis=-1, keepdims=True)
    return inverse * (scaled - first_mean - normed * second_mean)


def dot_nt(a, b):
    return lax.dot_general(a, b, (((1,), (1,)), ((), ())), preferred_element_type=jnp.float32)


def dot_tn(a, b):
    return lax.dot_general(a, b, (((0,), (0,)), ((), ())), preferred_element_type=jnp.float32)


def dot_nn(a, b):
    return jnp.dot(a, b, preferred_element_type=jnp.float32)


def on_device(
    tokens,
    lengths,
    dealing,
    project_weight,
    query_projection_bias,
    value_projection_bias,
    attention_output_weight,
    attention_output_bias,
    first_gain,
    first_shift,
    feed_input_weight,
    feed_input_bias,
    feed_output_weight,
    feed_output_bias,
    second_gain,
    second_shift,
    output_grad,
):
    n_data = lax.axis_size("dp")
    n_tensor = lax.axis_size("tensor")
    n_all = n_data * n_tensor
    data_index = lax.axis_index("dp")
    tensor_index = lax.axis_index("tensor")
    seq_total = dealing.shape[0]
    seq_here = seq_total // n_data
    assert n_tensor == 4 and seq_here == 2
    piece_rows = tokens.shape[0]
    block_rows = piece_rows * n_data
    seq_rows = block_rows * n_tensor
    half_rows = seq_rows // 2
    width = tokens.shape[2]
    head_cols = attention_output_weight.shape[1]
    heads_here = head_cols // HD
    hidden_cols = feed_input_weight.shape[1]
    project_cols = project_weight.shape[1]
    score_scale = HD ** (-0.5)

    chip_side = tensor_index // 2
    core = tensor_index % 2
    partner_slice = tensor_index ^ 2
    across_chips = [(k, k ^ 2) for k in range(n_tensor)]
    across_cores = [(k, k ^ 1) for k in range(n_tensor)]

    def to_chip_partner(value):
        return lax.ppermute(value, "tensor", across_chips)

    def to_core_partner(value):
        return lax.ppermute(value, "tensor", across_cores)

    def gather_dp(block):
        return lax.all_gather(block, "dp", axis=0, tiled=True)

    def scatter_dp(total):
        return lax.psum_scatter(
            total.astype(jnp.bfloat16), "dp", scatter_dimension=0, tiled=True
        ).astype(jnp.float32)

    def scatter_dp_permutes(total):
        if n_data > 8:
            return scatter_dp(total)
        pieces = total.astype(jnp.bfloat16).reshape(n_data, -1, *total.shape[1:])
        acc = lax.dynamic_index_in_dim(
            total.reshape(pieces.shape), data_index, 0, keepdims=False
        )
        for k in range(1, n_data):
            sent = lax.dynamic_index_in_dim(pieces, (data_index + k) % n_data, 0, keepdims=False)
            acc = acc + lax.ppermute(
                sent, "dp", [(j, (j + k) % n_data) for j in range(n_data)]
            ).astype(jnp.float32)
        return acc

    def gather_cores(mine):
        low = mine.astype(jnp.bfloat16)
        return jnp.concatenate([low, to_core_partner(low)], axis=0)

    def scatter_cores(partial_sum):
        sent = to_core_partner(partial_sum[half_rows:].astype(jnp.bfloat16))
        return partial_sum[:half_rows] + sent.astype(jnp.float32)

    slot_ids = jnp.arange(seq_total, dtype=jnp.int32)
    placing = (dealing[None, :] == slot_ids[:, None]).astype(jnp.bfloat16)
    def deal(values):
        sent = jnp.einsum(
            "qs,psd->pqd", placing, values, preferred_element_type=jnp.float32
        ).astype(jnp.bfloat16)
        here = lax.all_to_all(sent, "dp", split_axis=1, concat_axis=0, tiled=True)
        slot_mine = lax.dynamic_index_in_dim(here, chip_side, axis=1, keepdims=False)
        slot_other = lax.dynamic_index_in_dim(here, 1 - chip_side, axis=1, keepdims=False)
        return jnp.concatenate([slot_mine, to_chip_partner(slot_other)], axis=0)

    inputs_mine = deal(tokens)
    cot_mine = deal(output_grad)
    inputs_full = jnp.concatenate([inputs_mine, to_core_partner(inputs_mine)], axis=0)

    my_slot = data_index * seq_here + chip_side
    seq_length = jnp.sum(jnp.where(dealing == my_slot, lengths, 0))
    blocks = jnp.stack(
        [
            tensor_index,
            partner_slice,
            tensor_index ^ 1,
            partner_slice ^ 1,
        ]
    )
    row_ids = jnp.arange(seq_rows, dtype=jnp.int32)
    owner = blocks[row_ids // block_rows]
    inner = row_ids % block_rows
    position = (inner // piece_rows * n_tensor + owner) * piece_rows + inner % piece_rows
    key_valid = position < seq_length

    attn_both = gather_dp(
        jnp.concatenate(
            [project_weight, attention_output_weight, to_chip_partner(project_weight)], axis=1
        )
    )
    feed_both = gather_dp(
        jnp.concatenate(
            [feed_input_weight, feed_output_weight, to_chip_partner(feed_input_weight)], axis=1
        )
    )
    output_own = attn_both[:, project_cols : project_cols + head_cols]
    down_own = feed_both[:, hidden_cols : 2 * hidden_cols]
    slices = (tensor_index, partner_slice)
    project_ws = [attn_both[:, :project_cols], attn_both[:, project_cols + head_cols :]]
    output_ws = [output_own, to_chip_partner(output_own)]
    up_ws = [feed_both[:, :hidden_cols], feed_both[:, 2 * hidden_cols :]]
    down_ws = [down_own, to_chip_partner(down_own)]

    def project_bias(k):
        query_part = lax.dynamic_slice_in_dim(query_projection_bias, k * head_cols, head_cols)
        value_part = lax.dynamic_slice_in_dim(value_projection_bias, k * head_cols, head_cols)
        return jnp.concatenate([query_part, jnp.zeros_like(query_part), value_part])

    project_biases = [project_bias(k) for k in slices]
    up_biases = [
        lax.dynamic_slice_in_dim(feed_input_bias, k * hidden_cols, hidden_cols) for k in slices
    ]

    def split_heads(qkv_block):
        query_rows = qkv_block[:, :head_cols].reshape(seq_rows, heads_here, HD)
        key_rows = qkv_block[:, head_cols : 2 * head_cols].reshape(seq_rows, heads_here, HD)
        value_rows = qkv_block[:, 2 * head_cols :].reshape(seq_rows, heads_here, HD)
        return (query_rows, key_rows, value_rows)

    def masked_scores(query_rows, key_rows):
        raw_scores = (
            jnp.einsum("qhe,khe->hqk", query_rows, key_rows, preferred_element_type=jnp.float32)
            * score_scale
        )
        return jnp.where(key_valid[None, None, :], raw_scores, MASKED)

    def attend(qkv_block):
        query_rows, key_rows, value_rows = split_heads(qkv_block)
        scores = masked_scores(query_rows, key_rows)
        row_max = jnp.max(scores, axis=-1, keepdims=True)
        exponent = jnp.exp(scores - row_max)
        row_total = jnp.sum(exponent, axis=-1, keepdims=True)
        weights = (exponent / row_total).astype(jnp.bfloat16)
        mixed_heads = jnp.einsum(
            "hqk,khe->qhe", weights, value_rows, preferred_element_type=jnp.float32
        )
        return (
            mixed_heads.reshape(seq_rows, head_cols).astype(jnp.bfloat16),
            (row_max + jnp.log(row_total))[..., 0],
        )

    def attend_back(qkv_block, row_lse, grad_block):
        query_rows, key_rows, value_rows = split_heads(qkv_block)
        weights = jnp.exp(masked_scores(query_rows, key_rows) - row_lse[..., None])
        grad_heads = grad_block.reshape(seq_rows, heads_here, HD)
        grad_weights = jnp.einsum(
            "qhe,khe->hqk", grad_heads, value_rows, preferred_element_type=jnp.float32
        )
        inner_sum = jnp.sum(weights * grad_weights, axis=-1, keepdims=True)
        grad_scores = (weights * (grad_weights - inner_sum)).astype(jnp.bfloat16)
        grad_query = (
            jnp.einsum("hqk,khe->qhe", grad_scores, key_rows, preferred_element_type=jnp.float32)
            * score_scale
        )
        grad_key = (
            jnp.einsum("hqk,qhe->khe", grad_scores, query_rows, preferred_element_type=jnp.float32)
            * score_scale
        )
        grad_value = jnp.einsum(
            "hqk,qhe->khe", weights.astype(jnp.bfloat16), grad_heads,
            preferred_element_type=jnp.float32,
        )
        joined = jnp.concatenate(
            [
                grad_query.reshape(seq_rows, head_cols),
                grad_key.reshape(seq_rows, head_cols),
                grad_value.reshape(seq_rows, head_cols),
            ],
            axis=-1,
        )
        return joined.astype(jnp.bfloat16)

    gelu_exact = partial(jax.nn.gelu, approximate=False)
    groups = range(2)

    projected = [
        (dot_nn(inputs_full, project_ws[g]) + project_biases[g]).astype(jnp.bfloat16)
        for g in groups
    ]
    attended = [attend(projected[g]) for g in groups]
    mixed = [a[0] for a in attended]
    log_total = [a[1] for a in attended]
    branch = scatter_cores(sum(dot_nt(mixed[g], output_ws[g]) for g in groups))
    first, normed_first, inverse_first = norm_forward(
        inputs_mine.astype(jnp.float32) + branch + attention_output_bias, first_gain, first_shift
    )
    first_full = gather_cores(first)
    preact = [dot_nn(first_full, up_ws[g]) + up_biases[g] for g in groups]
    gelu_pairs = [jax.vjp(gelu_exact, preact[g]) for g in groups]
    hidden = [p[0].astype(jnp.bfloat16) for p in gelu_pairs]
    feed = scatter_cores(sum(dot_nt(hidden[g], down_ws[g]) for g in groups))
    second, normed_second, inverse_second = norm_forward(
        first + feed + feed_output_bias, second_gain, second_shift
    )
    out_mine = second.astype(jnp.bfloat16)
    out_other = to_chip_partner(out_mine[block_rows:])
    out_own = out_mine[:block_rows]
    on_left = chip_side == 0
    layer_output = jnp.stack(
        [jnp.where(on_left, out_own, out_other), jnp.where(on_left, out_other, out_own)], axis=1
    )

    cot = cot_mine.astype(jnp.float32)
    second_gain_part = jnp.sum(cot * normed_second, axis=0)
    second_shift_part = jnp.sum(cot, axis=0)
    grad_second = norm_backward(cot, normed_second, inverse_second, second_gain)
    down_bias_part = jnp.sum(grad_second, axis=0)
    grad_feed_full = gather_cores(grad_second)
    grad_hidden = [dot_nn(grad_feed_full, down_ws[g]) for g in groups]
    down_grads = [dot_tn(grad_feed_full, hidden[g]) for g in groups]
    grad_preact = [gelu_pairs[g][1](grad_hidden[g])[0].astype(jnp.bfloat16) for g in groups]
    up_grads = [dot_tn(first_full, grad_preact[g]) for g in groups]
    up_bias_sums = [jnp.sum(grad_preact[g], axis=0, dtype=jnp.float32) for g in groups]
    grad_first = grad_second + scatter_cores(sum(dot_nt(grad_preact[g], up_ws[g]) for g in groups))
    first_gain_part = jnp.sum(grad_first * normed_first, axis=0)
    first_shift_part = jnp.sum(grad_first, axis=0)
    grad_residual = norm_backward(grad_first, normed_first, inverse_first, first_gain)
    output_bias_part = jnp.sum(grad_residual, axis=0)
    branch_grad_full = gather_cores(grad_residual)
    grad_mixed = [dot_nn(branch_grad_full, output_ws[g]).astype(jnp.bfloat16) for g in groups]
    output_grads = [dot_tn(branch_grad_full, mixed[g]) for g in groups]

    def place(parts, part_len, total_len):
        blank = jnp.zeros((total_len,), jnp.float32)
        for g in groups:
            blank = lax.dynamic_update_slice_in_dim(blank, parts[g], slices[g] * part_len, 0)
        return blank

    rows_block = width // n_data
    vec_block = width // n_all
    up_placed = place(up_bias_sums, hidden_cols, hidden_cols * n_tensor)
    up_columns = (
        up_placed.reshape(n_data, n_tensor, rows_block).transpose(0, 2, 1).reshape(width, n_tensor)
    )
    early_columns = jnp.concatenate(
        [
            jnp.stack(
                [
                    output_bias_part,
                    first_gain_part,
                    first_shift_part,
                    down_bias_part,
                    second_gain_part,
                    second_shift_part,
                ],
                axis=1,
            ),
            up_columns,
        ],
        axis=1,
    )
    early_columns = early_columns + to_core_partner(early_columns)
    early_own = jnp.concatenate([up_grads[0], down_grads[0], output_grads[0]], axis=1)
    early_partner = jnp.concatenate([up_grads[1], down_grads[1], output_grads[1]], axis=1)
    early_cols = early_own.shape[1]
    early_pack = jnp.concatenate([early_own, early_partner, early_columns], axis=1).astype(
        jnp.bfloat16
    )
    early_pack, grad_mixed = lax.optimization_barrier((early_pack, grad_mixed))
    early_reduced = lax.psum_scatter(
        early_pack, "dp", scatter_dimension=0, tiled=True
    ).astype(jnp.float32)
    early_sent = to_chip_partner(early_reduced[:, early_cols:].astype(jnp.bfloat16)).astype(
        jnp.float32
    )
    early_shard = early_reduced[:, :early_cols] + early_sent[:, :early_cols]
    early_small = early_reduced[:, 2 * early_cols :] + early_sent[:, early_cols:]
    up_shard = early_shard[:, :hidden_cols]
    down_shard = early_shard[:, hidden_cols : 2 * hidden_cols]
    output_shard = early_shard[:, 2 * hidden_cols :]

    grad_projected = [attend_back(projected[g], log_total[g], grad_mixed[g]) for g in groups]
    project_grads = [dot_tn(inputs_full, grad_projected[g]) for g in groups]
    qkv_bias_sums = [jnp.sum(grad_projected[g], axis=0, dtype=jnp.float32) for g in groups]
    grad_inputs = grad_residual + scatter_cores(
        sum(dot_nt(grad_projected[g], project_ws[g]) for g in groups)
    )

    late_columns = jnp.stack(
        [
            place([q[:head_cols] for q in qkv_bias_sums], head_cols, width),
            place([q[2 * head_cols :] for q in qkv_bias_sums], head_cols, width),
        ],
        axis=1,
    )
    late_columns = late_columns + to_core_partner(late_columns)
    late_own = jnp.concatenate([project_grads[0], late_columns], axis=1)
    late_partner = jnp.concatenate([project_grads[1], late_columns], axis=1)
    late_total = late_own + to_chip_partner(late_partner.astype(jnp.bfloat16)).astype(jnp.float32)
    late_shard = scatter_dp_permutes(late_total)
    project_shard = late_shard[:, :project_cols]

    def mine_of(column):
        return lax.dynamic_slice_in_dim(column, tensor_index * vec_block, vec_block)

    early = [mine_of(early_small[:, k]) for k in range(6)]
    up_bias_shard = lax.dynamic_index_in_dim(early_small[:, 6:], tensor_index, axis=1, keepdims=False)
    late = [mine_of(late_shard[:, project_cols + k]) for k in range(2)]
    small = [
        late[0],
        late[1],
        early[0],
        early[1],
        early[2],
        up_bias_shard,
        early[3],
        early[4],
        early[5],
    ]

    grad_low = grad_inputs.astype(jnp.bfloat16)
    grad_other = to_chip_partner(grad_low[block_rows:])
    grad_own = grad_low[:block_rows]
    grad_here = jnp.stack(
        [jnp.where(on_left, grad_own, grad_other), jnp.where(on_left, grad_other, grad_own)],
        axis=1,
    )
    returned = lax.all_to_all(grad_here, "dp", split_axis=0, concat_axis=1, tiled=True)
    tokens_grad = jnp.einsum(
        "qs,pqd->psd", placing, returned, preferred_element_type=jnp.float32
    ).astype(jnp.bfloat16)

    return (
        layer_output,
        tokens_grad,
        project_shard,
        small[0],
        small[1],
        output_shard,
        small[2],
        small[3],
        small[4],
        up_shard,
        small[5],
        down_shard,
        small[6],
        small[7],
        small[8],
    )


def solution(mesh):
    in_specs = (
        P(("dp", "tensor"), None, None),
        P(),
        P(),
        P("dp", "tensor"),
        P(),
        P(),
        P("dp", "tensor"),
        P(),
        P(),
        P(),
        P("dp", "tensor"),
        P(),
        P("dp", "tensor"),
        P(),
        P(),
        P(),
        P(("dp", "tensor"), None, None),
    )
    out_specs = (
        P("tensor", "dp", None),
        P(("dp", "tensor"), None, None),
        P("dp", "tensor"),
        P(("dp", "tensor")),
        P(("dp", "tensor")),
        P("dp", "tensor"),
        P(("dp", "tensor")),
        P(("dp", "tensor")),
        P(("dp", "tensor")),
        P("dp", "tensor"),
        P(("dp", "tensor")),
        P("dp", "tensor"),
        P(("dp", "tensor")),
        P(("dp", "tensor")),
        P(("dp", "tensor")),
    )
    return jax.shard_map(
        on_device, mesh=mesh, in_specs=in_specs, out_specs=out_specs, check_vma=False
    )
```

```python
from functools import partial

import jax
import jax.numpy as jnp
from jax import lax
from jax.sharding import PartitionSpec as P

HD = 64


EPSILON = 1e-12
MASKED = -1e30


def norm_forward(value, gain, shift):
    centred = value - jnp.mean(value, axis=-1, keepdims=True)
    inverse = lax.rsqrt(jnp.mean(centred * centred, axis=-1, keepdims=True) + EPSILON)
    normed = centred * inverse
    return (normed * gain + shift, normed, inverse)


def norm_backward(upstream, normed, inverse, gain):
    scaled = upstream * gain
    first_mean = jnp.mean(scaled, axis=-1, keepdims=True)
    second_mean = jnp.mean(scaled * normed, axis=-1, keepdims=True)
    return inverse * (scaled - first_mean - normed * second_mean)


def dot_nt(a, b):
    return lax.dot_general(a, b, (((1,), (1,)), ((), ())), preferred_element_type=jnp.float32)


def dot_tn(a, b):
    return lax.dot_general(a, b, (((0,), (0,)), ((), ())), preferred_element_type=jnp.float32)


def dot_nn(a, b):
    return jnp.dot(a, b, preferred_element_type=jnp.float32)


def on_device(
    tokens,
    lengths,
    dealing,
    project_weight,
    query_projection_bias,
    value_projection_bias,
    attention_output_weight,
    attention_output_bias,
    first_gain,
    first_shift,
    feed_input_weight,
    feed_input_bias,
    feed_output_weight,
    feed_output_bias,
    second_gain,
    second_shift,
    output_grad,
):
    n_data = lax.axis_size("dp")
    n_tensor = lax.axis_size("tensor")
    n_all = n_data * n_tensor
    data_index = lax.axis_index("dp")
    tensor_index = lax.axis_index("tensor")
    seq_total = dealing.shape[0]
    seq_here = seq_total // n_data
    assert n_tensor == 4 and seq_here == 2
    piece_rows = tokens.shape[0]
    block_rows = piece_rows * n_data
    seq_rows = block_rows * n_tensor
    half_rows = seq_rows // 2
    width = tokens.shape[2]
    head_cols = attention_output_weight.shape[1]
    heads_here = head_cols // HD
    hidden_cols = feed_input_weight.shape[1]
    project_cols = project_weight.shape[1]
    score_scale = HD ** (-0.5)

    chip_side = tensor_index // 2
    core = tensor_index % 2
    partner_slice = tensor_index ^ 2
    across_chips = [(k, k ^ 2) for k in range(n_tensor)]
    across_cores = [(k, k ^ 1) for k in range(n_tensor)]

    def to_chip_partner(value):
        return lax.ppermute(value, "tensor", across_chips)

    def to_core_partner(value):
        return lax.ppermute(value, "tensor", across_cores)

    def gather_dp(block):
        return lax.all_gather(block, "dp", axis=0, tiled=True)

    def scatter_dp(total):
        return lax.psum_scatter(
            total.astype(jnp.bfloat16), "dp", scatter_dimension=0, tiled=True
        ).astype(jnp.float32)

    def gather_dp_permutes(block):
        if n_data > 8:
            return gather_dp(block)
        got = [block] + [
            lax.ppermute(block, "dp", [(j, (j + k) % n_data) for j in range(n_data)])
            for k in range(1, n_data)
        ]
        stacked = jnp.stack(got)
        ordered = jnp.take(stacked, (data_index - jnp.arange(n_data)) % n_data, axis=0)
        return ordered.reshape(n_data * block.shape[0], *block.shape[1:])

    def scatter_dp_permutes(total):
        if n_data > 8:
            return scatter_dp(total)
        pieces = total.astype(jnp.bfloat16).reshape(n_data, -1, *total.shape[1:])
        acc = lax.dynamic_index_in_dim(
            total.reshape(pieces.shape), data_index, 0, keepdims=False
        )
        for k in range(1, n_data):
            sent = lax.dynamic_index_in_dim(pieces, (data_index + k) % n_data, 0, keepdims=False)
            acc = acc + lax.ppermute(
                sent, "dp", [(j, (j + k) % n_data) for j in range(n_data)]
            ).astype(jnp.float32)
        return acc

    def gather_cores(mine):
        low = mine.astype(jnp.bfloat16)
        return jnp.concatenate([low, to_core_partner(low)], axis=0)

    def scatter_cores(partial_sum):
        sent = to_core_partner(partial_sum[half_rows:].astype(jnp.bfloat16))
        return partial_sum[:half_rows] + sent.astype(jnp.float32)

    slot_ids = jnp.arange(seq_total, dtype=jnp.int32)
    placing = (dealing[None, :] == slot_ids[:, None]).astype(jnp.bfloat16)
    def deal(values):
        sent = jnp.einsum(
            "qs,psd->pqd", placing, values, preferred_element_type=jnp.float32
        ).astype(jnp.bfloat16)
        here = lax.all_to_all(sent, "dp", split_axis=1, concat_axis=0, tiled=True)
        slot_mine = lax.dynamic_index_in_dim(here, chip_side, axis=1, keepdims=False)
        slot_other = lax.dynamic_index_in_dim(here, 1 - chip_side, axis=1, keepdims=False)
        return jnp.concatenate([slot_mine, to_chip_partner(slot_other)], axis=0)

    inputs_mine = deal(tokens)
    cot_mine = deal(output_grad)
    inputs_full = jnp.concatenate([inputs_mine, to_core_partner(inputs_mine)], axis=0)

    my_slot = data_index * seq_here + chip_side
    seq_length = jnp.sum(jnp.where(dealing == my_slot, lengths, 0))
    blocks = jnp.stack(
        [
            tensor_index,
            partner_slice,
            tensor_index ^ 1,
            partner_slice ^ 1,
        ]
    )
    row_ids = jnp.arange(seq_rows, dtype=jnp.int32)
    owner = blocks[row_ids // block_rows]
    inner = row_ids % block_rows
    position = (inner // piece_rows * n_tensor + owner) * piece_rows + inner % piece_rows
    key_valid = position < seq_length

    attn_w = jnp.concatenate([project_weight, attention_output_weight], axis=1)
    feed_w = jnp.concatenate([feed_input_weight, feed_output_weight], axis=1)
    attn_own = gather_dp_permutes(attn_w)
    feed_w, attn_own = lax.optimization_barrier((feed_w, attn_own))
    feed_own = gather_dp(feed_w)
    attn_part = to_chip_partner(attn_own)
    feed_part = to_chip_partner(feed_own)
    slices = (tensor_index, partner_slice)
    attn_sets = (attn_own, attn_part)
    feed_sets = (feed_own, feed_part)
    project_ws = [a[:, :project_cols] for a in attn_sets]
    output_ws = [a[:, project_cols:] for a in attn_sets]
    up_ws = [f[:, :hidden_cols] for f in feed_sets]
    down_ws = [f[:, hidden_cols:] for f in feed_sets]

    def project_bias(k):
        query_part = lax.dynamic_slice_in_dim(query_projection_bias, k * head_cols, head_cols)
        value_part = lax.dynamic_slice_in_dim(value_projection_bias, k * head_cols, head_cols)
        return jnp.concatenate([query_part, jnp.zeros_like(query_part), value_part])

    project_biases = [project_bias(k) for k in slices]
    up_biases = [
        lax.dynamic_slice_in_dim(feed_input_bias, k * hidden_cols, hidden_cols) for k in slices
    ]

    def split_heads(qkv_block):
        query_rows = qkv_block[:, :head_cols].reshape(seq_rows, heads_here, HD)
        key_rows = qkv_block[:, head_cols : 2 * head_cols].reshape(seq_rows, heads_here, HD)
        value_rows = qkv_block[:, 2 * head_cols :].reshape(seq_rows, heads_here, HD)
        return (query_rows, key_rows, value_rows)

    def masked_scores(query_rows, key_rows):
        raw_scores = (
            jnp.einsum("qhe,khe->hqk", query_rows, key_rows, preferred_element_type=jnp.float32)
            * score_scale
        )
        return jnp.where(key_valid[None, None, :], raw_scores, MASKED)

    def attend(qkv_block):
        query_rows, key_rows, value_rows = split_heads(qkv_block)
        scores = masked_scores(query_rows, key_rows)
        row_max = jnp.max(scores, axis=-1, keepdims=True)
        exponent = jnp.exp(scores - row_max)
        row_total = jnp.sum(exponent, axis=-1, keepdims=True)
        weights = (exponent / row_total).astype(jnp.bfloat16)
        mixed_heads = jnp.einsum(
            "hqk,khe->qhe", weights, value_rows, preferred_element_type=jnp.float32
        )
        return (
            mixed_heads.reshape(seq_rows, head_cols).astype(jnp.bfloat16),
            (row_max + jnp.log(row_total))[..., 0],
        )

    def attend_back(qkv_block, row_lse, grad_block):
        query_rows, key_rows, value_rows = split_heads(qkv_block)
        weights = jnp.exp(masked_scores(query_rows, key_rows) - row_lse[..., None])
        grad_heads = grad_block.reshape(seq_rows, heads_here, HD)
        grad_weights = jnp.einsum(
            "qhe,khe->hqk", grad_heads, value_rows, preferred_element_type=jnp.float32
        )
        inner_sum = jnp.sum(weights * grad_weights, axis=-1, keepdims=True)
        grad_scores = (weights * (grad_weights - inner_sum)).astype(jnp.bfloat16)
        grad_query = (
            jnp.einsum("hqk,khe->qhe", grad_scores, key_rows, preferred_element_type=jnp.float32)
            * score_scale
        )
        grad_key = (
            jnp.einsum("hqk,qhe->khe", grad_scores, query_rows, preferred_element_type=jnp.float32)
            * score_scale
        )
        grad_value = jnp.einsum(
            "hqk,qhe->khe", weights.astype(jnp.bfloat16), grad_heads,
            preferred_element_type=jnp.float32,
        )
        joined = jnp.concatenate(
            [
                grad_query.reshape(seq_rows, head_cols),
                grad_key.reshape(seq_rows, head_cols),
                grad_value.reshape(seq_rows, head_cols),
            ],
            axis=-1,
        )
        return joined.astype(jnp.bfloat16)

    gelu_exact = partial(jax.nn.gelu, approximate=False)
    groups = range(2)

    projected = [
        (dot_nn(inputs_full, project_ws[g]) + project_biases[g]).astype(jnp.bfloat16)
        for g in groups
    ]
    attended = [attend(projected[g]) for g in groups]
    mixed = [a[0] for a in attended]
    log_total = [a[1] for a in attended]
    branch = scatter_cores(sum(dot_nt(mixed[g], output_ws[g]) for g in groups))
    first, normed_first, inverse_first = norm_forward(
        inputs_mine.astype(jnp.float32) + branch + attention_output_bias, first_gain, first_shift
    )
    first_full = gather_cores(first)
    preact = [dot_nn(first_full, up_ws[g]) + up_biases[g] for g in groups]
    gelu_pairs = [jax.vjp(gelu_exact, preact[g]) for g in groups]
    hidden = [p[0].astype(jnp.bfloat16) for p in gelu_pairs]
    feed = scatter_cores(sum(dot_nt(hidden[g], down_ws[g]) for g in groups))
    second, normed_second, inverse_second = norm_forward(
        first + feed + feed_output_bias, second_gain, second_shift
    )
    out_mine = second.astype(jnp.bfloat16)
    out_other = to_chip_partner(out_mine[block_rows:])
    out_own = out_mine[:block_rows]
    on_left = chip_side == 0
    layer_output = jnp.stack(
        [jnp.where(on_left, out_own, out_other), jnp.where(on_left, out_other, out_own)], axis=1
    )

    cot = cot_mine.astype(jnp.float32)
    second_gain_part = jnp.sum(cot * normed_second, axis=0)
    second_shift_part = jnp.sum(cot, axis=0)
    grad_second = norm_backward(cot, normed_second, inverse_second, second_gain)
    down_bias_part = jnp.sum(grad_second, axis=0)
    grad_feed_full = gather_cores(grad_second)
    grad_hidden = [dot_nn(grad_feed_full, down_ws[g]) for g in groups]
    down_grads = [dot_tn(grad_feed_full, hidden[g]) for g in groups]
    grad_preact = [gelu_pairs[g][1](grad_hidden[g])[0].astype(jnp.bfloat16) for g in groups]
    up_grads = [dot_tn(first_full, grad_preact[g]) for g in groups]
    up_bias_sums = [jnp.sum(grad_preact[g], axis=0, dtype=jnp.float32) for g in groups]
    grad_first = grad_second + scatter_cores(sum(dot_nt(grad_preact[g], up_ws[g]) for g in groups))
    first_gain_part = jnp.sum(grad_first * normed_first, axis=0)
    first_shift_part = jnp.sum(grad_first, axis=0)
    grad_residual = norm_backward(grad_first, normed_first, inverse_first, first_gain)
    output_bias_part = jnp.sum(grad_residual, axis=0)
    branch_grad_full = gather_cores(grad_residual)
    grad_mixed = [dot_nn(branch_grad_full, output_ws[g]).astype(jnp.bfloat16) for g in groups]
    output_grads = [dot_tn(branch_grad_full, mixed[g]) for g in groups]

    def place(parts, part_len, total_len):
        blank = jnp.zeros((total_len,), jnp.float32)
        for g in groups:
            blank = lax.dynamic_update_slice_in_dim(blank, parts[g], slices[g] * part_len, 0)
        return blank

    rows_block = width // n_data
    vec_block = width // n_all
    up_placed = place(up_bias_sums, hidden_cols, hidden_cols * n_tensor)
    up_columns = (
        up_placed.reshape(n_data, n_tensor, rows_block).transpose(0, 2, 1).reshape(width, n_tensor)
    )
    early_columns = jnp.concatenate(
        [
            jnp.stack(
                [
                    output_bias_part,
                    first_gain_part,
                    first_shift_part,
                    down_bias_part,
                    second_gain_part,
                    second_shift_part,
                ],
                axis=1,
            ),
            up_columns,
        ],
        axis=1,
    )
    early_columns = early_columns + to_core_partner(early_columns)
    early_own = jnp.concatenate([up_grads[0], down_grads[0], output_grads[0]], axis=1)
    early_partner = jnp.concatenate([up_grads[1], down_grads[1], output_grads[1]], axis=1)
    early_cols = early_own.shape[1]
    early_pack = jnp.concatenate([early_own, early_partner, early_columns], axis=1).astype(
        jnp.bfloat16
    )
    early_pack, grad_mixed = lax.optimization_barrier((early_pack, grad_mixed))
    early_reduced = lax.psum_scatter(
        early_pack, "dp", scatter_dimension=0, tiled=True
    ).astype(jnp.float32)
    early_sent = to_chip_partner(early_reduced[:, early_cols:].astype(jnp.bfloat16)).astype(
        jnp.float32
    )
    early_shard = early_reduced[:, :early_cols] + early_sent[:, :early_cols]
    early_small = early_reduced[:, 2 * early_cols :] + early_sent[:, early_cols:]
    up_shard = early_shard[:, :hidden_cols]
    down_shard = early_shard[:, hidden_cols : 2 * hidden_cols]
    output_shard = early_shard[:, 2 * hidden_cols :]

    grad_projected = [attend_back(projected[g], log_total[g], grad_mixed[g]) for g in groups]
    project_grads = [dot_tn(inputs_full, grad_projected[g]) for g in groups]
    qkv_bias_sums = [jnp.sum(grad_projected[g], axis=0, dtype=jnp.float32) for g in groups]
    grad_inputs = grad_residual + scatter_cores(
        sum(dot_nt(grad_projected[g], project_ws[g]) for g in groups)
    )

    late_columns = jnp.stack(
        [
            place([q[:head_cols] for q in qkv_bias_sums], head_cols, width),
            place([q[2 * head_cols :] for q in qkv_bias_sums], head_cols, width),
        ],
        axis=1,
    )
    late_columns = late_columns + to_core_partner(late_columns)
    late_own = jnp.concatenate([project_grads[0], late_columns], axis=1)
    late_partner = jnp.concatenate([project_grads[1], late_columns], axis=1)
    late_total = late_own + to_chip_partner(late_partner.astype(jnp.bfloat16)).astype(jnp.float32)
    late_shard = scatter_dp_permutes(late_total)
    project_shard = late_shard[:, :project_cols]

    def mine_of(column):
        return lax.dynamic_slice_in_dim(column, tensor_index * vec_block, vec_block)

    early = [mine_of(early_small[:, k]) for k in range(6)]
    up_bias_shard = lax.dynamic_index_in_dim(early_small[:, 6:], tensor_index, axis=1, keepdims=False)
    late = [mine_of(late_shard[:, project_cols + k]) for k in range(2)]
    small = [
        late[0],
        late[1],
        early[0],
        early[1],
        early[2],
        up_bias_shard,
        early[3],
        early[4],
        early[5],
    ]

    grad_low = grad_inputs.astype(jnp.bfloat16)
    grad_other = to_chip_partner(grad_low[block_rows:])
    grad_own = grad_low[:block_rows]
    grad_here = jnp.stack(
        [jnp.where(on_left, grad_own, grad_other), jnp.where(on_left, grad_other, grad_own)],
        axis=1,
    )
    returned = lax.all_to_all(grad_here, "dp", split_axis=0, concat_axis=1, tiled=True)
    tokens_grad = jnp.einsum(
        "qs,pqd->psd", placing, returned, preferred_element_type=jnp.float32
    ).astype(jnp.bfloat16)

    return (
        layer_output,
        tokens_grad,
        project_shard,
        small[0],
        small[1],
        output_shard,
        small[2],
        small[3],
        small[4],
        up_shard,
        small[5],
        down_shard,
        small[6],
        small[7],
        small[8],
    )


def solution(mesh):
    in_specs = (
        P(("dp", "tensor"), None, None),
        P(),
        P(),
        P("dp", "tensor"),
        P(),
        P(),
        P("dp", "tensor"),
        P(),
        P(),
        P(),
        P("dp", "tensor"),
        P(),
        P("dp", "tensor"),
        P(),
        P(),
        P(),
        P(("dp", "tensor"), None, None),
    )
    out_specs = (
        P("tensor", "dp", None),
        P(("dp", "tensor"), None, None),
        P("dp", "tensor"),
        P(("dp", "tensor")),
        P(("dp", "tensor")),
        P("dp", "tensor"),
        P(("dp", "tensor")),
        P(("dp", "tensor")),
        P(("dp", "tensor")),
        P("dp", "tensor"),
        P(("dp", "tensor")),
        P("dp", "tensor"),
        P(("dp", "tensor")),
        P(("dp", "tensor")),
        P(("dp", "tensor")),
    )
    return jax.shard_map(
        on_device, mesh=mesh, in_specs=in_specs, out_specs=out_specs, check_vma=False
    )
```

```python
from functools import partial

import jax
import jax.numpy as jnp
from jax import lax
from jax.sharding import PartitionSpec as P

HD = 64


EPSILON = 1e-12
MASKED = -1e30


def norm_forward(value, gain, shift):
    centred = value - jnp.mean(value, axis=-1, keepdims=True)
    inverse = lax.rsqrt(jnp.mean(centred * centred, axis=-1, keepdims=True) + EPSILON)
    normed = centred * inverse
    return (normed * gain + shift, normed, inverse)


def norm_backward(upstream, normed, inverse, gain):
    scaled = upstream * gain
    first_mean = jnp.mean(scaled, axis=-1, keepdims=True)
    second_mean = jnp.mean(scaled * normed, axis=-1, keepdims=True)
    return inverse * (scaled - first_mean - normed * second_mean)


def dot_nt(a, b):
    return lax.dot_general(a, b, (((1,), (1,)), ((), ())), preferred_element_type=jnp.float32)


def dot_tn(a, b):
    return lax.dot_general(a, b, (((0,), (0,)), ((), ())), preferred_element_type=jnp.float32)


def dot_nn(a, b):
    return jnp.dot(a, b, preferred_element_type=jnp.float32)


def on_device(
    tokens,
    lengths,
    dealing,
    project_weight,
    query_projection_bias,
    value_projection_bias,
    attention_output_weight,
    attention_output_bias,
    first_gain,
    first_shift,
    feed_input_weight,
    feed_input_bias,
    feed_output_weight,
    feed_output_bias,
    second_gain,
    second_shift,
    output_grad,
):
    n_data = lax.axis_size("dp")
    n_tensor = lax.axis_size("tensor")
    n_all = n_data * n_tensor
    data_index = lax.axis_index("dp")
    tensor_index = lax.axis_index("tensor")
    seq_total = dealing.shape[0]
    seq_here = seq_total // n_data
    assert n_tensor == 4 and seq_here == 2
    piece_rows = tokens.shape[0]
    block_rows = piece_rows * n_data
    seq_rows = block_rows * n_tensor
    half_rows = seq_rows // 2
    width = tokens.shape[2]
    head_cols = attention_output_weight.shape[1]
    heads_here = head_cols // HD
    hidden_cols = feed_input_weight.shape[1]
    project_cols = project_weight.shape[1]
    score_scale = HD ** (-0.5)

    chip_side = tensor_index // 2
    core = tensor_index % 2
    partner_slice = tensor_index ^ 2
    across_chips = [(k, k ^ 2) for k in range(n_tensor)]
    across_cores = [(k, k ^ 1) for k in range(n_tensor)]

    def to_chip_partner(value):
        return lax.ppermute(value, "tensor", across_chips)

    def to_core_partner(value):
        return lax.ppermute(value, "tensor", across_cores)

    def gather_dp(block):
        return lax.all_gather(block, "dp", axis=0, tiled=True)

    def scatter_dp(total):
        return lax.psum_scatter(
            total.astype(jnp.bfloat16), "dp", scatter_dimension=0, tiled=True
        ).astype(jnp.float32)

    def scatter_dp_permutes(total):
        if n_data > 8:
            return scatter_dp(total)
        pieces = total.astype(jnp.bfloat16).reshape(n_data, -1, *total.shape[1:])
        acc = lax.dynamic_index_in_dim(
            total.reshape(pieces.shape), data_index, 0, keepdims=False
        )
        for k in range(1, n_data):
            sent = lax.dynamic_index_in_dim(pieces, (data_index + k) % n_data, 0, keepdims=False)
            acc = acc + lax.ppermute(
                sent, "dp", [(j, (j + k) % n_data) for j in range(n_data)]
            ).astype(jnp.float32)
        return acc

    def scatter_dp_halving(total):
        if n_data != 8:
            return scatter_dp(total)
        y_bit = data_index % 2
        z_low = (data_index // 2) % 2
        z_high = data_index // 4
        perms = {
            "y": [(j, j ^ 1) for j in range(8)],
            "z1": [(j, j ^ 2) for j in range(8)],
            "z2": [(j, j ^ 4) for j in range(8)],
        }
        bits = {"y": y_bit, "z1": z_low, "z2": z_high}
        axis_of = {"z2": 0, "z1": 1, "y": 2}

        def run(part, order):
            cols = part.shape[1]
            acc = part.reshape(2, 2, 2, rows_block, cols)
            left = ["z2", "z1", "y"]
            for stage in order:
                k = left.index(stage)
                bit = bits[stage]
                keep = lax.dynamic_index_in_dim(acc, bit, axis=k, keepdims=False)
                send = lax.dynamic_index_in_dim(acc, 1 - bit, axis=k, keepdims=False)
                got = lax.ppermute(send.astype(jnp.bfloat16), "dp", perms[stage])
                acc = keep.astype(jnp.float32) + got.astype(jnp.float32)
                left.remove(stage)
            return acc

        split = min(total.shape[1], max(128, (total.shape[1] // 2) // 128 * 128))
        first = run(total[:, :split], ("y", "z1", "z2"))
        if split == total.shape[1]:
            return first
        second = run(total[:, split:], ("z1", "z2", "y"))
        return jnp.concatenate([first, second], axis=1)

    def gather_cores(mine):
        low = mine.astype(jnp.bfloat16)
        return jnp.concatenate([low, to_core_partner(low)], axis=0)

    def scatter_cores(partial_sum):
        sent = to_core_partner(partial_sum[half_rows:].astype(jnp.bfloat16))
        return partial_sum[:half_rows] + sent.astype(jnp.float32)

    slot_ids = jnp.arange(seq_total, dtype=jnp.int32)
    placing = (dealing[None, :] == slot_ids[:, None]).astype(jnp.bfloat16)
    def deal(values):
        sent = jnp.einsum(
            "qs,psd->pqd", placing, values, preferred_element_type=jnp.float32
        ).astype(jnp.bfloat16)
        here = lax.all_to_all(sent, "dp", split_axis=1, concat_axis=0, tiled=True)
        slot_mine = lax.dynamic_index_in_dim(here, chip_side, axis=1, keepdims=False)
        slot_other = lax.dynamic_index_in_dim(here, 1 - chip_side, axis=1, keepdims=False)
        return jnp.concatenate([slot_mine, to_chip_partner(slot_other)], axis=0)

    inputs_mine = deal(tokens)
    cot_mine = deal(output_grad)
    inputs_full = jnp.concatenate([inputs_mine, to_core_partner(inputs_mine)], axis=0)

    my_slot = data_index * seq_here + chip_side
    seq_length = jnp.sum(jnp.where(dealing == my_slot, lengths, 0))
    blocks = jnp.stack(
        [
            tensor_index,
            partner_slice,
            tensor_index ^ 1,
            partner_slice ^ 1,
        ]
    )
    row_ids = jnp.arange(seq_rows, dtype=jnp.int32)
    owner = blocks[row_ids // block_rows]
    inner = row_ids % block_rows
    position = (inner // piece_rows * n_tensor + owner) * piece_rows + inner % piece_rows
    key_valid = position < seq_length

    attn_w = jnp.concatenate([project_weight, attention_output_weight], axis=1)
    feed_w = jnp.concatenate([feed_input_weight, feed_output_weight], axis=1)
    attn_own = gather_dp(attn_w)
    feed_own = gather_dp(feed_w)
    attn_part = to_chip_partner(attn_own)
    feed_part = to_chip_partner(feed_own)
    slices = (tensor_index, partner_slice)
    attn_sets = (attn_own, attn_part)
    feed_sets = (feed_own, feed_part)
    project_ws = [a[:, :project_cols] for a in attn_sets]
    output_ws = [a[:, project_cols:] for a in attn_sets]
    up_ws = [f[:, :hidden_cols] for f in feed_sets]
    down_ws = [f[:, hidden_cols:] for f in feed_sets]

    def project_bias(k):
        query_part = lax.dynamic_slice_in_dim(query_projection_bias, k * head_cols, head_cols)
        value_part = lax.dynamic_slice_in_dim(value_projection_bias, k * head_cols, head_cols)
        return jnp.concatenate([query_part, jnp.zeros_like(query_part), value_part])

    project_biases = [project_bias(k) for k in slices]
    up_biases = [
        lax.dynamic_slice_in_dim(feed_input_bias, k * hidden_cols, hidden_cols) for k in slices
    ]

    def split_heads(qkv_block):
        query_rows = qkv_block[:, :head_cols].reshape(seq_rows, heads_here, HD)
        key_rows = qkv_block[:, head_cols : 2 * head_cols].reshape(seq_rows, heads_here, HD)
        value_rows = qkv_block[:, 2 * head_cols :].reshape(seq_rows, heads_here, HD)
        return (query_rows, key_rows, value_rows)

    def masked_scores(query_rows, key_rows):
        raw_scores = (
            jnp.einsum("qhe,khe->hqk", query_rows, key_rows, preferred_element_type=jnp.float32)
            * score_scale
        )
        return jnp.where(key_valid[None, None, :], raw_scores, MASKED)

    def attend(qkv_block):
        query_rows, key_rows, value_rows = split_heads(qkv_block)
        scores = masked_scores(query_rows, key_rows)
        row_max = jnp.max(scores, axis=-1, keepdims=True)
        exponent = jnp.exp(scores - row_max)
        row_total = jnp.sum(exponent, axis=-1, keepdims=True)
        weights = (exponent / row_total).astype(jnp.bfloat16)
        mixed_heads = jnp.einsum(
            "hqk,khe->qhe", weights, value_rows, preferred_element_type=jnp.float32
        )
        return (
            mixed_heads.reshape(seq_rows, head_cols).astype(jnp.bfloat16),
            (row_max + jnp.log(row_total))[..., 0],
        )

    def attend_back(qkv_block, row_lse, grad_block):
        query_rows, key_rows, value_rows = split_heads(qkv_block)
        weights = jnp.exp(masked_scores(query_rows, key_rows) - row_lse[..., None])
        grad_heads = grad_block.reshape(seq_rows, heads_here, HD)
        grad_weights = jnp.einsum(
            "qhe,khe->hqk", grad_heads, value_rows, preferred_element_type=jnp.float32
        )
        inner_sum = jnp.sum(weights * grad_weights, axis=-1, keepdims=True)
        grad_scores = (weights * (grad_weights - inner_sum)).astype(jnp.bfloat16)
        grad_query = (
            jnp.einsum("hqk,khe->qhe", grad_scores, key_rows, preferred_element_type=jnp.float32)
            * score_scale
        )
        grad_key = (
            jnp.einsum("hqk,qhe->khe", grad_scores, query_rows, preferred_element_type=jnp.float32)
            * score_scale
        )
        grad_value = jnp.einsum(
            "hqk,qhe->khe", weights.astype(jnp.bfloat16), grad_heads,
            preferred_element_type=jnp.float32,
        )
        joined = jnp.concatenate(
            [
                grad_query.reshape(seq_rows, head_cols),
                grad_key.reshape(seq_rows, head_cols),
                grad_value.reshape(seq_rows, head_cols),
            ],
            axis=-1,
        )
        return joined.astype(jnp.bfloat16)

    gelu_exact = partial(jax.nn.gelu, approximate=False)
    groups = range(2)

    projected = [
        (dot_nn(inputs_full, project_ws[g]) + project_biases[g]).astype(jnp.bfloat16)
        for g in groups
    ]
    attended = [attend(projected[g]) for g in groups]
    mixed = [a[0] for a in attended]
    log_total = [a[1] for a in attended]
    branch = scatter_cores(sum(dot_nt(mixed[g], output_ws[g]) for g in groups))
    first, normed_first, inverse_first = norm_forward(
        inputs_mine.astype(jnp.float32) + branch + attention_output_bias, first_gain, first_shift
    )
    first_full = gather_cores(first)
    preact = [dot_nn(first_full, up_ws[g]) + up_biases[g] for g in groups]
    gelu_pairs = [jax.vjp(gelu_exact, preact[g]) for g in groups]
    hidden = [p[0].astype(jnp.bfloat16) for p in gelu_pairs]
    feed = scatter_cores(sum(dot_nt(hidden[g], down_ws[g]) for g in groups))
    second, normed_second, inverse_second = norm_forward(
        first + feed + feed_output_bias, second_gain, second_shift
    )
    out_mine = second.astype(jnp.bfloat16)
    out_other = to_chip_partner(out_mine[block_rows:])
    out_own = out_mine[:block_rows]
    on_left = chip_side == 0
    layer_output = jnp.stack(
        [jnp.where(on_left, out_own, out_other), jnp.where(on_left, out_other, out_own)], axis=1
    )

    cot = cot_mine.astype(jnp.float32)
    second_gain_part = jnp.sum(cot * normed_second, axis=0)
    second_shift_part = jnp.sum(cot, axis=0)
    grad_second = norm_backward(cot, normed_second, inverse_second, second_gain)
    down_bias_part = jnp.sum(grad_second, axis=0)
    grad_feed_full = gather_cores(grad_second)
    grad_hidden = [dot_nn(grad_feed_full, down_ws[g]) for g in groups]
    down_grads = [dot_tn(grad_feed_full, hidden[g]) for g in groups]
    grad_preact = [gelu_pairs[g][1](grad_hidden[g])[0].astype(jnp.bfloat16) for g in groups]
    up_grads = [dot_tn(first_full, grad_preact[g]) for g in groups]
    up_bias_sums = [jnp.sum(grad_preact[g], axis=0, dtype=jnp.float32) for g in groups]
    grad_first = grad_second + scatter_cores(sum(dot_nt(grad_preact[g], up_ws[g]) for g in groups))
    first_gain_part = jnp.sum(grad_first * normed_first, axis=0)
    first_shift_part = jnp.sum(grad_first, axis=0)
    grad_residual = norm_backward(grad_first, normed_first, inverse_first, first_gain)
    output_bias_part = jnp.sum(grad_residual, axis=0)
    branch_grad_full = gather_cores(grad_residual)
    grad_mixed = [dot_nn(branch_grad_full, output_ws[g]).astype(jnp.bfloat16) for g in groups]
    output_grads = [dot_tn(branch_grad_full, mixed[g]) for g in groups]

    def place(parts, part_len, total_len):
        blank = jnp.zeros((total_len,), jnp.float32)
        for g in groups:
            blank = lax.dynamic_update_slice_in_dim(blank, parts[g], slices[g] * part_len, 0)
        return blank

    rows_block = width // n_data
    vec_block = width // n_all
    up_placed = place(up_bias_sums, hidden_cols, hidden_cols * n_tensor)
    up_columns = (
        up_placed.reshape(n_data, n_tensor, rows_block).transpose(0, 2, 1).reshape(width, n_tensor)
    )
    early_columns = jnp.concatenate(
        [
            jnp.stack(
                [
                    output_bias_part,
                    first_gain_part,
                    first_shift_part,
                    down_bias_part,
                    second_gain_part,
                    second_shift_part,
                ],
                axis=1,
            ),
            up_columns,
        ],
        axis=1,
    )
    early_columns = early_columns + to_core_partner(early_columns)
    early_own = jnp.concatenate([up_grads[0], down_grads[0], output_grads[0]], axis=1)
    early_partner = jnp.concatenate([up_grads[1], down_grads[1], output_grads[1]], axis=1)
    early_cols = early_own.shape[1]
    early_pack = jnp.concatenate([early_own, early_partner, early_columns], axis=1).astype(
        jnp.bfloat16
    )
    early_pack, grad_mixed = lax.optimization_barrier((early_pack, grad_mixed))
    early_reduced = scatter_dp_halving(early_pack)
    early_sent = to_chip_partner(early_reduced[:, early_cols:].astype(jnp.bfloat16)).astype(
        jnp.float32
    )
    early_shard = early_reduced[:, :early_cols] + early_sent[:, :early_cols]
    early_small = early_reduced[:, 2 * early_cols :] + early_sent[:, early_cols:]
    up_shard = early_shard[:, :hidden_cols]
    down_shard = early_shard[:, hidden_cols : 2 * hidden_cols]
    output_shard = early_shard[:, 2 * hidden_cols :]

    grad_projected = [attend_back(projected[g], log_total[g], grad_mixed[g]) for g in groups]
    project_grads = [dot_tn(inputs_full, grad_projected[g]) for g in groups]
    qkv_bias_sums = [jnp.sum(grad_projected[g], axis=0, dtype=jnp.float32) for g in groups]
    grad_inputs = grad_residual + scatter_cores(
        sum(dot_nt(grad_projected[g], project_ws[g]) for g in groups)
    )

    late_columns = jnp.stack(
        [
            place([q[:head_cols] for q in qkv_bias_sums], head_cols, width),
            place([q[2 * head_cols :] for q in qkv_bias_sums], head_cols, width),
        ],
        axis=1,
    )
    late_columns = late_columns + to_core_partner(late_columns)
    late_own = jnp.concatenate([project_grads[0], late_columns], axis=1)
    late_partner = jnp.concatenate([project_grads[1], late_columns], axis=1)
    late_total = late_own + to_chip_partner(late_partner.astype(jnp.bfloat16)).astype(jnp.float32)
    late_shard = scatter_dp_permutes(late_total)
    project_shard = late_shard[:, :project_cols]

    def mine_of(column):
        return lax.dynamic_slice_in_dim(column, tensor_index * vec_block, vec_block)

    early = [mine_of(early_small[:, k]) for k in range(6)]
    up_bias_shard = lax.dynamic_index_in_dim(early_small[:, 6:], tensor_index, axis=1, keepdims=False)
    late = [mine_of(late_shard[:, project_cols + k]) for k in range(2)]
    small = [
        late[0],
        late[1],
        early[0],
        early[1],
        early[2],
        up_bias_shard,
        early[3],
        early[4],
        early[5],
    ]

    grad_low = grad_inputs.astype(jnp.bfloat16)
    grad_other = to_chip_partner(grad_low[block_rows:])
    grad_own = grad_low[:block_rows]
    grad_here = jnp.stack(
        [jnp.where(on_left, grad_own, grad_other), jnp.where(on_left, grad_other, grad_own)],
        axis=1,
    )
    returned = lax.all_to_all(grad_here, "dp", split_axis=0, concat_axis=1, tiled=True)
    tokens_grad = jnp.einsum(
        "qs,pqd->psd", placing, returned, preferred_element_type=jnp.float32
    ).astype(jnp.bfloat16)

    return (
        layer_output,
        tokens_grad,
        project_shard,
        small[0],
        small[1],
        output_shard,
        small[2],
        small[3],
        small[4],
        up_shard,
        small[5],
        down_shard,
        small[6],
        small[7],
        small[8],
    )


def solution(mesh):
    in_specs = (
        P(("dp", "tensor"), None, None),
        P(),
        P(),
        P("dp", "tensor"),
        P(),
        P(),
        P("dp", "tensor"),
        P(),
        P(),
        P(),
        P("dp", "tensor"),
        P(),
        P("dp", "tensor"),
        P(),
        P(),
        P(),
        P(("dp", "tensor"), None, None),
    )
    out_specs = (
        P("tensor", "dp", None),
        P(("dp", "tensor"), None, None),
        P("dp", "tensor"),
        P(("dp", "tensor")),
        P(("dp", "tensor")),
        P("dp", "tensor"),
        P(("dp", "tensor")),
        P(("dp", "tensor")),
        P(("dp", "tensor")),
        P("dp", "tensor"),
        P(("dp", "tensor")),
        P("dp", "tensor"),
        P(("dp", "tensor")),
        P(("dp", "tensor")),
        P(("dp", "tensor")),
    )
    return jax.shard_map(
        on_device, mesh=mesh, in_specs=in_specs, out_specs=out_specs, check_vma=False
    )
```

```python
from functools import partial

import jax
import jax.numpy as jnp
from jax import lax
from jax.sharding import PartitionSpec as P

HD = 64


EPSILON = 1e-12
MASKED = -1e30


def norm_forward(value, gain, shift):
    centred = value - jnp.mean(value, axis=-1, keepdims=True)
    inverse = lax.rsqrt(jnp.mean(centred * centred, axis=-1, keepdims=True) + EPSILON)
    normed = centred * inverse
    return (normed * gain + shift, normed, inverse)


def norm_backward(upstream, normed, inverse, gain):
    scaled = upstream * gain
    first_mean = jnp.mean(scaled, axis=-1, keepdims=True)
    second_mean = jnp.mean(scaled * normed, axis=-1, keepdims=True)
    return inverse * (scaled - first_mean - normed * second_mean)


def dot_nt(a, b):
    return lax.dot_general(a, b, (((1,), (1,)), ((), ())), preferred_element_type=jnp.float32)


def dot_tn(a, b):
    return lax.dot_general(a, b, (((0,), (0,)), ((), ())), preferred_element_type=jnp.float32)


def dot_nn(a, b):
    return jnp.dot(a, b, preferred_element_type=jnp.float32)


def on_device(
    tokens,
    lengths,
    dealing,
    project_weight,
    query_projection_bias,
    value_projection_bias,
    attention_output_weight,
    attention_output_bias,
    first_gain,
    first_shift,
    feed_input_weight,
    feed_input_bias,
    feed_output_weight,
    feed_output_bias,
    second_gain,
    second_shift,
    output_grad,
):
    n_data = lax.axis_size("dp")
    n_tensor = lax.axis_size("tensor")
    n_all = n_data * n_tensor
    data_index = lax.axis_index("dp")
    tensor_index = lax.axis_index("tensor")
    seq_total = dealing.shape[0]
    seq_here = seq_total // n_data
    assert n_tensor == 4 and seq_here == 2
    piece_rows = tokens.shape[0]
    block_rows = piece_rows * n_data
    seq_rows = block_rows * n_tensor
    half_rows = seq_rows // 2
    width = tokens.shape[2]
    head_cols = attention_output_weight.shape[1]
    heads_here = head_cols // HD
    hidden_cols = feed_input_weight.shape[1]
    project_cols = project_weight.shape[1]
    score_scale = HD ** (-0.5)

    chip_side = tensor_index // 2
    core = tensor_index % 2
    partner_slice = tensor_index ^ 2
    across_chips = [(k, k ^ 2) for k in range(n_tensor)]
    across_cores = [(k, k ^ 1) for k in range(n_tensor)]

    def to_chip_partner(value):
        return lax.ppermute(value, "tensor", across_chips)

    def to_core_partner(value):
        return lax.ppermute(value, "tensor", across_cores)

    def gather_dp(block):
        return lax.all_gather(block, "dp", axis=0, tiled=True)

    def scatter_dp(total):
        return lax.psum_scatter(
            total.astype(jnp.bfloat16), "dp", scatter_dimension=0, tiled=True
        ).astype(jnp.float32)

    def scatter_dp_permutes(total):
        if n_data > 8:
            return scatter_dp(total)
        pieces = total.astype(jnp.bfloat16).reshape(n_data, -1, *total.shape[1:])
        acc = lax.dynamic_index_in_dim(
            total.reshape(pieces.shape), data_index, 0, keepdims=False
        )
        for k in range(1, n_data):
            sent = lax.dynamic_index_in_dim(pieces, (data_index + k) % n_data, 0, keepdims=False)
            acc = acc + lax.ppermute(
                sent, "dp", [(j, (j + k) % n_data) for j in range(n_data)]
            ).astype(jnp.float32)
        return acc

    def gather_cores(mine):
        low = mine.astype(jnp.bfloat16)
        return jnp.concatenate([low, to_core_partner(low)], axis=0)

    def scatter_cores(partial_sum):
        sent = to_core_partner(partial_sum[half_rows:].astype(jnp.bfloat16))
        return partial_sum[:half_rows] + sent.astype(jnp.float32)

    slot_ids = jnp.arange(seq_total, dtype=jnp.int32)
    placing = (dealing[None, :] == slot_ids[:, None]).astype(jnp.bfloat16)
    def deal(values):
        sent = jnp.einsum(
            "qs,psd->pqd", placing, values, preferred_element_type=jnp.float32
        ).astype(jnp.bfloat16)
        here = lax.all_to_all(sent, "dp", split_axis=1, concat_axis=0, tiled=True)
        slot_mine = lax.dynamic_index_in_dim(here, chip_side, axis=1, keepdims=False)
        slot_other = lax.dynamic_index_in_dim(here, 1 - chip_side, axis=1, keepdims=False)
        return jnp.concatenate([slot_mine, to_chip_partner(slot_other)], axis=0)

    inputs_mine = deal(tokens)
    cot_mine = deal(output_grad)
    inputs_full = jnp.concatenate([inputs_mine, to_core_partner(inputs_mine)], axis=0)

    my_slot = data_index * seq_here + chip_side
    seq_length = jnp.sum(jnp.where(dealing == my_slot, lengths, 0))
    blocks = jnp.stack(
        [
            tensor_index,
            partner_slice,
            tensor_index ^ 1,
            partner_slice ^ 1,
        ]
    )
    row_ids = jnp.arange(seq_rows, dtype=jnp.int32)
    owner = blocks[row_ids // block_rows]
    inner = row_ids % block_rows
    position = (inner // piece_rows * n_tensor + owner) * piece_rows + inner % piece_rows
    key_valid = position < seq_length

    attn_w = jnp.concatenate([project_weight, attention_output_weight], axis=1)
    feed_w = jnp.concatenate([feed_input_weight, feed_output_weight], axis=1)
    attn_own = gather_dp(attn_w)
    feed_own = gather_dp(feed_w)
    attn_part = to_chip_partner(attn_own)
    feed_part = to_chip_partner(feed_own)
    slices = (tensor_index, partner_slice)
    attn_sets = (attn_own, attn_part)
    feed_sets = (feed_own, feed_part)
    project_ws = [a[:, :project_cols] for a in attn_sets]
    output_ws = [a[:, project_cols:] for a in attn_sets]
    up_ws = [f[:, :hidden_cols] for f in feed_sets]
    down_ws = [f[:, hidden_cols:] for f in feed_sets]

    def project_bias(k):
        query_part = lax.dynamic_slice_in_dim(query_projection_bias, k * head_cols, head_cols)
        value_part = lax.dynamic_slice_in_dim(value_projection_bias, k * head_cols, head_cols)
        return jnp.concatenate([query_part, jnp.zeros_like(query_part), value_part])

    project_biases = [project_bias(k) for k in slices]
    up_biases = [
        lax.dynamic_slice_in_dim(feed_input_bias, k * hidden_cols, hidden_cols) for k in slices
    ]

    def split_heads(qkv_block):
        query_rows = qkv_block[:, :head_cols].reshape(seq_rows, heads_here, HD)
        key_rows = qkv_block[:, head_cols : 2 * head_cols].reshape(seq_rows, heads_here, HD)
        value_rows = qkv_block[:, 2 * head_cols :].reshape(seq_rows, heads_here, HD)
        return (query_rows, key_rows, value_rows)

    def masked_scores(query_rows, key_rows):
        raw_scores = (
            jnp.einsum("qhe,khe->hqk", query_rows, key_rows, preferred_element_type=jnp.float32)
            * score_scale
        )
        return jnp.where(key_valid[None, None, :], raw_scores, MASKED)

    def attend(qkv_block):
        query_rows, key_rows, value_rows = split_heads(qkv_block)
        scores = masked_scores(query_rows, key_rows)
        row_max = jnp.max(scores, axis=-1, keepdims=True)
        exponent = jnp.exp(scores - row_max)
        row_total = jnp.sum(exponent, axis=-1, keepdims=True)
        weights = (exponent / row_total).astype(jnp.bfloat16)
        mixed_heads = jnp.einsum(
            "hqk,khe->qhe", weights, value_rows, preferred_element_type=jnp.float32
        )
        return (
            mixed_heads.reshape(seq_rows, head_cols).astype(jnp.bfloat16),
            (row_max + jnp.log(row_total))[..., 0],
        )

    def attend_back(qkv_block, row_lse, grad_block):
        query_rows, key_rows, value_rows = split_heads(qkv_block)
        weights = jnp.exp(masked_scores(query_rows, key_rows) - row_lse[..., None])
        grad_heads = grad_block.reshape(seq_rows, heads_here, HD)
        grad_weights = jnp.einsum(
            "qhe,khe->hqk", grad_heads, value_rows, preferred_element_type=jnp.float32
        )
        inner_sum = jnp.sum(weights * grad_weights, axis=-1, keepdims=True)
        grad_scores = (weights * (grad_weights - inner_sum)).astype(jnp.bfloat16)
        grad_query = (
            jnp.einsum("hqk,khe->qhe", grad_scores, key_rows, preferred_element_type=jnp.float32)
            * score_scale
        )
        grad_key = (
            jnp.einsum("hqk,qhe->khe", grad_scores, query_rows, preferred_element_type=jnp.float32)
            * score_scale
        )
        grad_value = jnp.einsum(
            "hqk,qhe->khe", weights.astype(jnp.bfloat16), grad_heads,
            preferred_element_type=jnp.float32,
        )
        joined = jnp.concatenate(
            [
                grad_query.reshape(seq_rows, head_cols),
                grad_key.reshape(seq_rows, head_cols),
                grad_value.reshape(seq_rows, head_cols),
            ],
            axis=-1,
        )
        return joined.astype(jnp.bfloat16)

    gelu_exact = partial(jax.nn.gelu, approximate=False)
    groups = range(2)

    projected = [
        (dot_nn(inputs_full, project_ws[g]) + project_biases[g]).astype(jnp.bfloat16)
        for g in groups
    ]
    attended = [attend(projected[g]) for g in groups]
    mixed = [a[0] for a in attended]
    log_total = [a[1] for a in attended]
    branch = scatter_cores(sum(dot_nt(mixed[g], output_ws[g]) for g in groups))
    first, normed_first, inverse_first = norm_forward(
        inputs_mine.astype(jnp.float32) + branch + attention_output_bias, first_gain, first_shift
    )
    first_full = gather_cores(first)
    preact = [dot_nn(first_full, up_ws[g]) + up_biases[g] for g in groups]
    gelu_pairs = [jax.vjp(gelu_exact, preact[g]) for g in groups]
    hidden = [p[0].astype(jnp.bfloat16) for p in gelu_pairs]
    feed = scatter_cores(sum(dot_nt(hidden[g], down_ws[g]) for g in groups))
    second, normed_second, inverse_second = norm_forward(
        first + feed + feed_output_bias, second_gain, second_shift
    )
    out_mine = second.astype(jnp.bfloat16)
    out_other = to_chip_partner(out_mine[block_rows:])
    out_own = out_mine[:block_rows]
    on_left = chip_side == 0
    layer_output = jnp.stack(
        [jnp.where(on_left, out_own, out_other), jnp.where(on_left, out_other, out_own)], axis=1
    )

    cot = cot_mine.astype(jnp.float32)
    second_gain_part = jnp.sum(cot * normed_second, axis=0)
    second_shift_part = jnp.sum(cot, axis=0)
    grad_second = norm_backward(cot, normed_second, inverse_second, second_gain)
    down_bias_part = jnp.sum(grad_second, axis=0)
    grad_feed_full = gather_cores(grad_second)
    grad_hidden = [dot_nn(grad_feed_full, down_ws[g]) for g in groups]
    down_grads = [dot_tn(grad_feed_full, hidden[g]) for g in groups]
    grad_preact = [gelu_pairs[g][1](grad_hidden[g])[0].astype(jnp.bfloat16) for g in groups]
    up_grads = [dot_tn(first_full, grad_preact[g]) for g in groups]
    up_bias_sums = [jnp.sum(grad_preact[g], axis=0, dtype=jnp.float32) for g in groups]
    feed_own_grad = jnp.concatenate([up_grads[0], down_grads[0]], axis=1)
    feed_partner_grad = jnp.concatenate([up_grads[1], down_grads[1]], axis=1)
    early_cols = feed_own_grad.shape[1]
    early_pack = jnp.concatenate([feed_own_grad, feed_partner_grad], axis=1).astype(jnp.bfloat16)
    first_partial = sum(dot_nt(grad_preact[g], up_ws[g]) for g in groups)
    early_pack, first_partial = lax.optimization_barrier((early_pack, first_partial))
    early_reduced = lax.psum_scatter(
        early_pack, "dp", scatter_dimension=0, tiled=True
    ).astype(jnp.float32)
    early_sent = to_chip_partner(early_reduced[:, early_cols:].astype(jnp.bfloat16)).astype(
        jnp.float32
    )
    early_shard = early_reduced[:, :early_cols] + early_sent
    up_shard = early_shard[:, :hidden_cols]
    down_shard = early_shard[:, hidden_cols:]
    grad_first = grad_second + scatter_cores(first_partial)
    first_gain_part = jnp.sum(grad_first * normed_first, axis=0)
    first_shift_part = jnp.sum(grad_first, axis=0)
    grad_residual = norm_backward(grad_first, normed_first, inverse_first, first_gain)
    output_bias_part = jnp.sum(grad_residual, axis=0)
    branch_grad_full = gather_cores(grad_residual)
    grad_mixed = [dot_nn(branch_grad_full, output_ws[g]).astype(jnp.bfloat16) for g in groups]
    output_grads = [dot_tn(branch_grad_full, mixed[g]) for g in groups]

    def place(parts, part_len, total_len):
        blank = jnp.zeros((total_len,), jnp.float32)
        for g in groups:
            blank = lax.dynamic_update_slice_in_dim(blank, parts[g], slices[g] * part_len, 0)
        return blank

    rows_block = width // n_data
    vec_block = width // n_all
    up_placed = place(up_bias_sums, hidden_cols, hidden_cols * n_tensor)
    up_columns = (
        up_placed.reshape(n_data, n_tensor, rows_block).transpose(0, 2, 1).reshape(width, n_tensor)
    )
    early_columns = jnp.concatenate(
        [
            jnp.stack(
                [
                    output_bias_part,
                    first_gain_part,
                    first_shift_part,
                    down_bias_part,
                    second_gain_part,
                    second_shift_part,
                ],
                axis=1,
            ),
            up_columns,
        ],
        axis=1,
    )
    early_columns = early_columns + to_core_partner(early_columns)

    grad_projected = [attend_back(projected[g], log_total[g], grad_mixed[g]) for g in groups]
    project_grads = [dot_tn(inputs_full, grad_projected[g]) for g in groups]
    qkv_bias_sums = [jnp.sum(grad_projected[g], axis=0, dtype=jnp.float32) for g in groups]
    grad_inputs = grad_residual + scatter_cores(
        sum(dot_nt(grad_projected[g], project_ws[g]) for g in groups)
    )

    late_columns = jnp.stack(
        [
            place([q[:head_cols] for q in qkv_bias_sums], head_cols, width),
            place([q[2 * head_cols :] for q in qkv_bias_sums], head_cols, width),
        ],
        axis=1,
    )
    late_columns = late_columns + to_core_partner(late_columns)
    small_columns = jnp.concatenate([early_columns, late_columns], axis=1)
    late_own = jnp.concatenate([project_grads[0], output_grads[0], small_columns], axis=1)
    late_partner = jnp.concatenate([project_grads[1], output_grads[1], small_columns], axis=1)
    late_total = late_own + to_chip_partner(late_partner.astype(jnp.bfloat16)).astype(jnp.float32)
    late_shard = scatter_dp_permutes(late_total)
    project_shard = late_shard[:, :project_cols]
    output_shard = late_shard[:, project_cols : project_cols + head_cols]
    early_at = project_cols + head_cols
    early_small = late_shard[:, early_at : early_at + early_columns.shape[1]]
    late_small = late_shard[:, early_at + early_columns.shape[1] :]

    def mine_of(column):
        return lax.dynamic_slice_in_dim(column, tensor_index * vec_block, vec_block)

    early = [mine_of(early_small[:, k]) for k in range(6)]
    up_bias_shard = lax.dynamic_index_in_dim(early_small[:, 6:], tensor_index, axis=1, keepdims=False)
    late = [mine_of(late_small[:, k]) for k in range(2)]
    small = [
        late[0],
        late[1],
        early[0],
        early[1],
        early[2],
        up_bias_shard,
        early[3],
        early[4],
        early[5],
    ]

    grad_low = grad_inputs.astype(jnp.bfloat16)
    grad_other = to_chip_partner(grad_low[block_rows:])
    grad_own = grad_low[:block_rows]
    grad_here = jnp.stack(
        [jnp.where(on_left, grad_own, grad_other), jnp.where(on_left, grad_other, grad_own)],
        axis=1,
    )
    returned = lax.all_to_all(grad_here, "dp", split_axis=0, concat_axis=1, tiled=True)
    tokens_grad = jnp.einsum(
        "qs,pqd->psd", placing, returned, preferred_element_type=jnp.float32
    ).astype(jnp.bfloat16)

    return (
        layer_output,
        tokens_grad,
        project_shard,
        small[0],
        small[1],
        output_shard,
        small[2],
        small[3],
        small[4],
        up_shard,
        small[5],
        down_shard,
        small[6],
        small[7],
        small[8],
    )


def solution(mesh):
    in_specs = (
        P(("dp", "tensor"), None, None),
        P(),
        P(),
        P("dp", "tensor"),
        P(),
        P(),
        P("dp", "tensor"),
        P(),
        P(),
        P(),
        P("dp", "tensor"),
        P(),
        P("dp", "tensor"),
        P(),
        P(),
        P(),
        P(("dp", "tensor"), None, None),
    )
    out_specs = (
        P("tensor", "dp", None),
        P(("dp", "tensor"), None, None),
        P("dp", "tensor"),
        P(("dp", "tensor")),
        P(("dp", "tensor")),
        P("dp", "tensor"),
        P(("dp", "tensor")),
        P(("dp", "tensor")),
        P(("dp", "tensor")),
        P("dp", "tensor"),
        P(("dp", "tensor")),
        P("dp", "tensor"),
        P(("dp", "tensor")),
        P(("dp", "tensor")),
        P(("dp", "tensor")),
    )
    return jax.shard_map(
        on_device, mesh=mesh, in_specs=in_specs, out_specs=out_specs, check_vma=False
    )
```

```python
from functools import partial

import jax
import jax.numpy as jnp
from jax import lax
from jax.experimental.layout import Layout, with_layout_constraint
from jax.sharding import PartitionSpec as P

HD = 64


EPSILON = 1e-12
MASKED = -1e30


def norm_forward(value, gain, shift):
    centred = value - jnp.mean(value, axis=-1, keepdims=True)
    inverse = lax.rsqrt(jnp.mean(centred * centred, axis=-1, keepdims=True) + EPSILON)
    normed = centred * inverse
    return (normed * gain + shift, normed, inverse)


def norm_backward(upstream, normed, inverse, gain):
    scaled = upstream * gain
    first_mean = jnp.mean(scaled, axis=-1, keepdims=True)
    second_mean = jnp.mean(scaled * normed, axis=-1, keepdims=True)
    return inverse * (scaled - first_mean - normed * second_mean)


def dot_nt(a, b):
    return lax.dot_general(a, b, (((1,), (1,)), ((), ())), preferred_element_type=jnp.float32)


def dot_tn(a, b):
    return lax.dot_general(a, b, (((0,), (0,)), ((), ())), preferred_element_type=jnp.float32)


def dot_rows(a, b):
    return with_layout_constraint(dot_tn(a, b), Layout(major_to_minor=(0, 1)))


def dot_nn(a, b):
    return jnp.dot(a, b, preferred_element_type=jnp.float32)


def on_device(
    tokens,
    lengths,
    dealing,
    project_weight,
    query_projection_bias,
    value_projection_bias,
    attention_output_weight,
    attention_output_bias,
    first_gain,
    first_shift,
    feed_input_weight,
    feed_input_bias,
    feed_output_weight,
    feed_output_bias,
    second_gain,
    second_shift,
    output_grad,
):
    n_data = lax.axis_size("dp")
    n_tensor = lax.axis_size("tensor")
    n_all = n_data * n_tensor
    data_index = lax.axis_index("dp")
    tensor_index = lax.axis_index("tensor")
    seq_total = dealing.shape[0]
    seq_here = seq_total // n_data
    assert n_tensor == 4 and seq_here == 2
    piece_rows = tokens.shape[0]
    block_rows = piece_rows * n_data
    seq_rows = block_rows * n_tensor
    half_rows = seq_rows // 2
    width = tokens.shape[2]
    head_cols = attention_output_weight.shape[1]
    heads_here = head_cols // HD
    hidden_cols = feed_input_weight.shape[1]
    project_cols = project_weight.shape[1]
    score_scale = HD ** (-0.5)

    chip_side = tensor_index // 2
    core = tensor_index % 2
    partner_slice = tensor_index ^ 2
    across_chips = [(k, k ^ 2) for k in range(n_tensor)]
    across_cores = [(k, k ^ 1) for k in range(n_tensor)]

    def to_chip_partner(value):
        return lax.ppermute(value, "tensor", across_chips)

    def to_core_partner(value):
        return lax.ppermute(value, "tensor", across_cores)

    def gather_dp(block):
        return lax.all_gather(block, "dp", axis=0, tiled=True)

    def scatter_dp(total):
        return lax.psum_scatter(
            total.astype(jnp.bfloat16), "dp", scatter_dimension=0, tiled=True
        ).astype(jnp.float32)

    def scatter_dp_permutes(total):
        if n_data > 8:
            return scatter_dp(total)
        pieces = total.astype(jnp.bfloat16).reshape(n_data, -1, *total.shape[1:])
        acc = lax.dynamic_index_in_dim(
            total.reshape(pieces.shape), data_index, 0, keepdims=False
        )
        for k in range(1, n_data):
            sent = lax.dynamic_index_in_dim(pieces, (data_index + k) % n_data, 0, keepdims=False)
            acc = acc + lax.ppermute(
                sent, "dp", [(j, (j + k) % n_data) for j in range(n_data)]
            ).astype(jnp.float32)
        return acc

    def gather_cores(mine):
        low = mine.astype(jnp.bfloat16)
        return jnp.concatenate([low, to_core_partner(low)], axis=0)

    def scatter_cores(partial_sum):
        sent = to_core_partner(partial_sum[half_rows:].astype(jnp.bfloat16))
        return partial_sum[:half_rows] + sent.astype(jnp.float32)

    slot_ids = jnp.arange(seq_total, dtype=jnp.int32)
    placing = (dealing[None, :] == slot_ids[:, None]).astype(jnp.bfloat16)
    def deal(values):
        sent = jnp.einsum(
            "qs,psd->pqd", placing, values, preferred_element_type=jnp.float32
        ).astype(jnp.bfloat16)
        here = lax.all_to_all(sent, "dp", split_axis=1, concat_axis=0, tiled=True)
        slot_mine = lax.dynamic_index_in_dim(here, chip_side, axis=1, keepdims=False)
        slot_other = lax.dynamic_index_in_dim(here, 1 - chip_side, axis=1, keepdims=False)
        return jnp.concatenate([slot_mine, to_chip_partner(slot_other)], axis=0)

    inputs_mine = deal(tokens)
    cot_mine = deal(output_grad)
    inputs_full = jnp.concatenate([inputs_mine, to_core_partner(inputs_mine)], axis=0)

    my_slot = data_index * seq_here + chip_side
    seq_length = jnp.sum(jnp.where(dealing == my_slot, lengths, 0))
    blocks = jnp.stack(
        [
            tensor_index,
            partner_slice,
            tensor_index ^ 1,
            partner_slice ^ 1,
        ]
    )
    row_ids = jnp.arange(seq_rows, dtype=jnp.int32)
    owner = blocks[row_ids // block_rows]
    inner = row_ids % block_rows
    position = (inner // piece_rows * n_tensor + owner) * piece_rows + inner % piece_rows
    key_valid = position < seq_length

    attn_w = jnp.concatenate([project_weight, attention_output_weight], axis=1)
    feed_w = jnp.concatenate([feed_input_weight, feed_output_weight], axis=1)
    attn_own = gather_dp(attn_w)
    feed_own = gather_dp(feed_w)
    attn_part = to_chip_partner(attn_own)
    feed_part = to_chip_partner(feed_own)
    slices = (tensor_index, partner_slice)
    attn_sets = (attn_own, attn_part)
    feed_sets = (feed_own, feed_part)
    project_ws = [a[:, :project_cols] for a in attn_sets]
    output_ws = [a[:, project_cols:] for a in attn_sets]
    up_ws = [f[:, :hidden_cols] for f in feed_sets]
    down_ws = [f[:, hidden_cols:] for f in feed_sets]

    def project_bias(k):
        query_part = lax.dynamic_slice_in_dim(query_projection_bias, k * head_cols, head_cols)
        value_part = lax.dynamic_slice_in_dim(value_projection_bias, k * head_cols, head_cols)
        return jnp.concatenate([query_part, jnp.zeros_like(query_part), value_part])

    project_biases = [project_bias(k) for k in slices]
    up_biases = [
        lax.dynamic_slice_in_dim(feed_input_bias, k * hidden_cols, hidden_cols) for k in slices
    ]

    def split_heads(qkv_block):
        query_rows = qkv_block[:, :head_cols].reshape(seq_rows, heads_here, HD)
        key_rows = qkv_block[:, head_cols : 2 * head_cols].reshape(seq_rows, heads_here, HD)
        value_rows = qkv_block[:, 2 * head_cols :].reshape(seq_rows, heads_here, HD)
        return (query_rows, key_rows, value_rows)

    def masked_scores(query_rows, key_rows):
        raw_scores = (
            jnp.einsum("qhe,khe->hqk", query_rows, key_rows, preferred_element_type=jnp.float32)
            * score_scale
        )
        return jnp.where(key_valid[None, None, :], raw_scores, MASKED)

    def attend(qkv_block):
        query_rows, key_rows, value_rows = split_heads(qkv_block)
        scores = masked_scores(query_rows, key_rows)
        row_max = jnp.max(scores, axis=-1, keepdims=True)
        exponent = jnp.exp(scores - row_max)
        row_total = jnp.sum(exponent, axis=-1, keepdims=True)
        weights = (exponent / row_total).astype(jnp.bfloat16)
        mixed_heads = jnp.einsum(
            "hqk,khe->qhe", weights, value_rows, preferred_element_type=jnp.float32
        )
        return (
            mixed_heads.reshape(seq_rows, head_cols).astype(jnp.bfloat16),
            (row_max + jnp.log(row_total))[..., 0],
        )

    def attend_back(qkv_block, row_lse, grad_block):
        query_rows, key_rows, value_rows = split_heads(qkv_block)
        weights = jnp.exp(masked_scores(query_rows, key_rows) - row_lse[..., None])
        grad_heads = grad_block.reshape(seq_rows, heads_here, HD)
        grad_weights = jnp.einsum(
            "qhe,khe->hqk", grad_heads, value_rows, preferred_element_type=jnp.float32
        )
        inner_sum = jnp.sum(weights * grad_weights, axis=-1, keepdims=True)
        grad_scores = (weights * (grad_weights - inner_sum)).astype(jnp.bfloat16)
        grad_query = (
            jnp.einsum("hqk,khe->qhe", grad_scores, key_rows, preferred_element_type=jnp.float32)
            * score_scale
        )
        grad_key = (
            jnp.einsum("hqk,qhe->khe", grad_scores, query_rows, preferred_element_type=jnp.float32)
            * score_scale
        )
        grad_value = jnp.einsum(
            "hqk,qhe->khe", weights.astype(jnp.bfloat16), grad_heads,
            preferred_element_type=jnp.float32,
        )
        joined = jnp.concatenate(
            [
                grad_query.reshape(seq_rows, head_cols),
                grad_key.reshape(seq_rows, head_cols),
                grad_value.reshape(seq_rows, head_cols),
            ],
            axis=-1,
        )
        return joined.astype(jnp.bfloat16)

    gelu_exact = partial(jax.nn.gelu, approximate=False)
    groups = range(2)

    projected = [
        (dot_nn(inputs_full, project_ws[g]) + project_biases[g]).astype(jnp.bfloat16)
        for g in groups
    ]
    attended = [attend(projected[g]) for g in groups]
    mixed = [a[0] for a in attended]
    log_total = [a[1] for a in attended]
    branch = scatter_cores(sum(dot_nt(mixed[g], output_ws[g]) for g in groups))
    first, normed_first, inverse_first = norm_forward(
        inputs_mine.astype(jnp.float32) + branch + attention_output_bias, first_gain, first_shift
    )
    first_full = gather_cores(first)
    preact = [dot_nn(first_full, up_ws[g]) + up_biases[g] for g in groups]
    gelu_pairs = [jax.vjp(gelu_exact, preact[g]) for g in groups]
    hidden = [p[0].astype(jnp.bfloat16) for p in gelu_pairs]
    feed = scatter_cores(sum(dot_nt(hidden[g], down_ws[g]) for g in groups))
    second, normed_second, inverse_second = norm_forward(
        first + feed + feed_output_bias, second_gain, second_shift
    )
    out_mine = second.astype(jnp.bfloat16)
    out_other = to_chip_partner(out_mine[block_rows:])
    out_own = out_mine[:block_rows]
    on_left = chip_side == 0
    layer_output = jnp.stack(
        [jnp.where(on_left, out_own, out_other), jnp.where(on_left, out_other, out_own)], axis=1
    )

    cot = cot_mine.astype(jnp.float32)
    second_gain_part = jnp.sum(cot * normed_second, axis=0)
    second_shift_part = jnp.sum(cot, axis=0)
    grad_second = norm_backward(cot, normed_second, inverse_second, second_gain)
    down_bias_part = jnp.sum(grad_second, axis=0)
    grad_feed_full = gather_cores(grad_second)
    grad_hidden = [dot_nn(grad_feed_full, down_ws[g]) for g in groups]
    down_grads = [dot_rows(grad_feed_full, hidden[g]) for g in groups]
    grad_preact = [gelu_pairs[g][1](grad_hidden[g])[0].astype(jnp.bfloat16) for g in groups]
    up_grads = [dot_rows(first_full, grad_preact[g]) for g in groups]
    up_bias_sums = [jnp.sum(grad_preact[g], axis=0, dtype=jnp.float32) for g in groups]
    grad_first = grad_second + scatter_cores(sum(dot_nt(grad_preact[g], up_ws[g]) for g in groups))
    first_gain_part = jnp.sum(grad_first * normed_first, axis=0)
    first_shift_part = jnp.sum(grad_first, axis=0)
    grad_residual = norm_backward(grad_first, normed_first, inverse_first, first_gain)
    output_bias_part = jnp.sum(grad_residual, axis=0)
    branch_grad_full = gather_cores(grad_residual)
    grad_mixed = [dot_nn(branch_grad_full, output_ws[g]).astype(jnp.bfloat16) for g in groups]
    output_grads = [dot_rows(branch_grad_full, mixed[g]) for g in groups]

    def place(parts, part_len, total_len):
        blank = jnp.zeros((total_len,), jnp.float32)
        for g in groups:
            blank = lax.dynamic_update_slice_in_dim(blank, parts[g], slices[g] * part_len, 0)
        return blank

    rows_block = width // n_data
    vec_block = width // n_all
    up_placed = place(up_bias_sums, hidden_cols, hidden_cols * n_tensor)
    up_columns = (
        up_placed.reshape(n_data, n_tensor, rows_block).transpose(0, 2, 1).reshape(width, n_tensor)
    )
    early_columns = jnp.concatenate(
        [
            jnp.stack(
                [
                    output_bias_part,
                    first_gain_part,
                    first_shift_part,
                    down_bias_part,
                    second_gain_part,
                    second_shift_part,
                ],
                axis=1,
            ),
            up_columns,
        ],
        axis=1,
    )
    early_columns = early_columns + to_core_partner(early_columns)
    early_own = jnp.concatenate([up_grads[0], down_grads[0], output_grads[0]], axis=1)
    early_partner = jnp.concatenate([up_grads[1], down_grads[1], output_grads[1]], axis=1)
    early_cols = early_own.shape[1]
    early_pack = jnp.concatenate([early_own, early_partner, early_columns], axis=1).astype(
        jnp.bfloat16
    )
    early_pack, grad_mixed = lax.optimization_barrier((early_pack, grad_mixed))
    early_reduced = lax.psum_scatter(
        early_pack, "dp", scatter_dimension=0, tiled=True
    ).astype(jnp.float32)
    early_sent = to_chip_partner(early_reduced[:, early_cols:].astype(jnp.bfloat16)).astype(
        jnp.float32
    )
    early_shard = early_reduced[:, :early_cols] + early_sent[:, :early_cols]
    early_small = early_reduced[:, 2 * early_cols :] + early_sent[:, early_cols:]
    up_shard = early_shard[:, :hidden_cols]
    down_shard = early_shard[:, hidden_cols : 2 * hidden_cols]
    output_shard = early_shard[:, 2 * hidden_cols :]

    grad_projected = [attend_back(projected[g], log_total[g], grad_mixed[g]) for g in groups]
    project_grads = [dot_tn(inputs_full, grad_projected[g]) for g in groups]
    qkv_bias_sums = [jnp.sum(grad_projected[g], axis=0, dtype=jnp.float32) for g in groups]
    grad_inputs = grad_residual + scatter_cores(
        sum(dot_nt(grad_projected[g], project_ws[g]) for g in groups)
    )

    late_columns = jnp.stack(
        [
            place([q[:head_cols] for q in qkv_bias_sums], head_cols, width),
            place([q[2 * head_cols :] for q in qkv_bias_sums], head_cols, width),
        ],
        axis=1,
    )
    late_columns = late_columns + to_core_partner(late_columns)
    late_own = jnp.concatenate([project_grads[0], late_columns], axis=1)
    late_partner = jnp.concatenate([project_grads[1], late_columns], axis=1)
    late_total = late_own + to_chip_partner(late_partner.astype(jnp.bfloat16)).astype(jnp.float32)
    late_shard = scatter_dp_permutes(late_total)
    project_shard = late_shard[:, :project_cols]

    def mine_of(column):
        return lax.dynamic_slice_in_dim(column, tensor_index * vec_block, vec_block)

    early = [mine_of(early_small[:, k]) for k in range(6)]
    up_bias_shard = lax.dynamic_index_in_dim(early_small[:, 6:], tensor_index, axis=1, keepdims=False)
    late = [mine_of(late_shard[:, project_cols + k]) for k in range(2)]
    small = [
        late[0],
        late[1],
        early[0],
        early[1],
        early[2],
        up_bias_shard,
        early[3],
        early[4],
        early[5],
    ]

    grad_low = grad_inputs.astype(jnp.bfloat16)
    grad_other = to_chip_partner(grad_low[block_rows:])
    grad_own = grad_low[:block_rows]
    grad_here = jnp.stack(
        [jnp.where(on_left, grad_own, grad_other), jnp.where(on_left, grad_other, grad_own)],
        axis=1,
    )
    returned = lax.all_to_all(grad_here, "dp", split_axis=0, concat_axis=1, tiled=True)
    tokens_grad = jnp.einsum(
        "qs,pqd->psd", placing, returned, preferred_element_type=jnp.float32
    ).astype(jnp.bfloat16)

    return (
        layer_output,
        tokens_grad,
        project_shard,
        small[0],
        small[1],
        output_shard,
        small[2],
        small[3],
        small[4],
        up_shard,
        small[5],
        down_shard,
        small[6],
        small[7],
        small[8],
    )


def solution(mesh):
    in_specs = (
        P(("dp", "tensor"), None, None),
        P(),
        P(),
        P("dp", "tensor"),
        P(),
        P(),
        P("dp", "tensor"),
        P(),
        P(),
        P(),
        P("dp", "tensor"),
        P(),
        P("dp", "tensor"),
        P(),
        P(),
        P(),
        P(("dp", "tensor"), None, None),
    )
    out_specs = (
        P("tensor", "dp", None),
        P(("dp", "tensor"), None, None),
        P("dp", "tensor"),
        P(("dp", "tensor")),
        P(("dp", "tensor")),
        P("dp", "tensor"),
        P(("dp", "tensor")),
        P(("dp", "tensor")),
        P(("dp", "tensor")),
        P("dp", "tensor"),
        P(("dp", "tensor")),
        P("dp", "tensor"),
        P(("dp", "tensor")),
        P(("dp", "tensor")),
        P(("dp", "tensor")),
    )
    return jax.shard_map(
        on_device, mesh=mesh, in_specs=in_specs, out_specs=out_specs, check_vma=False
    )
```

```python
from functools import partial

import jax
import jax.numpy as jnp
from jax import lax
from jax.sharding import PartitionSpec as P


HD = 64


EPSILON = 1e-12
MASKED = -1e30


def norm_forward(value, gain, shift):
    centred = value - jnp.mean(value, axis=-1, keepdims=True)
    inverse = lax.rsqrt(jnp.mean(centred * centred, axis=-1, keepdims=True) + EPSILON)
    normed = centred * inverse
    return (normed * gain + shift, normed, inverse)


def norm_backward(upstream, normed, inverse, gain):
    scaled = upstream * gain
    first_mean = jnp.mean(scaled, axis=-1, keepdims=True)
    second_mean = jnp.mean(scaled * normed, axis=-1, keepdims=True)
    return inverse * (scaled - first_mean - normed * second_mean)


def dot_nt(a, b):
    return lax.dot_general(a, b, (((1,), (1,)), ((), ())), preferred_element_type=jnp.float32)


def dot_tn(a, b):
    return lax.dot_general(a, b, (((0,), (0,)), ((), ())), preferred_element_type=jnp.float32)


def dot_nn(a, b):
    return jnp.dot(a, b, preferred_element_type=jnp.float32)


def on_device(
    tokens,
    lengths,
    dealing,
    project_weight,
    query_projection_bias,
    value_projection_bias,
    attention_output_weight,
    attention_output_bias,
    first_gain,
    first_shift,
    feed_input_weight,
    feed_input_bias,
    feed_output_weight,
    feed_output_bias,
    second_gain,
    second_shift,
    output_grad,
):
    n_data = lax.axis_size("dp")
    n_tensor = lax.axis_size("tensor")
    n_all = n_data * n_tensor
    data_index = lax.axis_index("dp")
    tensor_index = lax.axis_index("tensor")
    seq_total = dealing.shape[0]
    seq_here = seq_total // n_data
    assert n_tensor == 4 and seq_here == 2
    piece_rows = tokens.shape[0]
    block_rows = piece_rows * n_data
    seq_rows = block_rows * n_tensor
    half_rows = seq_rows // 2
    width = tokens.shape[2]
    head_cols = attention_output_weight.shape[1]
    heads_here = head_cols // HD
    hidden_cols = feed_input_weight.shape[1]
    project_cols = project_weight.shape[1]
    score_scale = HD ** (-0.5)

    chip_side = tensor_index // 2
    partner_slice = tensor_index ^ 2
    across_chips = [(k, k ^ 2) for k in range(n_tensor)]
    across_cores = [(k, k ^ 1) for k in range(n_tensor)]

    def to_chip_partner(value):
        return lax.ppermute(value, "tensor", across_chips)

    def to_core_partner(value):
        return lax.ppermute(value, "tensor", across_cores)

    def gather_dp(block):
        return lax.all_gather(block, "dp", axis=0, tiled=True)

    def scatter_dp(total):
        return lax.psum_scatter(
            total.astype(jnp.bfloat16), "dp", scatter_dimension=0, tiled=True
        ).astype(jnp.float32)

    def scatter_dp_permutes(total):
        if n_data > 8:
            return scatter_dp(total)
        pieces = total.astype(jnp.bfloat16).reshape(n_data, -1, *total.shape[1:])
        acc = lax.dynamic_index_in_dim(
            total.reshape(pieces.shape), data_index, 0, keepdims=False
        )
        for k in range(1, n_data):
            sent = lax.dynamic_index_in_dim(pieces, (data_index + k) % n_data, 0, keepdims=False)
            acc = acc + lax.ppermute(
                sent, "dp", [(j, (j + k) % n_data) for j in range(n_data)]
            ).astype(jnp.float32)
        return acc

    def gather_cores(mine):
        low = mine.astype(jnp.bfloat16)
        return jnp.concatenate([low, to_core_partner(low)], axis=0)

    def scatter_cores(partial_sum):
        sent = to_core_partner(partial_sum[half_rows:].astype(jnp.bfloat16))
        return partial_sum[:half_rows] + sent.astype(jnp.float32)

    slot_ids = jnp.arange(seq_total, dtype=jnp.int32)
    placing = (dealing[None, :] == slot_ids[:, None]).astype(jnp.bfloat16)

    def deal(values, after=None):
        sent = jnp.einsum(
            "qs,psd->pqd", placing, values, preferred_element_type=jnp.float32
        ).astype(jnp.bfloat16)
        if after is not None:
            sent, after = lax.optimization_barrier((sent, after))
        here = lax.all_to_all(sent, "dp", split_axis=1, concat_axis=0, tiled=True)
        slot_mine = lax.dynamic_index_in_dim(here, chip_side, axis=1, keepdims=False)
        slot_other = lax.dynamic_index_in_dim(here, 1 - chip_side, axis=1, keepdims=False)
        crossed = to_chip_partner(slot_other)
        return jnp.concatenate([slot_mine, crossed], axis=0)

    inputs_mine = deal(tokens)
    inputs_full = jnp.concatenate([inputs_mine, to_core_partner(inputs_mine)], axis=0)

    my_slot = data_index * seq_here + chip_side
    seq_length = jnp.sum(jnp.where(dealing == my_slot, lengths, 0))
    blocks = jnp.stack(
        [
            tensor_index,
            partner_slice,
            tensor_index ^ 1,
            partner_slice ^ 1,
        ]
    )
    row_ids = jnp.arange(seq_rows, dtype=jnp.int32)
    owner = blocks[row_ids // block_rows]
    inner = row_ids % block_rows
    position = (inner // piece_rows * n_tensor + owner) * piece_rows + inner % piece_rows
    key_valid = position < seq_length

    attn_w = jnp.concatenate([project_weight, attention_output_weight], axis=1)
    feed_w = jnp.concatenate([feed_input_weight, feed_output_weight], axis=1)
    attn_own = gather_dp(attn_w)
    feed_own = gather_dp(feed_w)
    attn_part = to_chip_partner(attn_own)
    feed_part = to_chip_partner(feed_own)
    cot_mine = deal(output_grad, feed_own)
    slices = (tensor_index, partner_slice)
    attn_sets = (attn_own, attn_part)
    feed_sets = (feed_own, feed_part)
    project_ws = [a[:, :project_cols] for a in attn_sets]
    output_ws = [a[:, project_cols:] for a in attn_sets]
    up_ws = [f[:, :hidden_cols] for f in feed_sets]
    down_ws = [f[:, hidden_cols:] for f in feed_sets]

    def project_bias(k):
        query_part = lax.dynamic_slice_in_dim(query_projection_bias, k * head_cols, head_cols)
        value_part = lax.dynamic_slice_in_dim(value_projection_bias, k * head_cols, head_cols)
        return jnp.concatenate([query_part, jnp.zeros_like(query_part), value_part])

    project_biases = [project_bias(k) for k in slices]
    up_biases = [
        lax.dynamic_slice_in_dim(feed_input_bias, k * hidden_cols, hidden_cols) for k in slices
    ]

    def split_heads(qkv_block):
        query_rows = qkv_block[:, :head_cols].reshape(seq_rows, heads_here, HD)
        key_rows = qkv_block[:, head_cols : 2 * head_cols].reshape(seq_rows, heads_here, HD)
        value_rows = qkv_block[:, 2 * head_cols :].reshape(seq_rows, heads_here, HD)
        return (query_rows, key_rows, value_rows)

    def masked_scores(query_rows, key_rows):
        raw_scores = (
            jnp.einsum("qhe,khe->hqk", query_rows, key_rows, preferred_element_type=jnp.float32)
            * score_scale
        )
        return jnp.where(key_valid[None, None, :], raw_scores, MASKED)

    def attend(qkv_block):
        query_rows, key_rows, value_rows = split_heads(qkv_block)
        scores = masked_scores(query_rows, key_rows)
        row_max = jnp.max(scores, axis=-1, keepdims=True)
        exponent = jnp.exp(scores - row_max)
        row_total = jnp.sum(exponent, axis=-1, keepdims=True)
        weights = (exponent / row_total).astype(jnp.bfloat16)
        mixed_heads = jnp.einsum(
            "hqk,khe->qhe", weights, value_rows, preferred_element_type=jnp.float32
        )
        return (
            mixed_heads.reshape(seq_rows, head_cols).astype(jnp.bfloat16),
            (row_max + jnp.log(row_total))[..., 0],
        )

    def attend_back(qkv_block, row_lse, grad_block):
        query_rows, key_rows, value_rows = split_heads(qkv_block)
        weights = jnp.exp(masked_scores(query_rows, key_rows) - row_lse[..., None])
        grad_heads = grad_block.reshape(seq_rows, heads_here, HD)
        grad_weights = jnp.einsum(
            "qhe,khe->hqk", grad_heads, value_rows, preferred_element_type=jnp.float32
        )
        inner_sum = jnp.sum(weights * grad_weights, axis=-1, keepdims=True)
        grad_scores = (weights * (grad_weights - inner_sum)).astype(jnp.bfloat16)
        grad_query = (
            jnp.einsum("hqk,khe->qhe", grad_scores, key_rows, preferred_element_type=jnp.float32)
            * score_scale
        )
        grad_key = (
            jnp.einsum("hqk,qhe->khe", grad_scores, query_rows, preferred_element_type=jnp.float32)
            * score_scale
        )
        grad_value = jnp.einsum(
            "hqk,qhe->khe", weights.astype(jnp.bfloat16), grad_heads,
            preferred_element_type=jnp.float32,
        )
        joined = jnp.concatenate(
            [
                grad_query.reshape(seq_rows, head_cols),
                grad_key.reshape(seq_rows, head_cols),
                grad_value.reshape(seq_rows, head_cols),
            ],
            axis=-1,
        )
        return joined.astype(jnp.bfloat16)

    gelu_exact = partial(jax.nn.gelu, approximate=False)
    groups = range(2)

    projected = [
        (dot_nn(inputs_full, project_ws[g]) + project_biases[g]).astype(jnp.bfloat16)
        for g in groups
    ]
    attended = [attend(projected[g]) for g in groups]
    mixed = [a[0] for a in attended]
    log_total = [a[1] for a in attended]
    branch = scatter_cores(sum(dot_nt(mixed[g], output_ws[g]) for g in groups))
    first, normed_first, inverse_first = norm_forward(
        inputs_mine.astype(jnp.float32) + branch + attention_output_bias, first_gain, first_shift
    )
    first_full = gather_cores(first)
    preact = [dot_nn(first_full, up_ws[0]) + up_biases[0]]
    gelu_pairs = [jax.vjp(gelu_exact, preact[0])]
    hidden = [gelu_pairs[0][0].astype(jnp.bfloat16)]
    preact.append(dot_nn(first_full, up_ws[1]) + up_biases[1])
    gelu_pairs.append(jax.vjp(gelu_exact, preact[1]))
    hidden.append(gelu_pairs[1][0].astype(jnp.bfloat16))
    feed = scatter_cores(sum(dot_nt(hidden[g], down_ws[g]) for g in groups))
    second, normed_second, inverse_second = norm_forward(
        first + feed + feed_output_bias, second_gain, second_shift
    )
    out_mine = second.astype(jnp.bfloat16)
    out_other = to_chip_partner(out_mine[block_rows:])
    out_own = out_mine[:block_rows]
    on_left = chip_side == 0
    layer_output = jnp.stack(
        [jnp.where(on_left, out_own, out_other), jnp.where(on_left, out_other, out_own)], axis=1
    )

    cot = cot_mine.astype(jnp.float32)
    second_gain_part = jnp.sum(cot * normed_second, axis=0)
    second_shift_part = jnp.sum(cot, axis=0)
    grad_second = norm_backward(cot, normed_second, inverse_second, second_gain)
    down_bias_part = jnp.sum(grad_second, axis=0)
    grad_feed_full = gather_cores(grad_second)
    grad_hidden = [dot_nn(grad_feed_full, down_ws[g]) for g in groups]
    down_grads = [dot_tn(grad_feed_full, hidden[g]) for g in groups]
    grad_preact = [gelu_pairs[g][1](grad_hidden[g])[0].astype(jnp.bfloat16) for g in groups]
    up_grads = [dot_tn(first_full, grad_preact[g]) for g in groups]
    up_bias_sums = [jnp.sum(grad_preact[g], axis=0, dtype=jnp.float32) for g in groups]
    grad_first = grad_second + scatter_cores(sum(dot_nt(grad_preact[g], up_ws[g]) for g in groups))
    first_gain_part = jnp.sum(grad_first * normed_first, axis=0)
    first_shift_part = jnp.sum(grad_first, axis=0)
    grad_residual = norm_backward(grad_first, normed_first, inverse_first, first_gain)
    output_bias_part = jnp.sum(grad_residual, axis=0)
    branch_grad_full = gather_cores(grad_residual)
    grad_mixed = [dot_nn(branch_grad_full, output_ws[g]).astype(jnp.bfloat16) for g in groups]
    output_grads = [dot_tn(branch_grad_full, mixed[g]) for g in groups]

    def place(parts, part_len, total_len):
        blank = jnp.zeros((total_len,), jnp.float32)
        for g in groups:
            blank = lax.dynamic_update_slice_in_dim(blank, parts[g], slices[g] * part_len, 0)
        return blank

    rows_block = width // n_data
    vec_block = width // n_all
    up_placed = place(up_bias_sums, hidden_cols, hidden_cols * n_tensor)
    up_columns = (
        up_placed.reshape(n_data, n_tensor, rows_block).transpose(0, 2, 1).reshape(width, n_tensor)
    )
    early_columns = jnp.concatenate(
        [
            jnp.stack(
                [
                    output_bias_part,
                    first_gain_part,
                    first_shift_part,
                    down_bias_part,
                    second_gain_part,
                    second_shift_part,
                ],
                axis=1,
            ),
            up_columns,
        ],
        axis=1,
    )
    early_columns = early_columns + to_core_partner(early_columns)
    early_own = jnp.concatenate([up_grads[0], down_grads[0], output_grads[0]], axis=1)
    early_partner = jnp.concatenate([up_grads[1], down_grads[1], output_grads[1]], axis=1)
    early_cols = early_own.shape[1]
    early_pack = jnp.concatenate([early_own, early_partner, early_columns], axis=1).astype(
        jnp.bfloat16
    )
    early_pack, grad_mixed = lax.optimization_barrier((early_pack, grad_mixed))
    early_reduced = lax.psum_scatter(
        early_pack, "dp", scatter_dimension=0, tiled=True
    ).astype(jnp.float32)
    early_sent = to_chip_partner(early_reduced[:, early_cols:].astype(jnp.bfloat16)).astype(
        jnp.float32
    )
    early_shard = early_reduced[:, :early_cols] + early_sent[:, :early_cols]
    early_small = early_reduced[:, 2 * early_cols :] + early_sent[:, early_cols:]
    up_shard = early_shard[:, :hidden_cols]
    down_shard = early_shard[:, hidden_cols : 2 * hidden_cols]
    output_shard = early_shard[:, 2 * hidden_cols :]

    grad_projected = [attend_back(projected[g], log_total[g], grad_mixed[g]) for g in groups]
    project_grads = [dot_tn(inputs_full, grad_projected[g]) for g in groups]
    qkv_bias_sums = [jnp.sum(grad_projected[g], axis=0, dtype=jnp.float32) for g in groups]
    grad_inputs = grad_residual + scatter_cores(
        sum(dot_nt(grad_projected[g], project_ws[g]) for g in groups)
    )

    late_columns = jnp.stack(
        [
            place([q[:head_cols] for q in qkv_bias_sums], head_cols, width),
            place([q[2 * head_cols :] for q in qkv_bias_sums], head_cols, width),
        ],
        axis=1,
    )
    late_columns = late_columns + to_core_partner(late_columns)
    late_own = jnp.concatenate([project_grads[0], late_columns], axis=1)
    late_partner = jnp.concatenate([project_grads[1], late_columns], axis=1)
    late_total = late_own + to_chip_partner(late_partner.astype(jnp.bfloat16)).astype(jnp.float32)
    late_shard = scatter_dp_permutes(late_total)
    project_shard = late_shard[:, :project_cols]

    def mine_of(column):
        return lax.dynamic_slice_in_dim(column, tensor_index * vec_block, vec_block)

    early = [mine_of(early_small[:, k]) for k in range(6)]
    up_bias_shard = lax.dynamic_index_in_dim(early_small[:, 6:], tensor_index, axis=1, keepdims=False)
    late = [mine_of(late_shard[:, project_cols + k]) for k in range(2)]
    small = [
        late[0],
        late[1],
        early[0],
        early[1],
        early[2],
        up_bias_shard,
        early[3],
        early[4],
        early[5],
    ]

    grad_low = grad_inputs.astype(jnp.bfloat16)
    grad_other = to_chip_partner(grad_low[block_rows:])
    grad_own = grad_low[:block_rows]
    grad_here = jnp.stack(
        [jnp.where(on_left, grad_own, grad_other), jnp.where(on_left, grad_other, grad_own)],
        axis=1,
    )
    returned = lax.all_to_all(grad_here, "dp", split_axis=0, concat_axis=1, tiled=True)
    tokens_grad = jnp.einsum(
        "qs,pqd->psd", placing, returned, preferred_element_type=jnp.float32
    ).astype(jnp.bfloat16)

    return (
        layer_output,
        tokens_grad,
        project_shard,
        small[0],
        small[1],
        output_shard,
        small[2],
        small[3],
        small[4],
        up_shard,
        small[5],
        down_shard,
        small[6],
        small[7],
        small[8],
    )


def solution(mesh):
    in_specs = (
        P(("dp", "tensor"), None, None),
        P(),
        P(),
        P("dp", "tensor"),
        P(),
        P(),
        P("dp", "tensor"),
        P(),
        P(),
        P(),
        P("dp", "tensor"),
        P(),
        P("dp", "tensor"),
        P(),
        P(),
        P(),
        P(("dp", "tensor"), None, None),
    )
    out_specs = (
        P("tensor", "dp", None),
        P(("dp", "tensor"), None, None),
        P("dp", "tensor"),
        P(("dp", "tensor")),
        P(("dp", "tensor")),
        P("dp", "tensor"),
        P(("dp", "tensor")),
        P(("dp", "tensor")),
        P(("dp", "tensor")),
        P("dp", "tensor"),
        P(("dp", "tensor")),
        P("dp", "tensor"),
        P(("dp", "tensor")),
        P(("dp", "tensor")),
        P(("dp", "tensor")),
    )

    return jax.shard_map(
        on_device, mesh=mesh, in_specs=in_specs, out_specs=out_specs, check_vma=False
    )
```

```python
from functools import partial

import jax
import jax.numpy as jnp
from jax import lax
from jax.sharding import PartitionSpec as P

HD = 64


EPSILON = 1e-12
MASKED = -1e30


def norm_forward(value, gain, shift):
    centred = value - jnp.mean(value, axis=-1, keepdims=True)
    inverse = lax.rsqrt(jnp.mean(centred * centred, axis=-1, keepdims=True) + EPSILON)
    normed = centred * inverse
    return (normed * gain + shift, normed, inverse)


def norm_backward(upstream, normed, inverse, gain):
    scaled = upstream * gain
    first_mean = jnp.mean(scaled, axis=-1, keepdims=True)
    second_mean = jnp.mean(scaled * normed, axis=-1, keepdims=True)
    return inverse * (scaled - first_mean - normed * second_mean)


def dot_nt(a, b):
    return lax.dot_general(a, b, (((1,), (1,)), ((), ())), preferred_element_type=jnp.float32)


def dot_tn(a, b):
    return lax.dot_general(a, b, (((0,), (0,)), ((), ())), preferred_element_type=jnp.float32)


def dot_nn(a, b):
    return jnp.dot(a, b, preferred_element_type=jnp.float32)


def on_device(
    tokens,
    lengths,
    dealing,
    project_weight,
    query_projection_bias,
    value_projection_bias,
    attention_output_weight,
    attention_output_bias,
    first_gain,
    first_shift,
    feed_input_weight,
    feed_input_bias,
    feed_output_weight,
    feed_output_bias,
    second_gain,
    second_shift,
    output_grad,
):
    n_data = lax.axis_size("dp")
    n_tensor = lax.axis_size("tensor")
    n_all = n_data * n_tensor
    data_index = lax.axis_index("dp")
    tensor_index = lax.axis_index("tensor")
    seq_total = dealing.shape[0]
    seq_here = seq_total // n_data
    assert n_tensor == 4 and seq_here == 2
    piece_rows = tokens.shape[0]
    block_rows = piece_rows * n_data
    seq_rows = block_rows * n_tensor
    half_rows = seq_rows // 2
    width = tokens.shape[2]
    head_cols = attention_output_weight.shape[1]
    heads_here = head_cols // HD
    hidden_cols = feed_input_weight.shape[1]
    project_cols = project_weight.shape[1]
    score_scale = HD ** (-0.5)

    chip_side = tensor_index // 2
    core = tensor_index % 2
    partner_slice = tensor_index ^ 2
    across_chips = [(k, k ^ 2) for k in range(n_tensor)]
    across_cores = [(k, k ^ 1) for k in range(n_tensor)]

    def to_chip_partner(value):
        return lax.ppermute(value, "tensor", across_chips)

    def to_core_partner(value):
        return lax.ppermute(value, "tensor", across_cores)

    def gather_dp(block):
        return lax.all_gather(block, "dp", axis=0, tiled=True)

    def scatter_dp(total):
        return lax.psum_scatter(
            total.astype(jnp.bfloat16), "dp", scatter_dimension=0, tiled=True
        ).astype(jnp.float32)

    def scatter_dp_permutes(total):
        if n_data > 8:
            return scatter_dp(total)
        pieces = total.astype(jnp.bfloat16).reshape(n_data, -1, *total.shape[1:])
        acc = lax.dynamic_index_in_dim(
            total.reshape(pieces.shape), data_index, 0, keepdims=False
        )
        for k in range(1, n_data):
            sent = lax.dynamic_index_in_dim(pieces, (data_index + k) % n_data, 0, keepdims=False)
            acc = acc + lax.ppermute(
                sent, "dp", [(j, (j + k) % n_data) for j in range(n_data)]
            ).astype(jnp.float32)
        return acc

    def gather_cores(mine):
        low = mine.astype(jnp.bfloat16)
        return jnp.concatenate([low, to_core_partner(low)], axis=0)

    def scatter_cores(partial_sum):
        sent = to_core_partner(partial_sum[half_rows:].astype(jnp.bfloat16))
        return partial_sum[:half_rows] + sent.astype(jnp.float32)

    slot_ids = jnp.arange(seq_total, dtype=jnp.int32)
    placing = (dealing[None, :] == slot_ids[:, None]).astype(jnp.bfloat16)
    def deal(values):
        sent = jnp.einsum(
            "qs,psd->pqd", placing, values, preferred_element_type=jnp.float32
        ).astype(jnp.bfloat16)
        here = lax.all_to_all(sent, "dp", split_axis=1, concat_axis=0, tiled=True)
        slot_mine = lax.dynamic_index_in_dim(here, chip_side, axis=1, keepdims=False)
        slot_other = lax.dynamic_index_in_dim(here, 1 - chip_side, axis=1, keepdims=False)
        return jnp.concatenate([slot_mine, to_chip_partner(slot_other)], axis=0)

    inputs_mine = deal(tokens)
    cot_mine = deal(output_grad)
    inputs_full = jnp.concatenate([inputs_mine, to_core_partner(inputs_mine)], axis=0)

    my_slot = data_index * seq_here + chip_side
    seq_length = jnp.sum(jnp.where(dealing == my_slot, lengths, 0))
    blocks = jnp.stack(
        [
            tensor_index,
            partner_slice,
            tensor_index ^ 1,
            partner_slice ^ 1,
        ]
    )
    row_ids = jnp.arange(seq_rows, dtype=jnp.int32)
    owner = blocks[row_ids // block_rows]
    inner = row_ids % block_rows
    position = (inner // piece_rows * n_tensor + owner) * piece_rows + inner % piece_rows
    key_valid = position < seq_length

    attn_w = jnp.concatenate([project_weight, attention_output_weight], axis=1)
    feed_w = jnp.concatenate([feed_input_weight, feed_output_weight], axis=1)
    attn_own = gather_dp(attn_w)
    feed_own = gather_dp(feed_w)
    attn_part = to_chip_partner(attn_own)
    feed_part = to_chip_partner(feed_own)
    slices = (tensor_index, partner_slice)
    attn_sets = (attn_own, attn_part)
    feed_sets = (feed_own, feed_part)
    project_ws = [a[:, :project_cols] for a in attn_sets]
    output_ws = [a[:, project_cols:] for a in attn_sets]
    up_ws = [f[:, :hidden_cols] for f in feed_sets]
    down_ws = [f[:, hidden_cols:] for f in feed_sets]

    def project_bias(k):
        query_part = lax.dynamic_slice_in_dim(query_projection_bias, k * head_cols, head_cols)
        value_part = lax.dynamic_slice_in_dim(value_projection_bias, k * head_cols, head_cols)
        return jnp.concatenate([query_part, jnp.zeros_like(query_part), value_part])

    project_biases = [project_bias(k) for k in slices]
    up_biases = [
        lax.dynamic_slice_in_dim(feed_input_bias, k * hidden_cols, hidden_cols) for k in slices
    ]

    def split_heads(qkv_block):
        query_rows = qkv_block[:, :head_cols].reshape(seq_rows, heads_here, HD)
        key_rows = qkv_block[:, head_cols : 2 * head_cols].reshape(seq_rows, heads_here, HD)
        value_rows = qkv_block[:, 2 * head_cols :].reshape(seq_rows, heads_here, HD)
        return (query_rows, key_rows, value_rows)

    def masked_scores(query_rows, key_rows):
        raw_scores = (
            jnp.einsum("qhe,khe->hqk", query_rows, key_rows, preferred_element_type=jnp.float32)
            * score_scale
        )
        return jnp.where(key_valid[None, None, :], raw_scores, MASKED)

    def attend(qkv_block):
        query_rows, key_rows, value_rows = split_heads(qkv_block)
        scores = masked_scores(query_rows, key_rows)
        row_max = jnp.max(scores, axis=-1, keepdims=True)
        exponent = jnp.exp(scores - row_max)
        row_total = jnp.sum(exponent, axis=-1, keepdims=True)
        probabilities = exponent / row_total
        mixed_heads = jnp.einsum(
            "hqk,khe->qhe", probabilities.astype(jnp.bfloat16), value_rows,
            preferred_element_type=jnp.float32,
        )
        return (
            mixed_heads.reshape(seq_rows, head_cols).astype(jnp.bfloat16),
            probabilities,
        )

    def attend_back(qkv_block, row_lse, grad_block):
        query_rows, key_rows, value_rows = split_heads(qkv_block)
        weights = row_lse
        grad_heads = grad_block.reshape(seq_rows, heads_here, HD)
        grad_weights = jnp.einsum(
            "qhe,khe->hqk", grad_heads, value_rows, preferred_element_type=jnp.float32
        )
        inner_sum = jnp.sum(weights * grad_weights, axis=-1, keepdims=True)
        grad_scores = (weights * (grad_weights - inner_sum)).astype(jnp.bfloat16)
        grad_query = (
            jnp.einsum("hqk,khe->qhe", grad_scores, key_rows, preferred_element_type=jnp.float32)
            * score_scale
        )
        grad_key = (
            jnp.einsum("hqk,qhe->khe", grad_scores, query_rows, preferred_element_type=jnp.float32)
            * score_scale
        )
        grad_value = jnp.einsum(
            "hqk,qhe->khe", weights.astype(jnp.bfloat16), grad_heads,
            preferred_element_type=jnp.float32,
        )
        joined = jnp.concatenate(
            [
                grad_query.reshape(seq_rows, head_cols),
                grad_key.reshape(seq_rows, head_cols),
                grad_value.reshape(seq_rows, head_cols),
            ],
            axis=-1,
        )
        return joined.astype(jnp.bfloat16)

    gelu_exact = partial(jax.nn.gelu, approximate=False)
    groups = range(2)

    projected = [
        (dot_nn(inputs_full, project_ws[g]) + project_biases[g]).astype(jnp.bfloat16)
        for g in groups
    ]
    attended = [attend(projected[g]) for g in groups]
    mixed = [a[0] for a in attended]
    log_total = [a[1] for a in attended]
    branch = scatter_cores(sum(dot_nt(mixed[g], output_ws[g]) for g in groups))
    first, normed_first, inverse_first = norm_forward(
        inputs_mine.astype(jnp.float32) + branch + attention_output_bias, first_gain, first_shift
    )
    first_full = gather_cores(first)
    preact = [dot_nn(first_full, up_ws[g]) + up_biases[g] for g in groups]
    gelu_pairs = [jax.vjp(gelu_exact, preact[g]) for g in groups]
    hidden = [p[0].astype(jnp.bfloat16) for p in gelu_pairs]
    feed = scatter_cores(sum(dot_nt(hidden[g], down_ws[g]) for g in groups))
    second, normed_second, inverse_second = norm_forward(
        first + feed + feed_output_bias, second_gain, second_shift
    )
    out_mine = second.astype(jnp.bfloat16)
    out_other = to_chip_partner(out_mine[block_rows:])
    out_own = out_mine[:block_rows]
    on_left = chip_side == 0
    layer_output = jnp.stack(
        [jnp.where(on_left, out_own, out_other), jnp.where(on_left, out_other, out_own)], axis=1
    )

    cot = cot_mine.astype(jnp.float32)
    second_gain_part = jnp.sum(cot * normed_second, axis=0)
    second_shift_part = jnp.sum(cot, axis=0)
    grad_second = norm_backward(cot, normed_second, inverse_second, second_gain)
    down_bias_part = jnp.sum(grad_second, axis=0)
    grad_feed_full = gather_cores(grad_second)
    grad_hidden = [dot_nn(grad_feed_full, down_ws[g]) for g in groups]
    down_grads = [dot_tn(grad_feed_full, hidden[g]) for g in groups]
    grad_preact = [gelu_pairs[g][1](grad_hidden[g])[0].astype(jnp.bfloat16) for g in groups]
    up_grads = [dot_tn(first_full, grad_preact[g]) for g in groups]
    up_bias_sums = [jnp.sum(grad_preact[g], axis=0, dtype=jnp.float32) for g in groups]
    grad_first = grad_second + scatter_cores(sum(dot_nt(grad_preact[g], up_ws[g]) for g in groups))
    first_gain_part = jnp.sum(grad_first * normed_first, axis=0)
    first_shift_part = jnp.sum(grad_first, axis=0)
    grad_residual = norm_backward(grad_first, normed_first, inverse_first, first_gain)
    output_bias_part = jnp.sum(grad_residual, axis=0)
    branch_grad_full = gather_cores(grad_residual)
    grad_mixed = [dot_nn(branch_grad_full, output_ws[g]).astype(jnp.bfloat16) for g in groups]
    output_grads = [dot_tn(branch_grad_full, mixed[g]) for g in groups]

    def place(parts, part_len, total_len):
        blank = jnp.zeros((total_len,), jnp.float32)
        for g in groups:
            blank = lax.dynamic_update_slice_in_dim(blank, parts[g], slices[g] * part_len, 0)
        return blank

    rows_block = width // n_data
    vec_block = width // n_all
    up_placed = place(up_bias_sums, hidden_cols, hidden_cols * n_tensor)
    up_columns = (
        up_placed.reshape(n_data, n_tensor, rows_block).transpose(0, 2, 1).reshape(width, n_tensor)
    )
    early_columns = jnp.concatenate(
        [
            jnp.stack(
                [
                    output_bias_part,
                    first_gain_part,
                    first_shift_part,
                    down_bias_part,
                    second_gain_part,
                    second_shift_part,
                ],
                axis=1,
            ),
            up_columns,
        ],
        axis=1,
    )
    early_columns = early_columns + to_core_partner(early_columns)
    early_own = jnp.concatenate([up_grads[0], down_grads[0], output_grads[0]], axis=1)
    early_partner = jnp.concatenate([up_grads[1], down_grads[1], output_grads[1]], axis=1)
    early_cols = early_own.shape[1]
    early_pack = jnp.concatenate([early_own, early_partner, early_columns], axis=1).astype(
        jnp.bfloat16
    )
    early_pack, grad_mixed = lax.optimization_barrier((early_pack, grad_mixed))
    early_reduced = lax.psum_scatter(
        early_pack, "dp", scatter_dimension=0, tiled=True
    ).astype(jnp.float32)
    early_sent = to_chip_partner(early_reduced[:, early_cols:].astype(jnp.bfloat16)).astype(
        jnp.float32
    )
    early_shard = early_reduced[:, :early_cols] + early_sent[:, :early_cols]
    early_small = early_reduced[:, 2 * early_cols :] + early_sent[:, early_cols:]
    up_shard = early_shard[:, :hidden_cols]
    down_shard = early_shard[:, hidden_cols : 2 * hidden_cols]
    output_shard = early_shard[:, 2 * hidden_cols :]

    grad_projected = [attend_back(projected[g], log_total[g], grad_mixed[g]) for g in groups]
    project_grads = [dot_tn(inputs_full, grad_projected[g]) for g in groups]
    qkv_bias_sums = [jnp.sum(grad_projected[g], axis=0, dtype=jnp.float32) for g in groups]
    grad_inputs = grad_residual + scatter_cores(
        sum(dot_nt(grad_projected[g], project_ws[g]) for g in groups)
    )

    late_columns = jnp.stack(
        [
            place([q[:head_cols] for q in qkv_bias_sums], head_cols, width),
            place([q[2 * head_cols :] for q in qkv_bias_sums], head_cols, width),
        ],
        axis=1,
    )
    late_columns = late_columns + to_core_partner(late_columns)
    late_own = jnp.concatenate([project_grads[0], late_columns], axis=1)
    late_partner = jnp.concatenate([project_grads[1], late_columns], axis=1)
    late_total = late_own + to_chip_partner(late_partner.astype(jnp.bfloat16)).astype(jnp.float32)
    late_shard = scatter_dp_permutes(late_total)
    project_shard = late_shard[:, :project_cols]

    def mine_of(column):
        return lax.dynamic_slice_in_dim(column, tensor_index * vec_block, vec_block)

    early = [mine_of(early_small[:, k]) for k in range(6)]
    up_bias_shard = lax.dynamic_index_in_dim(early_small[:, 6:], tensor_index, axis=1, keepdims=False)
    late = [mine_of(late_shard[:, project_cols + k]) for k in range(2)]
    small = [
        late[0],
        late[1],
        early[0],
        early[1],
        early[2],
        up_bias_shard,
        early[3],
        early[4],
        early[5],
    ]

    grad_low = grad_inputs.astype(jnp.bfloat16)
    grad_other = to_chip_partner(grad_low[block_rows:])
    grad_own = grad_low[:block_rows]
    grad_here = jnp.stack(
        [jnp.where(on_left, grad_own, grad_other), jnp.where(on_left, grad_other, grad_own)],
        axis=1,
    )
    returned = lax.all_to_all(grad_here, "dp", split_axis=0, concat_axis=1, tiled=True)
    tokens_grad = jnp.einsum(
        "qs,pqd->psd", placing, returned, preferred_element_type=jnp.float32
    ).astype(jnp.bfloat16)

    return (
        layer_output,
        tokens_grad,
        project_shard,
        small[0],
        small[1],
        output_shard,
        small[2],
        small[3],
        small[4],
        up_shard,
        small[5],
        down_shard,
        small[6],
        small[7],
        small[8],
    )


def solution(mesh):
    in_specs = (
        P(("dp", "tensor"), None, None),
        P(),
        P(),
        P("dp", "tensor"),
        P(),
        P(),
        P("dp", "tensor"),
        P(),
        P(),
        P(),
        P("dp", "tensor"),
        P(),
        P("dp", "tensor"),
        P(),
        P(),
        P(),
        P(("dp", "tensor"), None, None),
    )
    out_specs = (
        P("tensor", "dp", None),
        P(("dp", "tensor"), None, None),
        P("dp", "tensor"),
        P(("dp", "tensor")),
        P(("dp", "tensor")),
        P("dp", "tensor"),
        P(("dp", "tensor")),
        P(("dp", "tensor")),
        P(("dp", "tensor")),
        P("dp", "tensor"),
        P(("dp", "tensor")),
        P("dp", "tensor"),
        P(("dp", "tensor")),
        P(("dp", "tensor")),
        P(("dp", "tensor")),
    )
    return jax.shard_map(
        on_device, mesh=mesh, in_specs=in_specs, out_specs=out_specs, check_vma=False
    )
```
